768 devices in a mesh: slab: 192 (over z_lo, x, y, core), cross: 4 (over z_hi).
Axes of the slice: x: 4, y: 8, z: 12 (z_hi: 4, z_lo: 3; z = z_hi * 3 + z_lo), core: 2. Of those that a mesh axis runs over, the one named last changes fastest.
Arguments:
- velocity: float32 [3, 768, 64, 128], P(None, 'slab', 'cross'), may hold values from -6 to 6
- density: float32 [768, 64, 128], P('slab', 'cross'), may hold values from 0.5 to 2
- source: float32 [768, 64, 128], P('slab', 'cross'), may hold values from -6 to 6
- species: float32 [9, 768, 64, 128], P(None, 'slab', 'cross'), may hold values from 0 to 1
Outputs:
- velocity_out: float32 [3, 768, 64, 128], P(None, 'slab', 'cross')
- pressure: float32 [768, 64, 128], P('slab', 'cross')
- species_out: float32 [9, 768, 64, 128], P(None, 'slab', 'cross')
The draws below stay inside these ranges and needn't reach their ends.
All inputs are finite; a program needn't handle non-finite values.
Results may differ from the reference program's by a relative error of at most 0.0001.
Values sent between devices are 32-bit elements; how exact they have to be, the bound alone decides.
No kernel may reach another device: no remote copies, remote signals or barrier semaphores. Data moves between devices by JAX's collectives and lax.ppermute only.
A program may use at most 32 MiB of HBM per device.

```python
import math
import jax
import jax.numpy as jnp

NZ = 128
SPECIES = 9
CYCLES = 2
SMOOTH = 2
COARSE = 4
NX = 768
NY = 64


def shard_levels(key, shape, pieces, low, largest):
    gain = 1.0
    for axis_at, blocks in pieces:
        heights = jax.random.uniform(jax.random.fold_in(jax.random.fold_in(key, 6), axis_at), (blocks,), jnp.float32, low / len(pieces), largest / len(pieces))
        gain = gain * jnp.repeat(jnp.exp(heights), shape[axis_at] // blocks).reshape((-1,) + (1,) * (len(shape) - 1 - axis_at))
    return gain


def centred(rng, shape, scale, reach, pieces=(), dtype=jnp.bfloat16):
    drawn = jax.random.normal(rng, shape, jnp.float32) * scale
    if len(pieces) > 0:
        drawn = shard_levels(rng, shape, pieces, -0.22, 0.18) * drawn
    return jnp.clip(drawn, min=-reach, max=reach).astype(dtype)


def setup_inputs(seed: int = 0) -> dict:
    key_of = jax.random.split(jax.random.key(seed), 5)
    velocity = centred(key_of[0], (3, NX, NY, NZ), 1.0, 6.0, ((1, 192), (2, 4)), jnp.float32)
    density = jnp.clip(jnp.exp(math.log(2.0) - 1.3862944 * jax.random.uniform(key_of[1], (NX, NY, NZ), jnp.float32) ** shard_levels(key_of[1], (NX, NY, NZ), ((0, 192), (1, 4)), -0.2, 0.2)), 0.5, 2.0)
    source = centred(key_of[2], (NX, NY, NZ), 1.0, 6.0, ((0, 192), (1, 4)), jnp.float32)
    species = jnp.clip(1.0 * jax.random.uniform(key_of[3], (SPECIES, NX, NY, NZ), jnp.float32) ** shard_levels(key_of[3], (SPECIES, NX, NY, NZ), ((1, 192), (2, 4)), -0.2, 0.2), 0.0, 1.0)
    return dict(velocity=velocity, density=density, source=source, species=species)


damping = 0.8
time_step = 0.25


def pad_plane(field, width):
    return jnp.pad(field, ((width, width), (width, width), (0, 0)))


def pad_stack(field, width):
    return jnp.pad(field, ((0, 0), (width, width), (width, width), (0, 0)))


def pad_depth(field):
    return jnp.pad(field, ((0, 0), (0, 0), (1, 1)))


def face_weights(mobile):
    face_x = 0.5 * (mobile[:-1, 1:-1] + mobile[1:, 1:-1])
    face_y = 0.5 * (mobile[1:-1, :-1] + mobile[1:-1, 1:])
    inner = pad_depth(mobile[1:-1, 1:-1])
    face_z = 0.5 * (inner[..., :-1] + inner[..., 1:])
    diagonal = face_x[:-1] + face_x[1:] + face_y[:, :-1] + face_y[:, 1:] + face_z[..., :-1] + face_z[..., 1:]
    return face_x, face_y, face_z, diagonal


def operate(field, weights):
    face_x, face_y, face_z = weights[0], weights[1], weights[2]
    center = field[1:-1, 1:-1]
    column = pad_depth(center)
    total = face_x[1:] * (field[2:, 1:-1] - center) + face_x[:-1] * (field[:-2, 1:-1] - center)
    total = total + face_y[:, 1:] * (field[1:-1, 2:] - center) + face_y[:, :-1] * (field[1:-1, :-2] - center)
    total = total + face_z[..., 1:] * (column[..., 2:] - center) + face_z[..., :-1] * (column[..., :-2] - center)
    return total


def jacobi_step(field, target, weights):
    center = field[1:-1, 1:-1]
    return center + damping * (operate(field, weights) - target) / weights[3]


def divergence(moving):
    column = pad_depth(moving[2][1:-1, 1:-1])
    total = (moving[0][2:, 1:-1] - moving[0][:-2, 1:-1]) + (moving[1][1:-1, 2:] - moving[1][1:-1, :-2])
    return 0.5 * (total + (column[..., 2:] - column[..., :-2]))


def gradient(field):
    column = pad_depth(field[1:-1, 1:-1])
    along_x = 0.5 * (field[2:, 1:-1] - field[:-2, 1:-1])
    along_y = 0.5 * (field[1:-1, 2:] - field[1:-1, :-2])
    along_z = 0.5 * (column[..., 2:] - column[..., :-2])
    return jnp.stack([along_x, along_y, along_z], 0)


def restrict(field):
    cells_x, cells_y, cells_z = field.shape
    return field.reshape(cells_x // 2, 2, cells_y // 2, 2, cells_z // 2, 2).mean(axis=(1, 3, 5))


def prolong(field):
    cells_x, cells_y, cells_z = field.shape
    spread = jnp.broadcast_to(field[:, None, :, None, :, None], (cells_x, 2, cells_y, 2, cells_z, 2))
    return spread.reshape(2 * cells_x, 2 * cells_y, 2 * cells_z)


def advect(amounts, moving):
    flow_x = 0.5 * (moving[0][:-1, 1:-1] + moving[0][1:, 1:-1])
    flux_x = jnp.maximum(flow_x, 0.0) * amounts[:, :-1, 1:-1] + jnp.minimum(flow_x, 0.0) * amounts[:, 1:, 1:-1]
    flow_y = 0.5 * (moving[1][1:-1, :-1] + moving[1][1:-1, 1:])
    flux_y = jnp.maximum(flow_y, 0.0) * amounts[:, 1:-1, :-1] + jnp.minimum(flow_y, 0.0) * amounts[:, 1:-1, 1:]
    column = pad_depth(moving[2][1:-1, 1:-1])
    flow_z = 0.5 * (column[..., :-1] + column[..., 1:])
    center = amounts[:, 1:-1, 1:-1]
    stacked = jnp.pad(center, ((0, 0), (0, 0), (0, 0), (1, 1)))
    flux_z = jnp.maximum(flow_z, 0.0) * stacked[..., :-1] + jnp.minimum(flow_z, 0.0) * stacked[..., 1:]
    change = (flux_x[:, 1:] - flux_x[:, :-1]) + (flux_y[:, :, 1:] - flux_y[:, :, :-1]) + (flux_z[..., 1:] - flux_z[..., :-1])
    return center - time_step * change


def reference(velocity, density, source, species):
    mobility = 1.0 / density
    weights = face_weights(pad_plane(mobility, 1))
    target = divergence(pad_stack(velocity, 1)) - source
    coarse_weights = tuple(0.25 * part for part in face_weights(pad_plane(restrict(mobility), 1)))
    pressure = jnp.zeros_like(density)
    for cycle_index in range(CYCLES):
        for sweep_index in range(SMOOTH):
            pressure = jacobi_step(pad_plane(pressure, 1), target, weights)
        residual = target - operate(pad_plane(pressure, 1), weights)
        coarse_target = restrict(residual)
        correction = jnp.zeros_like(coarse_target)
        for sweep_index in range(COARSE):
            correction = jacobi_step(pad_plane(correction, 1), coarse_target, coarse_weights)
        pressure = pressure + prolong(correction)
        for sweep_index in range(SMOOTH):
            pressure = jacobi_step(pad_plane(pressure, 1), target, weights)
    velocity_out = velocity - mobility[None] * gradient(pad_plane(pressure, 1))
    species_out = advect(pad_stack(species, 1), pad_stack(velocity_out, 1))
    return velocity_out, pressure, species_out
```

```python
import functools

import jax
import jax.numpy as jnp
from jax import lax
from jax.experimental import pallas as pl
from jax.experimental.pallas import tpu as pltpu
from jax.sharding import PartitionSpec as P

INTERPRET = False
ROWS = 64
LANES = 128
BLOCK = 16
SPECIES = 9
EDGE = 160
damping = 0.8
time_step = 0.25


class Place:
    def __init__(self, counter, constant):
        self.counter = counter
        self.constant = constant

    def __add__(self, other):
        return Place(self.counter, self.constant + other)

    def __sub__(self, other):
        return Place(self.counter, self.constant - other)

    def __rmul__(self, factor):
        return Place(self.counter * factor, self.constant * factor)

    def index(self, shift=None):
        start = self.counter if shift is None else self.counter + shift
        return start + self.constant if self.constant else start


def loop(low, high, body):
    def step(i, carry):
        body(Place(i, low))
        return carry

    lax.fori_loop(0, high - low, step, 0)


def rows_of(shape):
    return lax.broadcasted_iota(jnp.int32, shape, 0)


def lanes_of(shape):
    return lax.broadcasted_iota(jnp.int32, shape, 1)


PLANE = (ROWS, LANES)


def roll_rows(x, by):
    return pltpu.roll(x, by % x.shape[0], 0)


def roll_lanes(x, by):
    return pltpu.roll(x, by % x.shape[1], 1)


class Weights:
    def __init__(self, ref, step):
        self.ref = ref
        self.step = step

    def fill(self, low, high, mobile, target, inside, scale):
        s = self.step
        row, lane = rows_of(PLANE), lanes_of(PLANE)
        y_low, y_high = row >= s, row < ROWS - s
        z_low, z_high = lane >= s, lane < LANES - s

        def body(i):
            m = mobile(i)
            x_m, x_p = mobile(i - 1), mobile(i + 1)
            y_m = jnp.where(y_low, roll_rows(m, s), 0.0)
            y_p = jnp.where(y_high, roll_rows(m, -s), 0.0)
            z_m = jnp.where(z_low, roll_lanes(m, s), 0.0)
            z_p = jnp.where(z_high, roll_lanes(m, -s), 0.0)
            diagonal = 3.0 * m + 0.5 * ((x_m + x_p) + (y_m + y_p) + (z_m + z_p))
            valid = inside(i)
            scaled = (damping * valid) / (diagonal + (1.0 - valid))
            half = 0.5 * scaled
            k = (i - low).index()
            self.ref[0, k] = (m + x_m) * half
            self.ref[1, k] = (m + x_p) * half
            self.ref[2, k] = jnp.where(y_low, (m + y_m) * half, 0.0)
            self.ref[3, k] = jnp.where(y_high, (m + y_p) * half, 0.0)
            self.ref[4, k] = jnp.where(z_low, (m + z_m) * half, 0.0)
            self.ref[5, k] = jnp.where(z_high, (m + z_p) * half, 0.0)
            self.ref[6, k] = target(i) * scaled * scale
            self.ref[7, k] = diagonal * (1.0 / damping)

        self.low = low
        loop(low, high, body)

    def change(self, field, i):
        s = self.step
        k = (i - self.low).index()
        p = field(i)
        total = self.ref[0, k] * field(i - 1) + self.ref[1, k] * field(i + 1)
        total = total + (self.ref[2, k] * roll_rows(p, s) + self.ref[3, k] * roll_rows(p, -s))
        total = total + (self.ref[4, k] * roll_lanes(p, s) + self.ref[5, k] * roll_lanes(p, -s))
        return p, (total - self.ref[6, k]) - damping * p


def at(ref, origin):
    return lambda i: ref[(i - origin).index()]


def sweep(weights, source, source_low, result, result_low, low, high):
    def body(i):
        p, change = weights.change(at(source, source_low), i)
        result[(i - result_low).index()] = p + change

    loop(low, high, body)


def first_sweep(weights, result, result_low, low, high):
    def body(i):
        result[(i - result_low).index()] = -weights.ref[6, (i - weights.low).index()]

    loop(low, high, body)


def pair_sum(q):
    row, lane = rows_of(PLANE), lanes_of(PLANE)
    q = q + jnp.where(lane % 2 == 0, roll_lanes(q, -1), roll_lanes(q, 1))
    return q + jnp.where(row % 2 == 0, roll_rows(q, -1), roll_rows(q, 1))


def packed(a, b, c, d):
    row, lane = rows_of(PLANE), lanes_of(PLANE)
    even = lane % 2 == 0
    return jnp.where(row % 2 == 0, jnp.where(even, a, b), jnp.where(even, c, d))


def unpacked(v):
    row, lane = rows_of(PLANE), lanes_of(PLANE)
    even, upper = lane % 2 == 0, row % 2 == 0
    first = jnp.where(even, v, roll_lanes(v, 1))
    second = jnp.where(even, roll_lanes(v, -1), v)

    def low_row(x):
        return jnp.where(upper, x, roll_rows(x, 1))

    def high_row(x):
        return jnp.where(upper, roll_rows(x, -1), x)

    return low_row(first), low_row(second), high_row(first), high_row(second)


def residual_planes(weights, field_ref, field_low, result, result_low, low, high):
    def body(i):
        field = at(field_ref, field_low)
        total = 0.0
        for half in range(2):
            _, change = weights.change(field, 2 * i + half)
            total = total - change * weights.ref[7, (2 * i + half - weights.low).index()]
        result[(i - result_low).index()] = 0.125 * pair_sum(total)

    loop(low, high, body)


def inside_of(first, count):
    def inside(i):
        place = i.index(first)
        return jnp.where((place >= 0) & (place < count), 1.0, 0.0)

    return inside


def bounded(place, k, count):
    return jnp.minimum(jnp.maximum(place[k], 0), count - 1)


def prepare(velocity, density, source, species, out):
    lane = lanes_of((BLOCK, LANES))
    row = rows_of((BLOCK, LANES))
    for x in range(4):
        out[BLOCK * x : BLOCK * (x + 1)] = 1.0 / density[x]
        u_p = velocity[0, x + 1] if x < 3 else 0.0
        u_m = velocity[0, x - 1] if x > 0 else 0.0
        v, w = velocity[1, x], velocity[2, x]
        v_p = jnp.where(row < BLOCK - 1, roll_rows(v, -1), 0.0)
        v_m = jnp.where(row > 0, roll_rows(v, 1), 0.0)
        w_p = jnp.where(lane < LANES - 1, roll_lanes(w, -1), 0.0)
        w_m = jnp.where(lane > 0, roll_lanes(w, 1), 0.0)
        moved = 0.5 * ((u_p - u_m) + (v_p - v_m) + (w_p - w_m))
        out[64 + BLOCK * x : 64 + BLOCK * (x + 1)] = moved - source[x]
        for s in range(SPECIES):
            r = EDGE + 4 * s + x
            out[r : r + 1] = species[s, x, 0:1]
            out[r + 36 : r + 37] = species[s, x, BLOCK - 1 : BLOCK]
        r = EDGE + 72 + x
        out[r : r + 1] = velocity[1, x, 0:1]
        out[r + 4 : r + 5] = velocity[1, x, BLOCK - 1 : BLOCK]
    out[128:144] = velocity[0, 0]
    out[144:160] = velocity[0, 3]


def assemble(place, gathered, mobile, target, edge, sent):
    north = place[0] == 0
    row = rows_of((BLOCK, LANES))
    for c in range(4):
        rows = slice(BLOCK * c, BLOCK * (c + 1))
        for k in range(2):
            block = 2 * c + k
            for x in range(4):
                mobile[4 * k + x, rows] = gathered[block, BLOCK * x : BLOCK * (x + 1)]
                t = gathered[block, 64 + BLOCK * x : 64 + BLOCK * (x + 1)]
                r = EDGE + 72 + x
                if c > 0:
                    t = t - jnp.where(row == 0, 0.5 * gathered[block - 2, r + 4 : r + 5], 0.0)
                if c < 3:
                    t = t + jnp.where(row == BLOCK - 1, 0.5 * gathered[block + 2, r : r + 1], 0.0)
                if k == 0 and x == 3:
                    t = t + 0.5 * gathered[block + 1, 128:144]
                if k == 1 and x == 0:
                    t = t - 0.5 * gathered[block - 1, 144:160]
                target[4 * k + x, rows] = t
        edge[0, rows] = gathered[2 * c, 128:144]
        edge[1, rows] = gathered[2 * c + 1, 144:160]
    one, two = jnp.where(north, 0, 1), jnp.where(north, 0, 2)
    for i in range(7):
        sent[i] = mobile[one + i]
    for i in range(6):
        sent[7 + i] = target[two + i]
    sent[13] = edge[one]


def first_cycle(
    n_chips, place, mobile, target, edge, got, swapped, species,
    mobile_w, target_w, pressure, residual, coarse, sent, rim,
    weights_ref, field,
):
    north, chip = place[0] == 0, bounded(place, 2, n_chips)

    def sides(i):
        a, b = got[i], swapped[i]
        return jnp.where(north, a, b), jnp.where(north, b, a)

    def copy_mobile(i):
        left, right = sides(i.index())
        mobile_w[i.index()] = left
        mobile_w[(i + 15).index()] = right

    loop(0, 7, copy_mobile)

    def copy_block(i):
        mobile_w[(i + 7).index()] = mobile[i.index()]
        target_w[(i + 6).index()] = target[i.index()]

    loop(0, 8, copy_block)

    def copy_target(i):
        left, right = sides((i + 7).index())
        target_w[i.index()] = left
        target_w[(i + 14).index()] = right

    loop(0, 6, copy_target)
    left, right = sides(13)
    target_w[5] = target_w[5] + 0.5 * edge[0]
    target_w[6] = target_w[6] - 0.5 * left
    target_w[13] = target_w[13] + 0.5 * right
    target_w[14] = target_w[14] - 0.5 * edge[1]

    weights = Weights(weights_ref, 1)
    weights.fill(-6, 14, at(mobile_w, -7), at(target_w, -6), inside_of(8 * chip, 8 * n_chips), 1.0)
    first_sweep(weights, field, -6, -6, 14)
    sweep(weights, field, -6, pressure, -5, -5, 13)
    residual_planes(weights, pressure, -5, residual, -2, -2, 6)

    def restrict(i):
        first, second = mobile_w[(2 * i + 1).index()], mobile_w[(2 * i + 2).index()]
        coarse[i.index()] = 0.125 * pair_sum(first + second)

    loop(0, 10, restrict)
    r = jnp.where(north, 4, 0)
    sent[0:64] = packed(residual[r], residual[r + 1], residual[r + 2], residual[r + 3])
    m = jnp.where(north, 6, 0)
    sent[64:128] = packed(coarse[m], coarse[m + 1], coarse[m + 2], coarse[m + 3])
    for s in range(SPECIES):
        sent[128 + BLOCK * s : 144 + BLOCK * s] = species[s, jnp.where(north, 0, 3)]
        rim[BLOCK * s : BLOCK * (s + 1)] = species[s, jnp.where(north, 3, 0)]


def coarse_sweeps(weights, one, two, low, high, origin):
    first_sweep(weights, one, origin, low, high)
    sweep(weights, one, origin, two, origin, low + 1, high - 1)
    sweep(weights, two, origin, one, origin, low + 2, high - 2)
    sweep(weights, one, origin, two, origin, low + 3, high - 3)


def second_cycle(
    n_chips, place, mobile_w, target_w, pressure, residual, coarse, got, swapped,
    pressure_new, residual_new, coarse_w, sent, sent_far,
    weights_ref, coarse_ref, residual_w, one, two, field, other,
):
    north, chip = place[0] == 0, bounded(place, 2, n_chips)

    def sides(low):
        a, b = got[low : low + 64], swapped[low : low + 64]
        return unpacked(jnp.where(north, a, b)), unpacked(jnp.where(north, b, a))

    left, right = sides(0)
    for i in range(4):
        residual_w[i] = left[i]
        residual_w[12 + i] = right[i]
    left, right = sides(64)
    for i in range(4):
        coarse_w[i] = left[i]
        coarse_w[14 + i] = right[i]

    def copy_residual(i):
        residual_w[(i + 4).index()] = residual[i.index()]

    def copy_coarse(i):
        coarse_w[(i + 4).index()] = coarse[i.index()]

    loop(0, 8, copy_residual)
    loop(0, 10, copy_coarse)

    coarse_weights = Weights(coarse_ref, 2)
    coarse_weights.fill(
        -6, 10, at(coarse_w, -7), at(residual_w, -6), inside_of(4 * chip, 4 * n_chips), 4.0
    )
    coarse_sweeps(coarse_weights, one, two, -6, 10, -6)

    def prolong(i):
        correction = two[(i + 3).index()]
        for half in range(2):
            k = (2 * i + half).index()
            field[k] = field[k] + correction

    def copy_pressure(i):
        field[(i + 1).index()] = pressure[i.index()]

    field[0] = jnp.zeros(PLANE, jnp.float32)
    field[19] = jnp.zeros(PLANE, jnp.float32)
    loop(0, 18, copy_pressure)
    loop(0, 10, prolong)

    weights = Weights(weights_ref, 1)
    weights.fill(-4, 12, at(mobile_w, -7), at(target_w, -6), inside_of(8 * chip, 8 * n_chips), 1.0)
    sweep(weights, field, -6, other, -6, -4, 12)
    sweep(weights, other, -6, field, -6, -3, 11)
    sweep(weights, field, -6, other, -6, -2, 10)
    sweep(weights, other, -6, pressure_new, -1, -1, 9)
    residual_planes(weights, pressure_new, -1, residual_new, 0, 0, 4)
    for i in range(3):
        sent[i] = pressure_new[jnp.where(north, 2, 5) + i]
    sent[3] = packed(residual_new[0], residual_new[1], residual_new[2], residual_new[3])
    sent_far[...] = residual_new[jnp.where(north, 0, 3)]


def finish(
    n_chips, place, mobile_w, target_w, pressure, residual, coarse_w, got, far, swapped,
    gathered, velocity, species, near_rims, swapped_rims,
    velocity_out, pressure_out, species_out,
    weights_ref, coarse_ref, residual_w, pressure_w, one, two, field, other, mobile_pad, final_pad,
):
    north, cross, chip = place[0] == 0, bounded(place, 1, 4), bounded(place, 2, n_chips)
    core = jnp.where(north, 0, 1)
    a, b = got[3], swapped[...]
    left, right = unpacked(jnp.where(north, a, b)), unpacked(jnp.where(north, b, a))
    for i in range(4):
        residual_w[1 + i] = left[i]
        residual_w[5 + i] = residual[i]
        residual_w[9 + i] = right[i]
    residual_w[0] = far[...]
    residual_w[13] = far[...]
    for i in range(3):
        pressure_w[i] = got[i]
        pressure_w[13 + i] = got[i]

    def copy_pressure(i):
        pressure_w[(i + 3).index()] = pressure[i.index()]

    loop(0, 10, copy_pressure)

    shift, coarse_shift = jnp.where(north, 0, 4), jnp.where(north, 0, 2)
    coarse_weights = Weights(coarse_ref, 2)
    coarse_weights.fill(
        -5,
        7,
        lambda i: coarse_w[(i + 7).index(coarse_shift)],
        lambda i: residual_w[(i + 5).index(coarse_shift)],
        inside_of(4 * chip + coarse_shift, 4 * n_chips),
        4.0,
    )
    coarse_sweeps(coarse_weights, one, two, -5, 7, -5)

    def prolong(i):
        correction = two[(i + 3).index()]
        for half in range(2):
            k = 2 * i + half
            field[k.index()] = pressure_w[k.index(shift)] + correction

    loop(0, 6, prolong)

    def mobile(i):
        return mobile_w[(i + 7).index(shift)]

    weights = Weights(weights_ref, 1)
    weights.fill(
        -3,
        7,
        mobile,
        lambda i: target_w[(i + 6).index(shift)],
        inside_of(8 * chip + shift, 8 * n_chips),
        1.0,
    )
    sweep(weights, field, -4, other, -4, -3, 7)

    nothing = jnp.zeros((8, LANES), jnp.float32)

    def last(i):
        p, change = weights.change(at(other, -4), i)
        k = (i + 2).index()
        final_pad[k, 0:8] = nothing
        final_pad[k, 8:72] = p + change
        final_pad[k, 72:80] = nothing

    loop(-2, 6, last)

    def pad_mobile(i):
        k = i.index()
        mobile_pad[k, 0:8] = nothing
        mobile_pad[k, 8:72] = mobile(i)
        mobile_pad[k, 72:80] = nothing

    loop(0, 4, pad_mobile)

    start = pl.multiple_of(cross * BLOCK, BLOCK)
    own = pl.ds(start + 8, BLOCK)
    own_in = pl.ds(start, BLOCK)
    row, lane = rows_of((BLOCK, LANES)), lanes_of((BLOCK, LANES))

    partner = gathered[2 * cross + jnp.where(north, 1, 0)]
    beside = jnp.where(north, partner[128:144], partner[144:160])

    outer = near_rims[SPECIES * BLOCK : (SPECIES + 1) * BLOCK]
    u_low = jnp.where(north, outer, beside)
    u_high = jnp.where(north, beside, outer)

    def u_out(x):
        if x < 0:
            u = u_low
        elif x > 3:
            u = u_high
        else:
            u = velocity[0, x]
        slope = 0.5 * (final_pad[x + 3, own] - final_pad[x + 1, own])
        return u - mobile_w[x + 7 + shift, own_in] * slope

    u = [u_out(x) for x in range(-1, 5)]
    below = gathered[2 * jnp.maximum(cross - 1, 0) + core, EDGE:240]
    above = gathered[2 * jnp.minimum(cross + 1, 3) + core, EDGE:240]
    has_below = jnp.where(cross > 0, 1.0, 0.0)
    has_above = jnp.where(cross < 3, 1.0, 0.0)
    wide = pl.ds(start, 32)
    for x in range(4):
        p = final_pad[x + 2, wide]
        m = mobile_pad[x, wide]
        p_own = p[8:24]
        v = velocity[1, x] - m[8:24] * (0.5 * (p[9:25] - p[7:23]))
        v_low = has_below * below[76 + x : 77 + x] - m[7:8] * (0.5 * (p[8:9] - p[6:7]))
        v_high = has_above * above[72 + x : 73 + x] - m[24:25] * (0.5 * (p[25:26] - p[23:24]))
        p_zp = jnp.where(lane < LANES - 1, roll_lanes(p_own, -1), 0.0)
        p_zm = jnp.where(lane > 0, roll_lanes(p_own, 1), 0.0)
        w = velocity[2, x] - m[8:24] * (0.5 * (p_zp - p_zm))
        velocity_out[0, x] = u[x + 1]
        velocity_out[1, x] = v
        velocity_out[2, x] = w
        pressure_out[x] = p_own

        flow_xm, flow_xp = 0.5 * (u[x] + u[x + 1]), 0.5 * (u[x + 1] + u[x + 2])
        v_m = jnp.where(row == 0, v_low, roll_rows(v, 1))
        v_p = jnp.where(row == BLOCK - 1, v_high, roll_rows(v, -1))
        flow_ym, flow_yp = 0.5 * (v_m + v), 0.5 * (v + v_p)
        w_m = jnp.where(lane > 0, roll_lanes(w, 1), 0.0)
        w_p = jnp.where(lane < LANES - 1, roll_lanes(w, -1), 0.0)
        flow_zm, flow_zp = 0.5 * (w_m + w), 0.5 * (w + w_p)

        def leaves(high, low):
            return jnp.maximum(high, 0.0) - jnp.minimum(low, 0.0)

        keep = 1.0 - time_step * (
            leaves(flow_xp, flow_xm) + leaves(flow_yp, flow_ym) + leaves(flow_zp, flow_zm)
        )
        from_xm, from_xp = (
            time_step * jnp.maximum(flow_xm, 0.0),
            -time_step * jnp.minimum(flow_xp, 0.0),
        )
        from_ym, from_yp = (
            time_step * jnp.maximum(flow_ym, 0.0),
            -time_step * jnp.minimum(flow_yp, 0.0),
        )
        from_zm = jnp.where(lane > 0, time_step * jnp.maximum(flow_zm, 0.0), 0.0)
        from_zp = jnp.where(lane < LANES - 1, -time_step * jnp.minimum(flow_zp, 0.0), 0.0)
        for s in range(SPECIES):
            c = species[s, x]
            rim = slice(BLOCK * s, BLOCK * (s + 1))
            if x > 0:
                c_xm = species[s, x - 1]
            else:
                c_xm = jnp.where(north, near_rims[rim], swapped_rims[rim])
            if x < 3:
                c_xp = species[s, x + 1]
            else:
                c_xp = jnp.where(north, swapped_rims[rim], near_rims[rim])
            r = 4 * s + x
            c_ym = jnp.where(row == 0, has_below * below[36 + r : 37 + r], roll_rows(c, 1))
            c_yp = jnp.where(row == BLOCK - 1, has_above * above[r : r + 1], roll_rows(c, -1))
            total = keep * c + (from_xm * c_xm + from_xp * c_xp)
            total = total + (from_ym * c_ym + from_yp * c_yp)
            total = total + (from_zm * roll_lanes(c, 1) + from_zp * roll_lanes(c, -1))
            species_out[s, x] = total


def call(kernel, outs, scratch, *operands, scalars=True, flops=1000000):
    specs = [pl.BlockSpec(memory_space=pltpu.VMEM) for _ in operands]
    if scalars:
        specs[0] = pl.BlockSpec(memory_space=pltpu.SMEM)
    single = len(outs) == 1
    shapes = [jax.ShapeDtypeStruct(shape, jnp.float32) for shape in outs]
    return pl.pallas_call(
        kernel,
        out_shape=shapes[0] if single else shapes,
        in_specs=specs,
        out_specs=pl.BlockSpec(memory_space=pltpu.VMEM)
        if single
        else [pl.BlockSpec(memory_space=pltpu.VMEM) for _ in outs],
        scratch_shapes=[pltpu.VMEM(shape, jnp.float32) for shape in scratch],
        cost_estimate=pl.CostEstimate(flops=flops, bytes_accessed=1000000, transcendentals=0),
        interpret=INTERPRET,
    )(*operands)


def local(n_chips, velocity, density, source, species):
    slab, cross = lax.axis_index("slab"), lax.axis_index("cross")
    core, chip = slab % 2, slab // 2
    place = jnp.stack([core, cross, chip]).astype(jnp.int32)
    groups = [[(2 * j + k) * 4 + c for c in range(4) for k in range(2)] for j in range(n_chips)]

    def beside(distance):
        pairs = []
        for j in range(n_chips - distance):
            left, right = 2 * j + 1, 2 * (j + distance)
            pairs += [(left, right), (right, left)]
        return pairs

    within = [pair for j in range(n_chips) for pair in ((2 * j, 2 * j + 1), (2 * j + 1, 2 * j))]

    def plane(n):
        return (n, ROWS, LANES)

    own = call(prepare, [(240, LANES)], [], velocity, density, source, species, scalars=False)
    gathered = lax.all_gather(own, ("slab", "cross"), axis_index_groups=groups)
    mobile, target, edge, sent = call(
        assemble, [plane(8), plane(8), plane(2), plane(14)], [], place, gathered
    )
    got = lax.ppermute(sent, "slab", beside(1))
    swapped = lax.ppermute(got, "slab", within)
    edge_rows = lax.dynamic_slice_in_dim(got[13], cross * BLOCK, BLOCK, 0)
    mobile_w, target_w, pressure, residual, coarse, sent, rim = call(
        functools.partial(first_cycle, n_chips),
        [plane(22), plane(20), plane(18), plane(8), plane(10), (272, LANES), (144, LANES)],
        [(8, *plane(20)), plane(20)],
        place, mobile, target, edge, got, swapped, species,
    )
    got = lax.ppermute(sent, "slab", beside(1))
    swapped = lax.ppermute(jnp.concatenate([got[:128], rim], 0), "slab", within)
    near_rims = jnp.concatenate([got[128:], edge_rows], 0)
    swapped_rims = swapped[128:]
    pressure, residual, coarse_w, sent, sent_far = call(
        functools.partial(second_cycle, n_chips),
        [plane(10), plane(4), plane(18), plane(4), PLANE],
        [(8, *plane(16)), (8, *plane(16)), plane(16), plane(16), plane(16), plane(20), plane(20)],
        place, mobile_w, target_w, pressure, residual, coarse, got, swapped,
    )
    got = lax.ppermute(sent, "slab", beside(1))
    far = lax.ppermute(sent_far, "slab", beside(2))
    swapped = lax.ppermute(got[3], "slab", within)
    return call(
        functools.partial(finish, n_chips),
        [velocity.shape, density.shape, species.shape],
        [
            (8, *plane(10)), (8, *plane(12)), plane(14), plane(16), plane(12), plane(12), plane(12),
            plane(12), (4, 80, LANES), (8, 80, LANES),
        ],
        place, mobile_w, target_w, pressure, residual, coarse_w, got, far, swapped,
        gathered, velocity, species, near_rims, swapped_rims,
    )


def solution(mesh):
    n_chips = mesh.shape["slab"] // 2
    block = P("slab", "cross", None)
    stack = P(None, "slab", "cross", None)
    return jax.shard_map(
        lambda *arrays: tuple(local(n_chips, *arrays)),
        mesh=mesh,
        in_specs=(stack, block, block, stack),
        out_specs=(stack, block, stack),
        check_vma=False,
    )
```

```python
import functools

import jax
import jax.numpy as jnp
from jax import lax
from jax.experimental import pallas as pl
from jax.experimental.pallas import tpu as pltpu
from jax.sharding import PartitionSpec as P

INTERPRET = False
ROWS = 64
LANES = 128
BLOCK = 16
SPECIES = 9
EDGE = 160
damping = 0.8
time_step = 0.25


class Place:
    def __init__(self, counter, constant):
        self.counter = counter
        self.constant = constant

    def __add__(self, other):
        return Place(self.counter, self.constant + other)

    def __sub__(self, other):
        return Place(self.counter, self.constant - other)

    def __rmul__(self, factor):
        return Place(self.counter * factor, self.constant * factor)

    def index(self, shift=None):
        start = self.counter if shift is None else self.counter + shift
        return start + self.constant


def loop(low, high, body):
    count = high - low
    some = next(u for u in (4, 5, 6, 3, 7, 2, 1) if count % u == 0)

    def several(start):
        for u in range(some):
            body(Place(start, low + u))

    def step(i, carry):
        several(i * some)
        return carry

    if count == some:
        several(0)
    else:
        lax.fori_loop(0, count // some, step, 0)


def rows_of(shape):
    return lax.broadcasted_iota(jnp.int32, shape, 0)


def lanes_of(shape):
    return lax.broadcasted_iota(jnp.int32, shape, 1)


PLANE = (ROWS, LANES)


def roll_rows(x, by):
    return pltpu.roll(x, by % x.shape[0], 0)


def roll_lanes(x, by):
    return pltpu.roll(x, by % x.shape[1], 1)


PAD = 8
PADDED = (ROWS + 2 * PAD, LANES)


class Field:
    def __init__(self, ref, low, shift=None):
        self.ref = ref
        self.low = low
        self.shift = shift

    def __call__(self, i, rows=0):
        k = (i - self.low).index(self.shift)
        return self.ref[k, PAD + rows : PAD + rows + ROWS]

    def put(self, i, value):
        self.ref[(i - self.low).index(), PAD : PAD + ROWS] = value


def clear_pads(ref):
    nothing = jnp.zeros((PAD, LANES), jnp.float32)
    for k in range(ref.shape[0]):
        ref[k, 0:PAD] = nothing
        ref[k, PAD + ROWS :] = nothing


class Weights:
    def __init__(self, ref, step):
        self.ref = ref
        self.step = step

    def fill(self, low, high, mobile, target, inside, scale):
        s = self.step
        lane = lanes_of(PLANE)
        z_low, z_high = lane >= s, lane < LANES - s

        def body(i):
            m = mobile(i)
            x_m, x_p = mobile(i - 1), mobile(i + 1)
            y_m, y_p = mobile(i, -s), mobile(i, s)
            z_m = jnp.where(z_low, roll_lanes(m, s), 0.0)
            z_p = jnp.where(z_high, roll_lanes(m, -s), 0.0)
            diagonal = 3.0 * m + 0.5 * ((x_m + x_p) + (y_m + y_p) + (z_m + z_p))
            valid = inside(i)
            scaled = (damping * valid) / (diagonal + (1.0 - valid))
            half = 0.5 * scaled
            k = (i - low).index()
            self.ref[0, k] = (m + x_m) * half
            self.ref[1, k] = (m + x_p) * half
            self.ref[2, k] = (m + y_m) * half
            self.ref[3, k] = (m + y_p) * half
            self.ref[4, k] = jnp.where(z_low, (m + z_m) * half, 0.0)
            self.ref[5, k] = jnp.where(z_high, (m + z_p) * half, 0.0)
            self.ref[6, k] = target(i) * (scaled * scale)
            self.ref[7, k] = diagonal * (1.0 / damping)

        self.low = low
        loop(low, high, body)

    def change(self, field, i):
        s = self.step
        k = (i - self.low).index()
        p = field(i)
        total = self.ref[0, k] * field(i - 1) + self.ref[1, k] * field(i + 1)
        total = total + (self.ref[2, k] * field(i, -s) + self.ref[3, k] * field(i, s))
        total = total + (self.ref[4, k] * roll_lanes(p, s) + self.ref[5, k] * roll_lanes(p, -s))
        return p, (total - self.ref[6, k]) - damping * p


def at(ref, origin, shift=None):
    return lambda i: ref[(i - origin).index(shift)]


def sweep(weights, source, result, low, high):
    def body(i):
        p, change = weights.change(source, i)
        result.put(i, p + change)

    loop(low, high, body)


def first_sweep(weights, result, low, high):
    def body(i):
        result.put(i, -weights.ref[6, (i - weights.low).index()])

    loop(low, high, body)


def pair_sum(q):
    row, lane = rows_of(PLANE), lanes_of(PLANE)
    q = q + jnp.where(lane % 2 == 0, roll_lanes(q, -1), roll_lanes(q, 1))
    return q + jnp.where(row % 2 == 0, roll_rows(q, -1), roll_rows(q, 1))


def packed(a, b, c, d):
    row, lane = rows_of(PLANE), lanes_of(PLANE)
    even = lane % 2 == 0
    return jnp.where(row % 2 == 0, jnp.where(even, a, b), jnp.where(even, c, d))


def unpacked(v):
    row, lane = rows_of(PLANE), lanes_of(PLANE)
    even, upper = lane % 2 == 0, row % 2 == 0
    first = jnp.where(even, v, roll_lanes(v, 1))
    second = jnp.where(even, roll_lanes(v, -1), v)

    def low_row(x):
        return jnp.where(upper, x, roll_rows(x, 1))

    def high_row(x):
        return jnp.where(upper, roll_rows(x, -1), x)

    return low_row(first), low_row(second), high_row(first), high_row(second)


def residual_planes(weights, field, result, result_low, low, high):
    def body(i):
        total = 0.0
        for half in range(2):
            _, change = weights.change(field, 2 * i + half)
            total = total - change * weights.ref[7, (2 * i + half - weights.low).index()]
        result[(i - result_low).index()] = 0.125 * pair_sum(total)

    loop(low, high, body)


def inside_of(first, count):
    def inside(i):
        place = i.index(first)
        return jnp.where((place >= 0) & (place < count), 1.0, 0.0)

    return inside


def whereabouts(n_chips):
    slab, cross = lax.axis_index("slab"), lax.axis_index("cross")
    chip = jnp.minimum(jnp.maximum(slab // 2, 0), n_chips - 1)
    return slab % 2 == 0, jnp.minimum(jnp.maximum(cross, 0), 3), chip


def prepare(velocity, density, source, species, out):
    lane = lanes_of((BLOCK, LANES))
    row = rows_of((BLOCK, LANES))
    for x in range(4):
        out[BLOCK * x : BLOCK * (x + 1)] = 1.0 / density[x]
        u_p = velocity[0, x + 1] if x < 3 else 0.0
        u_m = velocity[0, x - 1] if x > 0 else 0.0
        v, w = velocity[1, x], velocity[2, x]
        v_p = jnp.where(row < BLOCK - 1, roll_rows(v, -1), 0.0)
        v_m = jnp.where(row > 0, roll_rows(v, 1), 0.0)
        w_p = jnp.where(lane < LANES - 1, roll_lanes(w, -1), 0.0)
        w_m = jnp.where(lane > 0, roll_lanes(w, 1), 0.0)
        moved = 0.5 * ((u_p - u_m) + (v_p - v_m) + (w_p - w_m))
        out[64 + BLOCK * x : 64 + BLOCK * (x + 1)] = moved - source[x]
        for s in range(SPECIES):
            r = EDGE + 4 * s + x
            out[r : r + 1] = species[s, x, 0:1]
            out[r + 36 : r + 37] = species[s, x, BLOCK - 1 : BLOCK]
        r = EDGE + 72 + x
        out[r : r + 1] = velocity[1, x, 0:1]
        out[r + 4 : r + 5] = velocity[1, x, BLOCK - 1 : BLOCK]
    out[128:144] = velocity[0, 0]
    out[144:160] = velocity[0, 3]


def assemble(n_chips, gathered, mobile, target, edge, sent):
    north, _, _ = whereabouts(n_chips)
    row = rows_of((BLOCK, LANES))
    for c in range(4):
        rows = slice(BLOCK * c, BLOCK * (c + 1))
        for k in range(2):
            block = 2 * c + k
            for x in range(4):
                mobile[4 * k + x, rows] = gathered[block, BLOCK * x : BLOCK * (x + 1)]
                t = gathered[block, 64 + BLOCK * x : 64 + BLOCK * (x + 1)]
                r = EDGE + 72 + x
                if c > 0:
                    t = t - jnp.where(row == 0, 0.5 * gathered[block - 2, r + 4 : r + 5], 0.0)
                if c < 3:
                    t = t + jnp.where(row == BLOCK - 1, 0.5 * gathered[block + 2, r : r + 1], 0.0)
                if k == 0 and x == 3:
                    t = t + 0.5 * gathered[block + 1, 128:144]
                if k == 1 and x == 0:
                    t = t - 0.5 * gathered[block - 1, 144:160]
                target[4 * k + x, rows] = t
        edge[0, rows] = gathered[2 * c, 128:144]
        edge[1, rows] = gathered[2 * c + 1, 144:160]
    one, two = jnp.where(north, 0, 1), jnp.where(north, 0, 2)
    for i in range(7):
        sent[i] = mobile[one + i]
    for i in range(6):
        sent[7 + i] = target[two + i]
    sent[13] = edge[one]


def first_cycle(
    n_chips, mobile, target, edge, got, swapped, species,
    mobile_ref, target_w, pressure_ref, residual, coarse, outer, sent, rim,
    weights_ref, field_ref,
):
    north, _, chip = whereabouts(n_chips)
    clear_pads(mobile_ref)
    clear_pads(field_ref)
    clear_pads(pressure_ref)
    mobile_w, pressure = Field(mobile_ref, -7), Field(pressure_ref, -6)
    field = Field(field_ref, -6)

    def sides(i):
        a, b = got[i], swapped[i]
        return jnp.where(north, a, b), jnp.where(north, b, a)

    def copy_mobile(i):
        left, right = sides((i + 7).index())
        mobile_w.put(i, left)
        mobile_w.put(i + 15, right)

    loop(-7, 0, copy_mobile)

    def copy_block(i):
        mobile_w.put(i, mobile[i.index()])
        target_w[(i + 6).index()] = target[i.index()]

    loop(0, 8, copy_block)

    def copy_target(i):
        left, right = sides((i + 7).index())
        target_w[i.index()] = left
        target_w[(i + 14).index()] = right

    loop(0, 6, copy_target)
    left, right = sides(13)
    target_w[5] = target_w[5] + 0.5 * edge[0]
    target_w[6] = target_w[6] - 0.5 * left
    target_w[13] = target_w[13] + 0.5 * right
    target_w[14] = target_w[14] - 0.5 * edge[1]
    outer[...] = got[13]

    weights = Weights(weights_ref, 1)
    weights.fill(-6, 14, mobile_w, at(target_w, -6), inside_of(8 * chip, 8 * n_chips), 1.0)
    first_sweep(weights, field, -6, 14)
    sweep(weights, field, pressure, -5, 13)
    residual_planes(weights, pressure, residual, -2, -2, 6)

    def restrict(i):
        pair = mobile_w(2 * i) + mobile_w(2 * i + 1)
        coarse[(i + 3).index()] = 0.125 * pair_sum(pair)

    loop(-3, 7, restrict)
    r = jnp.where(north, 4, 0)
    sent[0:64] = packed(residual[r], residual[r + 1], residual[r + 2], residual[r + 3])
    m = jnp.where(north, 6, 0)
    sent[64:128] = packed(coarse[m], coarse[m + 1], coarse[m + 2], coarse[m + 3])
    near, beside = jnp.where(north, 0, 3), jnp.where(north, 3, 0)
    for s in range(SPECIES):
        sent[128 + BLOCK * s : 144 + BLOCK * s] = species[s, near]
        rim[BLOCK * s : BLOCK * (s + 1)] = species[s, beside]


def coarse_sweeps(weights, one, two, low, high):
    first_sweep(weights, one, low, high)
    sweep(weights, one, two, low + 1, high - 1)
    sweep(weights, two, one, low + 2, high - 2)
    sweep(weights, one, two, low + 3, high - 3)


def second_cycle(
    n_chips, mobile_ref, target_w, pressure_ref, residual, coarse, got, swapped,
    pressure_new_ref, residual_new, coarse_ref, sent, sent_far,
    weights_ref, coarse_weights_ref, residual_w, one_ref, two_ref, field_ref, other_ref,
):
    north, _, chip = whereabouts(n_chips)
    for ref in (pressure_new_ref, coarse_ref, one_ref, two_ref, field_ref, other_ref):
        clear_pads(ref)
    coarse_w, one, two = Field(coarse_ref, -7), Field(one_ref, -6), Field(two_ref, -6)
    field, other = Field(field_ref, -6), Field(other_ref, -6)
    pressure, pressure_new = Field(pressure_ref, -6), Field(pressure_new_ref, -1)

    def sides(low):
        a, b = got[low : low + 64], swapped[low : low + 64]
        return unpacked(jnp.where(north, a, b)), unpacked(jnp.where(north, b, a))

    left, right = sides(0)
    for i in range(4):
        residual_w[i] = left[i]
        residual_w[12 + i] = right[i]
    left, right = sides(64)
    for i in range(4):
        coarse_w.put(Place(0, i - 7), left[i])
        coarse_w.put(Place(0, i + 7), right[i])

    def copy_residual(i):
        residual_w[(i + 4).index()] = residual[i.index()]

    def copy_coarse(i):
        coarse_w.put(i - 3, coarse[i.index()])

    loop(0, 8, copy_residual)
    loop(0, 10, copy_coarse)

    coarse_weights = Weights(coarse_weights_ref, 2)
    coarse_weights.fill(
        -6, 10, coarse_w, at(residual_w, -6), inside_of(4 * chip, 4 * n_chips), 4.0
    )
    coarse_sweeps(coarse_weights, one, two, -6, 10)

    def prolong(i):
        correction = two(i)
        for half in range(2):
            k = 2 * i + half
            field.put(k, pressure(k) + correction)

    loop(-3, 7, prolong)

    weights = Weights(weights_ref, 1)
    weights.fill(
        -4, 12, Field(mobile_ref, -7), at(target_w, -6), inside_of(8 * chip, 8 * n_chips), 1.0
    )
    sweep(weights, field, other, -4, 12)
    sweep(weights, other, field, -3, 11)
    sweep(weights, field, other, -2, 10)
    sweep(weights, other, pressure_new, -1, 9)
    residual_planes(weights, pressure_new, residual_new, 0, 0, 4)
    first = jnp.where(north, 2, 5)
    for i in range(3):
        sent[i] = pressure_new_ref[first + i, PAD : PAD + ROWS]
    sent[3] = packed(residual_new[0], residual_new[1], residual_new[2], residual_new[3])
    sent_far[...] = residual_new[jnp.where(north, 0, 3)]


def finish(
    n_chips, mobile_ref, target_w, pressure, residual, coarse_ref, got, far, swapped,
    gathered, velocity, species, outer, near_rims, swapped_rims,
    velocity_out, pressure_out, species_out,
    weights_ref, coarse_weights_ref, residual_w, pressure_w, one_ref, two_ref, field_ref,
    other_ref, final_pad,
):
    north, cross, chip = whereabouts(n_chips)
    core = jnp.where(north, 0, 1)
    for ref in (one_ref, two_ref, field_ref, other_ref, final_pad):
        clear_pads(ref)
    one, two = Field(one_ref, -5), Field(two_ref, -5)
    field, other, final = Field(field_ref, -4), Field(other_ref, -4), Field(final_pad, -2)
    a, b = got[3], swapped[3]
    left, right = unpacked(jnp.where(north, a, b)), unpacked(jnp.where(north, b, a))
    for i in range(4):
        residual_w[1 + i] = left[i]
        residual_w[5 + i] = residual[i]
        residual_w[9 + i] = right[i]
    residual_w[0] = far[...]
    residual_w[13] = far[...]
    for i in range(3):
        pressure_w[i] = got[i]
        pressure_w[13 + i] = got[i]
    known = Field(pressure, -1)

    def copy_pressure(i):
        pressure_w[(i + 4).index()] = known(i)

    loop(-1, 9, copy_pressure)

    shift, coarse_shift = jnp.where(north, 0, 4), jnp.where(north, 0, 2)
    coarse_weights = Weights(coarse_weights_ref, 2)
    coarse_weights.fill(
        -5,
        7,
        Field(coarse_ref, -7, coarse_shift),
        at(residual_w, -5, coarse_shift),
        inside_of(4 * chip + coarse_shift, 4 * n_chips),
        4.0,
    )
    coarse_sweeps(coarse_weights, one, two, -5, 7)

    def prolong(i):
        correction = two(i)
        for half in range(2):
            k = 2 * i + half
            field.put(k, pressure_w[(k + 4).index(shift)] + correction)

    loop(-2, 4, prolong)

    weights = Weights(weights_ref, 1)
    weights.fill(
        -3,
        7,
        Field(mobile_ref, -7, shift),
        at(target_w, -6, shift),
        inside_of(8 * chip + shift, 8 * n_chips),
        1.0,
    )
    sweep(weights, field, other, -3, 7)
    sweep(weights, other, final, -2, 6)

    start = pl.multiple_of(cross * BLOCK, BLOCK)
    own = pl.ds(start + 8, BLOCK)
    row, lane = rows_of((BLOCK, LANES)), lanes_of((BLOCK, LANES))

    partner = gathered[2 * cross + jnp.where(north, 1, 0)]
    beside = jnp.where(north, partner[128:144], partner[144:160])

    beyond = outer[pl.ds(start, BLOCK)]
    u_low = jnp.where(north, beyond, beside)
    u_high = jnp.where(north, beside, beyond)

    def u_out(x):
        if x < 0:
            u = u_low
        elif x > 3:
            u = u_high
        else:
            u = velocity[0, x]
        slope = 0.5 * (final_pad[x + 3, own] - final_pad[x + 1, own])
        return u - mobile_ref[shift + (x + 7), own] * slope

    u = [u_out(x) for x in range(-1, 5)]
    below = gathered[2 * jnp.maximum(cross - 1, 0) + core, EDGE:240]
    above = gathered[2 * jnp.minimum(cross + 1, 3) + core, EDGE:240]
    has_below = jnp.where(cross > 0, 1.0, 0.0)
    has_above = jnp.where(cross < 3, 1.0, 0.0)
    wide = pl.ds(start, 32)
    for x in range(4):
        p = final_pad[x + 2, wide]
        m = mobile_ref[shift + (x + 7), wide]
        p_own = p[8:24]
        v = velocity[1, x] - m[8:24] * (0.5 * (p[9:25] - p[7:23]))
        v_low = has_below * below[76 + x : 77 + x] - m[7:8] * (0.5 * (p[8:9] - p[6:7]))
        v_high = has_above * above[72 + x : 73 + x] - m[24:25] * (0.5 * (p[25:26] - p[23:24]))
        p_zp = jnp.where(lane < LANES - 1, roll_lanes(p_own, -1), 0.0)
        p_zm = jnp.where(lane > 0, roll_lanes(p_own, 1), 0.0)
        w = velocity[2, x] - m[8:24] * (0.5 * (p_zp - p_zm))
        velocity_out[0, x] = u[x + 1]
        velocity_out[1, x] = v
        velocity_out[2, x] = w
        pressure_out[x] = p_own

        flow_xm, flow_xp = 0.5 * (u[x] + u[x + 1]), 0.5 * (u[x + 1] + u[x + 2])
        v_m = jnp.where(row == 0, v_low, roll_rows(v, 1))
        v_p = jnp.where(row == BLOCK - 1, v_high, roll_rows(v, -1))
        flow_ym, flow_yp = 0.5 * (v_m + v), 0.5 * (v + v_p)
        w_m = jnp.where(lane > 0, roll_lanes(w, 1), 0.0)
        w_p = jnp.where(lane < LANES - 1, roll_lanes(w, -1), 0.0)
        flow_zm, flow_zp = 0.5 * (w_m + w), 0.5 * (w + w_p)

        def leaves(high, low):
            return jnp.maximum(high, 0.0) - jnp.minimum(low, 0.0)

        keep = 1.0 - time_step * (
            leaves(flow_xp, flow_xm) + leaves(flow_yp, flow_ym) + leaves(flow_zp, flow_zm)
        )
        from_xm, from_xp = (
            time_step * jnp.maximum(flow_xm, 0.0),
            -time_step * jnp.minimum(flow_xp, 0.0),
        )
        from_ym, from_yp = (
            time_step * jnp.maximum(flow_ym, 0.0),
            -time_step * jnp.minimum(flow_yp, 0.0),
        )
        from_zm = jnp.where(lane > 0, time_step * jnp.maximum(flow_zm, 0.0), 0.0)
        from_zp = jnp.where(lane < LANES - 1, -time_step * jnp.minimum(flow_zp, 0.0), 0.0)
        for s in range(SPECIES):
            c = species[s, x]
            rim = slice(128 + BLOCK * s, 144 + BLOCK * s)
            if x > 0:
                c_xm = species[s, x - 1]
            else:
                c_xm = jnp.where(north, near_rims[rim], swapped_rims[rim])
            if x < 3:
                c_xp = species[s, x + 1]
            else:
                c_xp = jnp.where(north, swapped_rims[rim], near_rims[rim])
            r = 4 * s + x
            c_ym = jnp.where(row == 0, has_below * below[36 + r : 37 + r], roll_rows(c, 1))
            c_yp = jnp.where(row == BLOCK - 1, has_above * above[r : r + 1], roll_rows(c, -1))
            total = keep * c + (from_xm * c_xm + from_xp * c_xp)
            total = total + (from_ym * c_ym + from_yp * c_yp)
            total = total + (from_zm * roll_lanes(c, 1) + from_zp * roll_lanes(c, -1))
            species_out[s, x] = total


def call(kernel, outs, scratch, *operands):
    vmem = pl.BlockSpec(memory_space=pltpu.VMEM)
    shapes = [jax.ShapeDtypeStruct(shape, jnp.float32) for shape in outs]
    return pl.pallas_call(
        kernel,
        out_shape=shapes,
        in_specs=[vmem for _ in operands],
        out_specs=[vmem for _ in outs],
        scratch_shapes=[pltpu.VMEM(shape, jnp.float32) for shape in scratch],
        cost_estimate=pl.CostEstimate(flops=1000000, bytes_accessed=1000000, transcendentals=0),
        compiler_params=pltpu.CompilerParams(vmem_limit_bytes=24 * 2**20),
        interpret=INTERPRET,
    )(*operands)


def local(n_chips, velocity, density, source, species):
    groups = [[(2 * j + k) * 4 + c for c in range(4) for k in range(2)] for j in range(n_chips)]

    def beside(distance):
        pairs = []
        for j in range(n_chips - distance):
            left, right = 2 * j + 1, 2 * (j + distance)
            pairs += [(left, right), (right, left)]
        return pairs

    within = [pair for j in range(n_chips) for pair in ((2 * j, 2 * j + 1), (2 * j + 1, 2 * j))]

    def plane(n):
        return (n, ROWS, LANES)

    def padded(n):
        return (n, *PADDED)

    def bind(kernel):
        return functools.partial(kernel, n_chips)

    (own,) = call(prepare, [(240, LANES)], [], velocity, density, source, species)
    gathered = lax.all_gather(own, ("slab", "cross"), axis_index_groups=groups)
    mobile, target, edge, sent = call(
        bind(assemble), [plane(8), plane(8), plane(2), plane(14)], [], gathered
    )
    got = lax.ppermute(sent, "slab", beside(1))
    swapped = lax.ppermute(got, "slab", within)
    mobile_w, target_w, pressure, residual, coarse, outer, sent, rim = call(
        bind(first_cycle),
        [
            padded(22), plane(20), padded(20), plane(8), plane(10), PLANE, (272, LANES),
            (144, LANES),
        ],
        [(8, *plane(20)), padded(20)],
        mobile, target, edge, got, swapped, species,
    )
    near = lax.ppermute(sent, "slab", beside(1))
    far_side = lax.ppermute(jnp.concatenate([near[:128], rim], 0), "slab", within)
    pressure, residual, coarse_w, sent, sent_far = call(
        bind(second_cycle),
        [padded(10), plane(4), padded(18), plane(4), PLANE],
        [
            (8, *plane(16)), (8, *plane(16)), plane(16), padded(16), padded(16), padded(20),
            padded(20),
        ],
        mobile_w, target_w, pressure, residual, coarse, near, far_side,
    )
    got = lax.ppermute(sent, "slab", beside(1))
    far = lax.ppermute(sent_far, "slab", beside(2))
    swapped = lax.ppermute(got, "slab", within)
    return call(
        bind(finish),
        [velocity.shape, density.shape, species.shape],
        [
            (8, *plane(10)), (8, *plane(12)), plane(14), plane(16), padded(12), padded(12),
            padded(12), padded(12), padded(8),
        ],
        mobile_w, target_w, pressure, residual, coarse_w, got, far, swapped,
        gathered, velocity, species, outer, near, far_side,
    )


def solution(mesh):
    n_chips = mesh.shape["slab"] // 2
    block = P("slab", "cross", None)
    stack = P(None, "slab", "cross", None)
    return jax.shard_map(
        lambda *arrays: tuple(local(n_chips, *arrays)),
        mesh=mesh,
        in_specs=(stack, block, block, stack),
        out_specs=(stack, block, stack),
        check_vma=False,
    )
```

```python
import functools

import jax
import jax.numpy as jnp
from jax import lax
from jax.experimental import pallas as pl
from jax.experimental.pallas import tpu as pltpu
from jax.sharding import PartitionSpec as P


INTERPRET = False
HBM = pltpu.HBM
ROWS = 64
LANES = 128
BLOCK = 16
SPECIES = 9
EDGE = 160
OWN = EDGE + 8
damping = 0.8
time_step = 0.25


class Place:
    def __init__(self, counter, constant):
        self.counter = counter
        self.constant = constant

    def __add__(self, other):
        return Place(self.counter, self.constant + other)

    def __sub__(self, other):
        return Place(self.counter, self.constant - other)

    def __rmul__(self, factor):
        return Place(self.counter * factor, self.constant * factor)

    def index(self, shift=None):
        start = self.counter if shift is None else self.counter + shift
        return start + self.constant


def loop(low, high, body):
    count = high - low
    some = next(u for u in (4, 5, 6, 3, 7, 2, 1) if count % u == 0)

    def several(start):
        for u in range(some):
            body(Place(start, low + u))

    def step(i, carry):
        several(i * some)
        return carry

    if count == some:
        several(0)
    else:
        lax.fori_loop(0, count // some, step, 0)


def rows_of(shape):
    return lax.broadcasted_iota(jnp.int32, shape, 0)


def lanes_of(shape):
    return lax.broadcasted_iota(jnp.int32, shape, 1)


PLANE = (ROWS, LANES)


def roll_rows(x, by):
    return pltpu.roll(x, by % x.shape[0], 0)


def roll_lanes(x, by):
    return pltpu.roll(x, by % x.shape[1], 1)


PAD = 8
PADDED = (ROWS + 2 * PAD, LANES)


class Field:
    def __init__(self, ref, low, shift=None):
        self.ref = ref
        self.low = low
        self.shift = shift

    def __call__(self, i, rows=0):
        k = (i - self.low).index(self.shift)
        return self.ref[k, PAD + rows : PAD + rows + ROWS]

    def put(self, i, value):
        self.ref[(i - self.low).index(), PAD : PAD + ROWS] = value


def clear_pads(ref):
    nothing = jnp.zeros((PAD, LANES), jnp.float32)
    for k in range(ref.shape[0]):
        ref[k, 0:PAD] = nothing
        ref[k, PAD + ROWS :] = nothing


class Weights:
    def __init__(self, ref, step, low, shift=None, constant=None):
        self.ref = ref
        self.step = step
        self.low = low
        self.shift = shift
        self.constant = constant

    def place(self, i):
        return (i - self.low).index(self.shift)

    def fill(self, low, high, mobile, target, inside):
        s = self.step
        lane = lanes_of(PLANE)
        z_low, z_high = lane >= s, lane < LANES - s

        def body(i):
            m = mobile(i)
            x_m, x_p = mobile(i - 1), mobile(i + 1)
            y_m, y_p = mobile(i, -s), mobile(i, s)
            z_m = jnp.where(z_low, roll_lanes(m, s), 0.0)
            z_p = jnp.where(z_high, roll_lanes(m, -s), 0.0)
            diagonal = 3.0 * m + 0.5 * ((x_m + x_p) + (y_m + y_p) + (z_m + z_p))
            valid = inside(i)
            scaled = (damping * valid) / (diagonal + (1.0 - valid))
            half = 0.5 * scaled
            k = self.place(i)
            self.ref[0, k] = (m + x_m) * half
            self.ref[1, k] = (m + x_p) * half
            self.ref[2, k] = (m + y_m) * half
            self.ref[3, k] = (m + y_p) * half
            self.ref[4, k] = jnp.where(z_low, (m + z_m) * half, 0.0)
            self.ref[5, k] = jnp.where(z_high, (m + z_p) * half, 0.0)
            if s == 1:
                self.ref[6, k] = target(i) * scaled
                self.ref[7, k] = diagonal * (1.0 / damping)
            else:
                self.ref[6, k] = target(i) * (4.0 * scaled)
                self.ref[7, k] = 4.0 * scaled

        loop(low, high, body)

    def side(self, i):
        if self.constant is not None:
            return self.constant(i)
        return self.ref[6, self.place(i)]

    def change(self, field, i):
        s = self.step
        k = self.place(i)
        p = field(i)
        total = self.ref[0, k] * field(i - 1) + self.ref[1, k] * field(i + 1)
        total = total + (self.ref[2, k] * field(i, -s) + self.ref[3, k] * field(i, s))
        total = total + (self.ref[4, k] * roll_lanes(p, s) + self.ref[5, k] * roll_lanes(p, -s))
        return p, (total - self.side(i)) - damping * p


def at(ref, origin, shift=None):
    return lambda i: ref[(i - origin).index(shift)]


def sweep(weights, source, result, low, high):
    def body(i):
        p, change = weights.change(source, i)
        result.put(i, p + change)

    loop(low, high, body)


def first_sweep(weights, result, low, high):
    def body(i):
        result.put(i, -weights.side(i))

    loop(low, high, body)


def pair_sum(q):
    row, lane = rows_of(PLANE), lanes_of(PLANE)
    q = q + jnp.where(lane % 2 == 0, roll_lanes(q, -1), roll_lanes(q, 1))
    return q + jnp.where(row % 2 == 0, roll_rows(q, -1), roll_rows(q, 1))


def packed(a, b, c, d):
    row, lane = rows_of(PLANE), lanes_of(PLANE)
    even = lane % 2 == 0
    return jnp.where(row % 2 == 0, jnp.where(even, a, b), jnp.where(even, c, d))


def unpacked(v):
    row, lane = rows_of(PLANE), lanes_of(PLANE)
    even, upper = lane % 2 == 0, row % 2 == 0
    first = jnp.where(even, v, roll_lanes(v, 1))
    second = jnp.where(even, roll_lanes(v, -1), v)

    def low_row(x):
        return jnp.where(upper, x, roll_rows(x, 1))

    def high_row(x):
        return jnp.where(upper, roll_rows(x, -1), x)

    return low_row(first), low_row(second), high_row(first), high_row(second)


def residual_planes(weights, field, result, result_low, low, high):
    def body(i):
        total = 0.0
        for half in range(2):
            _, change = weights.change(field, 2 * i + half)
            total = total - change * weights.ref[7, weights.place(2 * i + half)]
        result[(i - result_low).index()] = 0.125 * pair_sum(total)

    loop(low, high, body)


def inside_of(first, count):
    def inside(i):
        place = i.index(first)
        return jnp.where((place >= 0) & (place < count), 1.0, 0.0)

    return inside


def whereabouts(n_chips):
    slab, cross = lax.axis_index("slab"), lax.axis_index("cross")
    chip = jnp.minimum(jnp.maximum(slab // 2, 0), n_chips - 1)
    return slab % 2 == 0, jnp.minimum(jnp.maximum(cross, 0), 3), chip


def prepare(velocity_in, density_in, source_in, out, velocity, density, source, semaphore):
    copies = [
        pltpu.make_async_copy(there, here, semaphore.at[k])
        for k, (there, here) in enumerate(
            [(density_in, density), (velocity_in, velocity), (source_in, source)]
        )
    ]
    for copy in copies:
        copy.start()
    lane = lanes_of((BLOCK, LANES))
    row = rows_of((BLOCK, LANES))
    copies[0].wait()
    for x in range(4):
        out[BLOCK * x : BLOCK * (x + 1)] = 1.0 / density[x]
    copies[1].wait()
    copies[2].wait()
    for x in range(4):
        u_p = velocity[0, x + 1] if x < 3 else 0.0
        u_m = velocity[0, x - 1] if x > 0 else 0.0
        v, w = velocity[1, x], velocity[2, x]
        v_p = jnp.where(row < BLOCK - 1, roll_rows(v, -1), 0.0)
        v_m = jnp.where(row > 0, roll_rows(v, 1), 0.0)
        w_p = jnp.where(lane < LANES - 1, roll_lanes(w, -1), 0.0)
        w_m = jnp.where(lane > 0, roll_lanes(w, 1), 0.0)
        moved = 0.5 * ((u_p - u_m) + (v_p - v_m) + (w_p - w_m))
        out[64 + BLOCK * x : 64 + BLOCK * (x + 1)] = moved - source[x]
        r = EDGE + x
        out[r : r + 1] = velocity[1, x, 0:1]
        out[r + 4 : r + 5] = velocity[1, x, BLOCK - 1 : BLOCK]
    out[128:144] = velocity[0, 0]
    out[144:160] = velocity[0, 3]


def assemble(n_chips, gathered, mobile, target, edge, sent):
    north, _, _ = whereabouts(n_chips)
    row = rows_of((BLOCK, LANES))
    for c in range(4):
        rows = slice(BLOCK * c, BLOCK * (c + 1))
        for k in range(2):
            block = 2 * c + k
            for x in range(4):
                mobile[4 * k + x, rows] = gathered[block, BLOCK * x : BLOCK * (x + 1)]
                t = gathered[block, 64 + BLOCK * x : 64 + BLOCK * (x + 1)]
                r = EDGE + x
                if c > 0:
                    t = t - jnp.where(row == 0, 0.5 * gathered[block - 2, r + 4 : r + 5], 0.0)
                if c < 3:
                    t = t + jnp.where(row == BLOCK - 1, 0.5 * gathered[block + 2, r : r + 1], 0.0)
                if k == 0 and x == 3:
                    t = t + 0.5 * gathered[block + 1, 128:144]
                if k == 1 and x == 0:
                    t = t - 0.5 * gathered[block - 1, 144:160]
                target[4 * k + x, rows] = t
        edge[0, rows] = gathered[2 * c, 128:144]
        edge[1, rows] = gathered[2 * c + 1, 144:160]
    one, two = jnp.where(north, 0, 1), jnp.where(north, 0, 2)
    for i in range(7):
        sent[i] = mobile[one + i]
    for i in range(6):
        sent[7 + i] = target[two + i]
    sent[13] = edge[one]


def first_cycle(
    n_chips, mobile, target, edge, got, swapped, species,
    mobile_ref, weights_ref, pressure_ref, residual, coarse, outer, sent, rim, edge_low, edge_high,
    target_w, field_ref,
):
    north, _, chip = whereabouts(n_chips)
    clear_pads(mobile_ref)
    clear_pads(field_ref)
    clear_pads(pressure_ref)
    mobile_w, pressure = Field(mobile_ref, -7), Field(pressure_ref, -6)
    field = Field(field_ref, -6)

    def sides(i):
        a, b = got[i], swapped[i]
        return jnp.where(north, a, b), jnp.where(north, b, a)

    def copy_mobile(i):
        left, right = sides((i + 7).index())
        mobile_w.put(i, left)
        mobile_w.put(i + 15, right)

    loop(-7, 0, copy_mobile)

    def copy_block(i):
        mobile_w.put(i, mobile[i.index()])
        target_w[(i + 6).index()] = target[i.index()]

    loop(0, 8, copy_block)

    def copy_target(i):
        left, right = sides((i + 7).index())
        target_w[i.index()] = left
        target_w[(i + 14).index()] = right

    loop(0, 6, copy_target)
    left, right = sides(13)
    target_w[5] = target_w[5] + 0.5 * edge[0]
    target_w[6] = target_w[6] - 0.5 * left
    target_w[13] = target_w[13] + 0.5 * right
    target_w[14] = target_w[14] - 0.5 * edge[1]
    outer[...] = got[13]

    weights = Weights(weights_ref, 1, -6)
    weights.fill(-6, 14, mobile_w, at(target_w, -6), inside_of(8 * chip, 8 * n_chips))
    first_sweep(weights, field, -6, 14)
    sweep(weights, field, pressure, -5, 13)
    residual_planes(weights, pressure, residual, -2, -2, 6)

    def restrict(i):
        pair = mobile_w(2 * i) + mobile_w(2 * i + 1)
        coarse[(i + 3).index()] = 0.125 * pair_sum(pair)

    loop(-3, 7, restrict)
    r = jnp.where(north, 4, 0)
    sent[0:64] = packed(residual[r], residual[r + 1], residual[r + 2], residual[r + 3])
    m = jnp.where(north, 6, 0)
    sent[64:128] = packed(coarse[m], coarse[m + 1], coarse[m + 2], coarse[m + 3])
    near, beside = jnp.where(north, 0, 3), jnp.where(north, 3, 0)
    for s in range(SPECIES):
        sent[128 + BLOCK * s : 144 + BLOCK * s] = species[s, near]
        rim[BLOCK * s : BLOCK * (s + 1)] = species[s, beside]
        for x in range(4):
            r = 4 * s + x
            edge_low[r : r + 1] = species[s, x, 0:1]
            edge_high[r : r + 1] = species[s, x, BLOCK - 1 : BLOCK]
    edge_low[36:40] = jnp.zeros((4, LANES), jnp.float32)
    edge_high[36:40] = jnp.zeros((4, LANES), jnp.float32)


def flow_rims(n_chips, gathered, outer, u_rims, v_rims):
    north, cross, _ = whereabouts(n_chips)
    core = jnp.where(north, 0, 1)
    start = pl.multiple_of(cross * BLOCK, BLOCK)
    partner = 2 * cross + jnp.where(north, 1, 0)
    first, last = gathered[partner, 128:144], gathered[partner, 144:160]
    beyond = outer[pl.ds(start, BLOCK)]
    u_rims[0] = jnp.where(north, beyond, last)
    u_rims[1] = jnp.where(north, first, beyond)
    below = gathered[2 * jnp.maximum(cross - 1, 0) + core, EDGE:OWN]
    above = gathered[2 * jnp.minimum(cross + 1, 3) + core, EDGE:OWN]
    v_rims[0:4] = jnp.where(cross > 0, below[4:8], 0.0)
    v_rims[4:8] = jnp.where(cross < 3, above[0:4], 0.0)


def species_rims(n_chips, near, beside, rims):
    north, _, _ = whereabouts(n_chips)
    a, b = near[128:272], beside[128:272]
    rims[0] = jnp.where(north, a, b)
    rims[1] = jnp.where(north, b, a)


def coarse_sweeps(weights, one, two, low, high):
    first_sweep(weights, one, low, high)
    sweep(weights, one, two, low + 1, high - 1)
    sweep(weights, two, one, low + 2, high - 2)
    sweep(weights, one, two, low + 3, high - 3)


def second_cycle(
    n_chips, weights_ref, pressure_ref, residual, coarse, got, swapped,
    pressure_new_ref, residual_new, coarse_weights_ref, sent, sent_far,
    coarse_ref, residual_w, one_ref, two_ref, field_ref, other_ref,
):
    north, _, chip = whereabouts(n_chips)
    for ref in (pressure_new_ref, coarse_ref, one_ref, two_ref, field_ref, other_ref):
        clear_pads(ref)
    coarse_w, one, two = Field(coarse_ref, -7), Field(one_ref, -6), Field(two_ref, -6)
    field, other = Field(field_ref, -6), Field(other_ref, -6)
    pressure, pressure_new = Field(pressure_ref, -6), Field(pressure_new_ref, -1)

    def sides(low):
        a, b = got[low : low + 64], swapped[low : low + 64]
        return unpacked(jnp.where(north, a, b)), unpacked(jnp.where(north, b, a))

    left, right = sides(0)
    for i in range(4):
        residual_w[i] = left[i]
        residual_w[12 + i] = right[i]
    left, right = sides(64)
    for i in range(4):
        coarse_w.put(Place(0, i - 7), left[i])
        coarse_w.put(Place(0, i + 7), right[i])

    def copy_residual(i):
        residual_w[(i + 4).index()] = residual[i.index()]

    def copy_coarse(i):
        coarse_w.put(i - 3, coarse[i.index()])

    loop(0, 8, copy_residual)
    loop(0, 10, copy_coarse)

    coarse_weights = Weights(coarse_weights_ref, 2, -6)
    coarse_weights.fill(-6, 10, coarse_w, at(residual_w, -6), inside_of(4 * chip, 4 * n_chips))
    coarse_sweeps(coarse_weights, one, two, -6, 10)

    def prolong(i):
        correction = two(i)
        for half in range(2):
            k = 2 * i + half
            field.put(k, pressure(k) + correction)

    loop(-3, 7, prolong)

    weights = Weights(weights_ref, 1, -6)
    sweep(weights, field, other, -4, 12)
    sweep(weights, other, field, -3, 11)
    sweep(weights, field, other, -2, 10)
    sweep(weights, other, pressure_new, -1, 9)
    residual_planes(weights, pressure_new, residual_new, 0, 0, 4)
    first = jnp.where(north, 2, 5)
    for i in range(3):
        sent[i] = pressure_new_ref[first + i, PAD : PAD + ROWS]
    sent[3] = packed(residual_new[0], residual_new[1], residual_new[2], residual_new[3])
    sent_far[...] = residual_new[jnp.where(north, 0, 3)]


def finish(
    n_chips, mobile_ref, weights_ref, pressure, residual, coarse_weights_ref, got, far, swapped,
    velocity, species, u_rims, v_rims, x_rims, y_low, y_high,
    velocity_out, pressure_out, species_out,
    residual_w, pressure_w, one_ref, two_ref, field_ref, other_ref, final_pad,
):
    north, cross, _ = whereabouts(n_chips)
    for ref in (one_ref, two_ref, field_ref, other_ref, final_pad):
        clear_pads(ref)
    one, two = Field(one_ref, -5), Field(two_ref, -5)
    field, other, final = Field(field_ref, -4), Field(other_ref, -4), Field(final_pad, -2)
    a, b = got[3], swapped[3]
    left, right = unpacked(jnp.where(north, a, b)), unpacked(jnp.where(north, b, a))
    for i in range(4):
        residual_w[1 + i] = left[i]
        residual_w[5 + i] = residual[i]
        residual_w[9 + i] = right[i]
    residual_w[0] = far[...]
    residual_w[13] = far[...]
    for i in range(3):
        pressure_w[i] = got[i]
        pressure_w[13 + i] = got[i]
    known = Field(pressure, -1)

    def copy_pressure(i):
        pressure_w[(i + 4).index()] = known(i)

    loop(-1, 9, copy_pressure)

    shift, coarse_shift = jnp.where(north, 0, 4), jnp.where(north, 0, 2)
    coarse_weights = Weights(coarse_weights_ref, 2, -6, coarse_shift, at(residual_w, -5))

    def right_side(i):
        k = (i + 5).index()
        factor = coarse_weights_ref[7, coarse_weights.place(i)]
        residual_w[k] = residual_w[(i + 5).index(coarse_shift)] * factor

    for k in range(12):
        right_side(Place(0, k - 5))
    coarse_sweeps(coarse_weights, one, two, -5, 7)

    def prolong(i):
        correction = two(i)
        for half in range(2):
            k = 2 * i + half
            field.put(k, pressure_w[(k + 4).index(shift)] + correction)

    loop(-2, 4, prolong)

    weights = Weights(weights_ref, 1, -6, shift)
    sweep(weights, field, other, -3, 7)
    sweep(weights, other, final, -2, 6)

    start = pl.multiple_of(cross * BLOCK, BLOCK)
    own = pl.ds(start + 8, BLOCK)
    row, lane = rows_of((BLOCK, LANES)), lanes_of((BLOCK, LANES))

    def u_out(x):
        if x < 0:
            u = u_rims[0]
        elif x > 3:
            u = u_rims[1]
        else:
            u = velocity[0, x]
        slope = 0.5 * (final_pad[x + 3, own] - final_pad[x + 1, own])
        return u - mobile_ref[shift + (x + 7), own] * slope

    u = [u_out(x) for x in range(-1, 5)]
    wide = pl.ds(start, 32)
    for x in range(4):
        p = final_pad[x + 2, wide]
        m = mobile_ref[shift + (x + 7), wide]
        p_own = p[8:24]
        v = velocity[1, x] - m[8:24] * (0.5 * (p[9:25] - p[7:23]))
        v_low = v_rims[x : x + 1] - m[7:8] * (0.5 * (p[8:9] - p[6:7]))
        v_high = v_rims[4 + x : 5 + x] - m[24:25] * (0.5 * (p[25:26] - p[23:24]))
        p_zp = jnp.where(lane < LANES - 1, roll_lanes(p_own, -1), 0.0)
        p_zm = jnp.where(lane > 0, roll_lanes(p_own, 1), 0.0)
        w = velocity[2, x] - m[8:24] * (0.5 * (p_zp - p_zm))
        velocity_out[0, x] = u[x + 1]
        velocity_out[1, x] = v
        velocity_out[2, x] = w
        pressure_out[x] = p_own

        flow_xm, flow_xp = 0.5 * (u[x] + u[x + 1]), 0.5 * (u[x + 1] + u[x + 2])
        v_m = jnp.where(row == 0, v_low, roll_rows(v, 1))
        v_p = jnp.where(row == BLOCK - 1, v_high, roll_rows(v, -1))
        flow_ym, flow_yp = 0.5 * (v_m + v), 0.5 * (v + v_p)
        w_m = jnp.where(lane > 0, roll_lanes(w, 1), 0.0)
        w_p = jnp.where(lane < LANES - 1, roll_lanes(w, -1), 0.0)
        flow_zm, flow_zp = 0.5 * (w_m + w), 0.5 * (w + w_p)

        def leaves(high, low):
            return jnp.maximum(high, 0.0) - jnp.minimum(low, 0.0)

        keep = 1.0 - time_step * (
            leaves(flow_xp, flow_xm) + leaves(flow_yp, flow_ym) + leaves(flow_zp, flow_zm)
        )
        from_xm, from_xp = (
            time_step * jnp.maximum(flow_xm, 0.0),
            -time_step * jnp.minimum(flow_xp, 0.0),
        )
        from_ym, from_yp = (
            time_step * jnp.maximum(flow_ym, 0.0),
            -time_step * jnp.minimum(flow_yp, 0.0),
        )
        from_zm = jnp.where(lane > 0, time_step * jnp.maximum(flow_zm, 0.0), 0.0)
        from_zp = jnp.where(lane < LANES - 1, -time_step * jnp.minimum(flow_zp, 0.0), 0.0)
        for s in range(SPECIES):
            c = species[s, x]
            rim = slice(BLOCK * s, BLOCK * (s + 1))
            if x > 0:
                c_xm = species[s, x - 1]
            else:
                c_xm = x_rims[0, rim]
            if x < 3:
                c_xp = species[s, x + 1]
            else:
                c_xp = x_rims[1, rim]
            r = 4 * s + x
            c_ym = jnp.where(row == 0, y_low[r : r + 1], roll_rows(c, 1))
            c_yp = jnp.where(row == BLOCK - 1, y_high[r : r + 1], roll_rows(c, -1))
            total = keep * c + (from_xm * c_xm + from_xp * c_xp)
            total = total + (from_ym * c_ym + from_yp * c_yp)
            total = total + (from_zm * roll_lanes(c, 1) + from_zp * roll_lanes(c, -1))
            species_out[s, x] = total


def call(kernel, outs, scratch, *operands, where=pltpu.VMEM, semaphores=0, grant=24):
    vmem = pl.BlockSpec(memory_space=pltpu.VMEM)
    shapes = [jax.ShapeDtypeStruct(shape, jnp.float32) for shape in outs]
    scratch = [pltpu.VMEM(shape, jnp.float32) for shape in scratch]
    if semaphores:
        scratch = [*scratch, pltpu.SemaphoreType.DMA((semaphores,))]
    return pl.pallas_call(
        kernel,
        out_shape=shapes,
        in_specs=[pl.BlockSpec(memory_space=where) for _ in operands],
        out_specs=[vmem for _ in outs],
        scratch_shapes=scratch,
        cost_estimate=pl.CostEstimate(flops=1000000, bytes_accessed=1000000, transcendentals=0),
        compiler_params=pltpu.CompilerParams(vmem_limit_bytes=grant * 2**20),
        interpret=INTERPRET,
    )(*operands)


def local(n_chips, velocity, density, source, species):
    groups = [[(2 * j + k) * 4 + c for c in range(4) for k in range(2)] for j in range(n_chips)]

    def beside(distance):
        pairs = []
        for j in range(n_chips - distance):
            left, right = 2 * j + 1, 2 * (j + distance)
            pairs += [(left, right), (right, left)]
        return pairs

    within = [pair for j in range(n_chips) for pair in ((2 * j, 2 * j + 1), (2 * j + 1, 2 * j))]
    upward = [(c, c + 1) for c in range(3)]
    downward = [(c + 1, c) for c in range(3)]

    def plane(n):
        return (n, ROWS, LANES)

    def padded(n):
        return (n, *PADDED)

    def bind(kernel):
        return functools.partial(kernel, n_chips)

    (own,) = call(
        prepare, [(OWN, LANES)], [velocity.shape, density.shape, source.shape],
        velocity, density, source,
        where=HBM, semaphores=3, grant=63,
    )
    gathered = lax.all_gather(own, ("slab", "cross"), axis_index_groups=groups)
    mobile, target, edge, sent = call(
        bind(assemble), [plane(8), plane(8), plane(2), plane(14)], [], gathered
    )
    got = lax.ppermute(sent, "slab", beside(1))
    swapped = lax.ppermute(got, "slab", within)
    mobile_w, weights, pressure, residual, coarse, outer, sent, rim, edge_low, edge_high = call(
        bind(first_cycle),
        [
            padded(22), (8, *plane(20)), padded(20), plane(8), plane(10), PLANE, (272, LANES),
            (144, LANES), (40, LANES), (40, LANES),
        ],
        [plane(20), padded(20)],
        mobile, target, edge, got, swapped, species,
    )
    near = lax.ppermute(sent, "slab", beside(1))
    y_low = lax.ppermute(edge_high, "cross", upward)
    y_high = lax.ppermute(edge_low, "cross", downward)
    u_rims, v_rims = call(bind(flow_rims), [(2, BLOCK, LANES), (8, LANES)], [], gathered, outer)
    opposite = lax.ppermute(jnp.concatenate([near[:128], rim], 0), "slab", within)
    pressure, residual, coarse_weights, sent, sent_far = call(
        bind(second_cycle),
        [padded(10), plane(4), (8, *plane(16)), plane(4), PLANE],
        [padded(18), plane(16), padded(16), padded(16), padded(20), padded(20)],
        weights, pressure, residual, coarse, near, opposite,
    )
    got = lax.ppermute(sent, "slab", beside(1))
    far = lax.ppermute(sent_far, "slab", beside(2))
    (x_rims,) = call(bind(species_rims), [(2, 144, LANES)], [], near, opposite)
    swapped = lax.ppermute(got, "slab", within)
    return call(
        bind(finish),
        [velocity.shape, density.shape, species.shape],
        [plane(14), plane(16), padded(12), padded(12), padded(12), padded(12), padded(8)],
        mobile_w, weights, pressure, residual, coarse_weights, got, far, swapped,
        velocity, species, u_rims, v_rims, x_rims, y_low, y_high,
    )


def solution(mesh):
    n_chips = mesh.shape["slab"] // 2
    block = P("slab", "cross", None)
    stack = P(None, "slab", "cross", None)

    def step(*arrays):
        return tuple(local(n_chips, *arrays))

    return jax.shard_map(
        step,
        mesh=mesh,
        in_specs=(stack, block, block, stack),
        out_specs=(stack, block, stack),
        check_vma=False,
    )
```

```python
import functools

import jax
import jax.numpy as jnp
from jax import lax
from jax.experimental import pallas as pl
from jax.experimental.pallas import tpu as pltpu
from jax.sharding import PartitionSpec as P


INTERPRET = False
HBM = pltpu.HBM
ROWS = 64
LANES = 128
BLOCK = 16
SPECIES = 9
EDGE = 160
OWN = EDGE + 8
damping = 0.8
time_step = 0.25


class Place:
    def __init__(self, counter, constant):
        self.counter = counter
        self.constant = constant

    def __add__(self, other):
        return Place(self.counter, self.constant + other)

    def __sub__(self, other):
        return Place(self.counter, self.constant - other)

    def __rmul__(self, factor):
        return Place(self.counter * factor, self.constant * factor)

    def index(self, shift=None):
        start = self.counter if shift is None else self.counter + shift
        return start + self.constant


def loop(low, high, body):
    count = high - low
    some = next(u for u in (4, 5, 6, 3, 7, 2, 1) if count % u == 0)

    def several(start):
        for u in range(some):
            body(Place(start, low + u))

    def step(i, carry):
        several(i * some)
        return carry

    if count == some:
        several(0)
    else:
        lax.fori_loop(0, count // some, step, 0)


def rows_of(shape):
    return lax.broadcasted_iota(jnp.int32, shape, 0)


def lanes_of(shape):
    return lax.broadcasted_iota(jnp.int32, shape, 1)


PLANE = (ROWS, LANES)


def roll_rows(x, by):
    return pltpu.roll(x, by % x.shape[0], 0)


def roll_lanes(x, by):
    return pltpu.roll(x, by % x.shape[1], 1)


PAD = 8
PADDED = (ROWS + 2 * PAD, LANES)


class Field:
    def __init__(self, ref, low, shift=None):
        self.ref = ref
        self.low = low
        self.shift = shift

    def __call__(self, i, rows=0):
        k = (i - self.low).index(self.shift)
        return self.ref[k, PAD + rows : PAD + rows + ROWS]

    def put(self, i, value):
        self.ref[(i - self.low).index(), PAD : PAD + ROWS] = value


def clear_pads(ref):
    nothing = jnp.zeros((PAD, LANES), jnp.float32)
    for k in range(ref.shape[0]):
        ref[k, 0:PAD] = nothing
        ref[k, PAD + ROWS :] = nothing


class Weights:
    def __init__(self, ref, step, low, shift=None, constant=None):
        self.ref = ref
        self.step = step
        self.low = low
        self.shift = shift
        self.constant = constant

    def place(self, i):
        return (i - self.low).index(self.shift)

    def fill(self, low, high, mobile, target, inside):
        s = self.step
        lane = lanes_of(PLANE)
        z_low, z_high = lane >= s, lane < LANES - s

        def body(i):
            m = mobile(i)
            x_m, x_p = mobile(i - 1), mobile(i + 1)
            y_m, y_p = mobile(i, -s), mobile(i, s)
            z_m = jnp.where(z_low, roll_lanes(m, s), 0.0)
            z_p = jnp.where(z_high, roll_lanes(m, -s), 0.0)
            diagonal = 3.0 * m + 0.5 * ((x_m + x_p) + (y_m + y_p) + (z_m + z_p))
            valid = inside(i)
            scaled = (damping * valid) / (diagonal + (1.0 - valid))
            half = 0.5 * scaled
            k = self.place(i)
            self.ref[0, k] = (m + x_m) * half
            self.ref[1, k] = (m + x_p) * half
            self.ref[2, k] = (m + y_m) * half
            self.ref[3, k] = (m + y_p) * half
            self.ref[4, k] = jnp.where(z_low, (m + z_m) * half, 0.0)
            self.ref[5, k] = jnp.where(z_high, (m + z_p) * half, 0.0)
            if s == 1:
                self.ref[6, k] = target(i) * scaled
                self.ref[7, k] = diagonal * (1.0 / damping)
            else:
                self.ref[6, k] = target(i) * (4.0 * scaled)
                self.ref[7, k] = 4.0 * scaled

        loop(low, high, body)

    def side(self, i):
        if self.constant is not None:
            return self.constant(i)
        return self.ref[6, self.place(i)]

    def change(self, field, i):
        s = self.step
        k = self.place(i)
        p = field(i)
        total = self.ref[0, k] * field(i - 1) + self.ref[1, k] * field(i + 1)
        total = total + (self.ref[2, k] * field(i, -s) + self.ref[3, k] * field(i, s))
        total = total + (self.ref[4, k] * roll_lanes(p, s) + self.ref[5, k] * roll_lanes(p, -s))
        return p, (total - self.side(i)) - damping * p


def at(ref, origin, shift=None):
    return lambda i: ref[(i - origin).index(shift)]


def sweep(weights, source, result, low, high):
    def body(i):
        p, change = weights.change(source, i)
        result.put(i, p + change)

    loop(low, high, body)


def first_sweep(weights, result, low, high):
    def body(i):
        result.put(i, -weights.side(i))

    loop(low, high, body)


def pair_sum(q):
    row, lane = rows_of(PLANE), lanes_of(PLANE)
    q = q + jnp.where(lane % 2 == 0, roll_lanes(q, -1), roll_lanes(q, 1))
    return q + jnp.where(row % 2 == 0, roll_rows(q, -1), roll_rows(q, 1))


def packed(a, b, c, d):
    row, lane = rows_of(PLANE), lanes_of(PLANE)
    even = lane % 2 == 0
    return jnp.where(row % 2 == 0, jnp.where(even, a, b), jnp.where(even, c, d))


def unpacked(v):
    row, lane = rows_of(PLANE), lanes_of(PLANE)
    even, upper = lane % 2 == 0, row % 2 == 0
    first = jnp.where(even, v, roll_lanes(v, 1))
    second = jnp.where(even, roll_lanes(v, -1), v)

    def low_row(x):
        return jnp.where(upper, x, roll_rows(x, 1))

    def high_row(x):
        return jnp.where(upper, roll_rows(x, -1), x)

    return low_row(first), low_row(second), high_row(first), high_row(second)


def residual_planes(weights, field, result, result_low, low, high):
    def body(i):
        total = 0.0
        for half in range(2):
            _, change = weights.change(field, 2 * i + half)
            total = total - change * weights.ref[7, weights.place(2 * i + half)]
        result[(i - result_low).index()] = 0.125 * pair_sum(total)

    loop(low, high, body)


def inside_of(first, count):
    def inside(i):
        place = i.index(first)
        return jnp.where((place >= 0) & (place < count), 1.0, 0.0)

    return inside


def whereabouts(n_chips):
    slab, cross = lax.axis_index("slab"), lax.axis_index("cross")
    chip = jnp.minimum(jnp.maximum(slab // 2, 0), n_chips - 1)
    return slab % 2 == 0, jnp.minimum(jnp.maximum(cross, 0), 3), chip


def prepare(velocity_in, density_in, source_in, out, velocity, density, source, semaphore):
    copies = [
        pltpu.make_async_copy(there, here, semaphore.at[k])
        for k, (there, here) in enumerate(
            [(density_in, density), (velocity_in, velocity), (source_in, source)]
        )
    ]
    for copy in copies:
        copy.start()
    lane = lanes_of((BLOCK, LANES))
    row = rows_of((BLOCK, LANES))
    copies[0].wait()
    for x in range(4):
        out[BLOCK * x : BLOCK * (x + 1)] = 1.0 / density[x]
    copies[1].wait()
    copies[2].wait()
    for x in range(4):
        u_p = velocity[0, x + 1] if x < 3 else 0.0
        u_m = velocity[0, x - 1] if x > 0 else 0.0
        v, w = velocity[1, x], velocity[2, x]
        v_p = jnp.where(row < BLOCK - 1, roll_rows(v, -1), 0.0)
        v_m = jnp.where(row > 0, roll_rows(v, 1), 0.0)
        w_p = jnp.where(lane < LANES - 1, roll_lanes(w, -1), 0.0)
        w_m = jnp.where(lane > 0, roll_lanes(w, 1), 0.0)
        moved = 0.5 * ((u_p - u_m) + (v_p - v_m) + (w_p - w_m))
        out[64 + BLOCK * x : 64 + BLOCK * (x + 1)] = moved - source[x]
        r = EDGE + x
        out[r : r + 1] = velocity[1, x, 0:1]
        out[r + 4 : r + 5] = velocity[1, x, BLOCK - 1 : BLOCK]
    out[128:144] = velocity[0, 0]
    out[144:160] = velocity[0, 3]


def assemble(n_chips, gathered, sent, sent_far, edge):
    north, _, _ = whereabouts(n_chips)
    row = rows_of((BLOCK, LANES))
    for c in range(4):
        rows = slice(BLOCK * c, BLOCK * (c + 1))
        for k in range(2):
            block = 2 * c + k
            for x in range(4):
                sent[4 * k + x, rows] = gathered[block, BLOCK * x : BLOCK * (x + 1)]
                t = gathered[block, 64 + BLOCK * x : 64 + BLOCK * (x + 1)]
                r = EDGE + x
                if c > 0:
                    t = t - jnp.where(row == 0, 0.5 * gathered[block - 2, r + 4 : r + 5], 0.0)
                if c < 3:
                    t = t + jnp.where(row == BLOCK - 1, 0.5 * gathered[block + 2, r : r + 1], 0.0)
                if k == 0 and x == 3:
                    t = t + 0.5 * gathered[block + 1, 128:144]
                if k == 1 and x == 0:
                    t = t - 0.5 * gathered[block - 1, 144:160]
                sent[8 + 4 * k + x, rows] = t
        edge[0, rows] = gathered[2 * c, 128:144]
        edge[1, rows] = gathered[2 * c + 1, 144:160]
    u = edge[jnp.where(north, 0, 1)]
    sent[16] = u
    sent_far[0] = sent[jnp.where(north, 0, 7)]
    sent_far[1] = u


def species_edges(n_chips, species, near, beside, edge_low, edge_high):
    north, _, _ = whereabouts(n_chips)
    outward, inward = jnp.where(north, 0, 3), jnp.where(north, 3, 0)
    for s in range(SPECIES):
        near[BLOCK * s : BLOCK * (s + 1)] = species[s, outward]
        beside[BLOCK * s : BLOCK * (s + 1)] = species[s, inward]
        for x in range(4):
            r = 4 * s + x
            edge_low[r : r + 1] = species[s, x, 0:1]
            edge_high[r : r + 1] = species[s, x, BLOCK - 1 : BLOCK]
    edge_low[36:40] = jnp.zeros((4, LANES), jnp.float32)
    edge_high[36:40] = jnp.zeros((4, LANES), jnp.float32)


def flow_rims(n_chips, gathered, u_beside, v_rims):
    north, cross, _ = whereabouts(n_chips)
    core = jnp.where(north, 0, 1)
    partner = 2 * cross + jnp.where(north, 1, 0)
    u_beside[...] = jnp.where(north, gathered[partner, 128:144], gathered[partner, 144:160])
    below = gathered[2 * jnp.maximum(cross - 1, 0) + core, EDGE:OWN]
    above = gathered[2 * jnp.minimum(cross + 1, 3) + core, EDGE:OWN]
    v_rims[0:4] = jnp.where(cross > 0, below[4:8], 0.0)
    v_rims[4:8] = jnp.where(cross < 3, above[0:4], 0.0)


def first_cycle(
    n_chips, own, edge, mine, swapped, species_near,
    mobile_ref, weights_ref, pressure_ref, residual, coarse, outer, sent,
    target_w, field_ref,
):
    north, _, chip = whereabouts(n_chips)
    clear_pads(mobile_ref)
    clear_pads(field_ref)
    clear_pads(pressure_ref)
    mobile_w, pressure = Field(mobile_ref, -9), Field(pressure_ref, -8)
    field = Field(field_ref, -8)

    def sides(k):
        a, b = mine[k], swapped[k]
        return jnp.where(north, a, b), jnp.where(north, b, a)

    def copy(i):
        k, later = i.index(), (i + 8).index()
        left, right = sides(k)
        mobile_w.put(i - 8, left)
        mobile_w.put(i, own[k])
        mobile_w.put(i + 8, right)
        left, right = sides(later)
        target_w[k] = left
        target_w[later] = own[later]
        target_w[(i + 16).index()] = right

    loop(0, 8, copy)
    left, right = sides(17)
    mobile_w.put(Place(0, -9), left)
    mobile_w.put(Place(0, 16), right)
    left, right = sides(18)
    target_w[0] = target_w[0] - 0.5 * left
    target_w[23] = target_w[23] + 0.5 * right
    left, right = sides(16)
    target_w[7] = target_w[7] + 0.5 * edge[0]
    target_w[8] = target_w[8] - 0.5 * left
    target_w[15] = target_w[15] + 0.5 * right
    target_w[16] = target_w[16] - 0.5 * edge[1]
    outer[...] = mine[16]

    weights = Weights(weights_ref, 1, -8)
    weights.fill(-8, 16, mobile_w, at(target_w, -8), inside_of(8 * chip, 8 * n_chips))
    first_sweep(weights, field, -8, 16)
    sweep(weights, field, pressure, -7, 15)
    residual_planes(weights, pressure, residual, -3, -3, 7)

    def restrict(i):
        pair = mobile_w(2 * i) + mobile_w(2 * i + 1)
        coarse[(i + 4).index()] = 0.125 * pair_sum(pair)

    loop(-4, 8, restrict)
    r = jnp.where(north, 6, 0)
    sent[0:64] = packed(residual[r], residual[r + 1], residual[r + 2], residual[r + 3])
    m = jnp.where(north, 8, 0)
    sent[64:128] = packed(coarse[m], coarse[m + 1], coarse[m + 2], coarse[m + 3])
    sent[128:272] = species_near[...]


def coarse_sweeps(weights, one, two, low, high):
    first_sweep(weights, one, low, high)
    sweep(weights, one, two, low + 1, high - 1)
    sweep(weights, two, one, low + 2, high - 2)
    sweep(weights, one, two, low + 3, high - 3)


def inner(n_chips, chip):
    return chip > 0, chip < n_chips - 1


def second_cycle(
    n_chips, weights_ref, pressure_ref, residual, coarse, got,
    pressure_new_ref, residual_new, coarse_weights_ref, sent,
    coarse_ref, residual_w, one_ref, two_ref, field_ref, other_ref,
):
    north, _, chip = whereabouts(n_chips)
    before, after = inner(n_chips, chip)
    for ref in (pressure_new_ref, coarse_ref, one_ref, two_ref, field_ref, other_ref):
        clear_pads(ref)
    coarse_w, one, two = Field(coarse_ref, -8), Field(one_ref, -7), Field(two_ref, -7)
    field, other = Field(field_ref, -8), Field(other_ref, -8)
    pressure, pressure_new = Field(pressure_ref, -8), Field(pressure_new_ref, -3)

    left = unpacked(jnp.where(before, got[0, 0:64], 0.0))
    right = unpacked(jnp.where(after, got[1, 272:336], 0.0))
    for i in range(4):
        residual_w[i] = left[i]
        residual_w[14 + i] = right[i]
    left = unpacked(jnp.where(before, got[0, 64:128], 0.0))
    right = unpacked(jnp.where(after, got[1, 336:400], 0.0))
    for i in range(4):
        coarse_w.put(Place(0, i - 8), left[i])
        coarse_w.put(Place(0, i + 8), right[i])

    def copy_residual(i):
        residual_w[(i + 4).index()] = residual[i.index()]

    def copy_coarse(i):
        coarse_w.put(i - 4, coarse[i.index()])

    loop(0, 10, copy_residual)
    loop(0, 12, copy_coarse)

    coarse_weights = Weights(coarse_weights_ref, 2, -7)
    coarse_weights.fill(-7, 11, coarse_w, at(residual_w, -7), inside_of(4 * chip, 4 * n_chips))
    coarse_sweeps(coarse_weights, one, two, -7, 11)

    def prolong(i):
        correction = two(i)
        for half in range(2):
            k = 2 * i + half
            field.put(k, pressure(k) + correction)

    loop(-4, 8, prolong)

    weights = Weights(weights_ref, 1, -8)
    sweep(weights, field, other, -6, 14)
    sweep(weights, other, field, -5, 13)
    sweep(weights, field, other, -4, 12)
    sweep(weights, other, pressure_new, -3, 11)
    residual_planes(weights, pressure_new, residual_new, -1, -1, 5)
    sent[0] = pressure_new_ref[jnp.where(north, 6, 7), PAD : PAD + ROWS]
    r = jnp.where(north, 2, 0)
    sent[1] = packed(
        residual_new[r], residual_new[r + 1], residual_new[r + 2], residual_new[r + 3]
    )


def finish(
    n_chips, mobile_ref, weights_ref, pressure, residual, coarse_weights_ref, got, swapped,
    velocity, species, outer, u_beside, v_rims, sides, y_low, y_high,
    velocity_out, pressure_out, species_out,
    residual_w, pressure_w, one_ref, two_ref, field_ref, other_ref, final_pad,
):
    north, cross, chip = whereabouts(n_chips)
    before, after = inner(n_chips, chip)
    for ref in (one_ref, two_ref, field_ref, other_ref, final_pad):
        clear_pads(ref)
    one, two = Field(one_ref, -5), Field(two_ref, -5)
    field, other, final = Field(field_ref, -4), Field(other_ref, -4), Field(final_pad, -2)
    left = unpacked(jnp.where(before, swapped[0, 0], 0.0))
    right = unpacked(jnp.where(after, swapped[1, 1], 0.0))
    for i in range(4):
        residual_w[i] = left[i]
        residual_w[10 + i] = right[i]
    for i in range(6):
        residual_w[4 + i] = residual[i]
    pressure_w[0] = jnp.where(before, got[0, 0], 0.0)
    pressure_w[15] = jnp.where(after, got[1, 0], 0.0)
    known = Field(pressure, -3)

    def copy_pressure(i):
        pressure_w[(i + 4).index()] = known(i)

    loop(-3, 11, copy_pressure)

    shift, coarse_shift = jnp.where(north, 0, 4), jnp.where(north, 0, 2)
    coarse_weights = Weights(coarse_weights_ref, 2, -7, coarse_shift, at(residual_w, -5))

    def right_side(i):
        k = (i + 5).index()
        factor = coarse_weights_ref[7, coarse_weights.place(i)]
        residual_w[k] = residual_w[(i + 5).index(coarse_shift)] * factor

    for k in range(12):
        right_side(Place(0, k - 5))
    coarse_sweeps(coarse_weights, one, two, -5, 7)

    def prolong(i):
        correction = two(i)
        for half in range(2):
            k = 2 * i + half
            field.put(k, pressure_w[(k + 4).index(shift)] + correction)

    loop(-2, 4, prolong)

    weights = Weights(weights_ref, 1, -8, shift)
    sweep(weights, field, other, -3, 7)
    sweep(weights, other, final, -2, 6)

    start = pl.multiple_of(cross * BLOCK, BLOCK)
    own = pl.ds(start + 8, BLOCK)
    row, lane = rows_of((BLOCK, LANES)), lanes_of((BLOCK, LANES))

    beyond = outer[pl.ds(start, BLOCK)]
    u_low = jnp.where(north, beyond, u_beside[...])
    u_high = jnp.where(north, u_beside[...], beyond)

    def u_out(x):
        if x < 0:
            u = u_low
        elif x > 3:
            u = u_high
        else:
            u = velocity[0, x]
        slope = 0.5 * (final_pad[x + 3, own] - final_pad[x + 1, own])
        return u - mobile_ref[shift + (x + 9), own] * slope

    u = [u_out(x) for x in range(-1, 5)]

    def species_beside(s, side):
        at_rim = BLOCK * s + (128 if side == 0 else 400)
        outside = sides[side, at_rim : at_rim + BLOCK]
        outside = jnp.where(before if side == 0 else after, outside, 0.0)
        inside = sides[side, 544 + BLOCK * s : 560 + BLOCK * s]
        return jnp.where(north, outside, inside) if side == 0 else jnp.where(north, inside, outside)

    wide = pl.ds(start, 32)
    for x in range(4):
        p = final_pad[x + 2, wide]
        m = mobile_ref[shift + (x + 9), wide]
        p_own = p[8:24]
        v = velocity[1, x] - m[8:24] * (0.5 * (p[9:25] - p[7:23]))
        v_low = v_rims[x : x + 1] - m[7:8] * (0.5 * (p[8:9] - p[6:7]))
        v_high = v_rims[4 + x : 5 + x] - m[24:25] * (0.5 * (p[25:26] - p[23:24]))
        p_zp = jnp.where(lane < LANES - 1, roll_lanes(p_own, -1), 0.0)
        p_zm = jnp.where(lane > 0, roll_lanes(p_own, 1), 0.0)
        w = velocity[2, x] - m[8:24] * (0.5 * (p_zp - p_zm))
        velocity_out[0, x] = u[x + 1]
        velocity_out[1, x] = v
        velocity_out[2, x] = w
        pressure_out[x] = p_own

        flow_xm, flow_xp = 0.5 * (u[x] + u[x + 1]), 0.5 * (u[x + 1] + u[x + 2])
        v_m = jnp.where(row == 0, v_low, roll_rows(v, 1))
        v_p = jnp.where(row == BLOCK - 1, v_high, roll_rows(v, -1))
        flow_ym, flow_yp = 0.5 * (v_m + v), 0.5 * (v + v_p)
        w_m = jnp.where(lane > 0, roll_lanes(w, 1), 0.0)
        w_p = jnp.where(lane < LANES - 1, roll_lanes(w, -1), 0.0)
        flow_zm, flow_zp = 0.5 * (w_m + w), 0.5 * (w + w_p)

        def leaves(high, low):
            return jnp.maximum(high, 0.0) - jnp.minimum(low, 0.0)

        keep = 1.0 - time_step * (
            leaves(flow_xp, flow_xm) + leaves(flow_yp, flow_ym) + leaves(flow_zp, flow_zm)
        )
        from_xm, from_xp = (
            time_step * jnp.maximum(flow_xm, 0.0),
            -time_step * jnp.minimum(flow_xp, 0.0),
        )
        from_ym, from_yp = (
            time_step * jnp.maximum(flow_ym, 0.0),
            -time_step * jnp.minimum(flow_yp, 0.0),
        )
        from_zm = jnp.where(lane > 0, time_step * jnp.maximum(flow_zm, 0.0), 0.0)
        from_zp = jnp.where(lane < LANES - 1, -time_step * jnp.minimum(flow_zp, 0.0), 0.0)
        for s in range(SPECIES):
            c = species[s, x]
            if x > 0:
                c_xm = species[s, x - 1]
            else:
                c_xm = species_beside(s, 0)
            if x < 3:
                c_xp = species[s, x + 1]
            else:
                c_xp = species_beside(s, 1)
            r = 4 * s + x
            c_ym = jnp.where(row == 0, y_low[r : r + 1], roll_rows(c, 1))
            c_yp = jnp.where(row == BLOCK - 1, y_high[r : r + 1], roll_rows(c, -1))
            total = keep * c + (from_xm * c_xm + from_xp * c_xp)
            total = total + (from_ym * c_ym + from_yp * c_yp)
            total = total + (from_zm * roll_lanes(c, 1) + from_zp * roll_lanes(c, -1))
            species_out[s, x] = total


def call(kernel, outs, scratch, *operands, where=pltpu.VMEM, semaphores=0, grant=24):
    vmem = pl.BlockSpec(memory_space=pltpu.VMEM)
    shapes = [jax.ShapeDtypeStruct(shape, jnp.float32) for shape in outs]
    scratch = [pltpu.VMEM(shape, jnp.float32) for shape in scratch]
    if semaphores:
        scratch = [*scratch, pltpu.SemaphoreType.DMA((semaphores,))]
    return pl.pallas_call(
        kernel,
        out_shape=shapes,
        in_specs=[pl.BlockSpec(memory_space=where) for _ in operands],
        out_specs=[vmem for _ in outs],
        scratch_shapes=scratch,
        cost_estimate=pl.CostEstimate(flops=1000000, bytes_accessed=1000000, transcendentals=0),
        compiler_params=pltpu.CompilerParams(vmem_limit_bytes=grant * 2**20),
        interpret=INTERPRET,
    )(*operands)


def gathered_over(array, groups):
    return lax.all_gather(array, ("slab", "cross"), axis_index_groups=groups)


def local(n_chips, velocity, density, source, species):
    def device(slab, cross):
        return 4 * slab + cross

    chips = [[device(2 * j + k, c) for c in range(4) for k in range(2)] for j in range(n_chips)]
    cores = [
        [device(2 * j, c), device(2 * j + 1, c)] for j in range(n_chips) for c in range(4)
    ]
    facing = [
        [device(2 * j + 1, c), device(2 * j + 2, c)] for j in range(n_chips - 1) for c in range(4)
    ]
    for slab in (0, 2 * n_chips - 1):
        facing += [[device(slab, 0), device(slab, 1)], [device(slab, 2), device(slab, 3)]]

    def beside(distance):
        pairs = []
        for j in range(n_chips - distance):
            left, right = 2 * j + 1, 2 * (j + distance)
            pairs += [(left, right), (right, left)]
        return pairs

    within = [pair for j in range(n_chips) for pair in ((2 * j, 2 * j + 1), (2 * j + 1, 2 * j))]
    upward = [(c, c + 1) for c in range(3)]
    downward = [(c + 1, c) for c in range(3)]

    def plane(n):
        return (n, ROWS, LANES)

    def padded(n):
        return (n, *PADDED)

    def bind(kernel):
        return functools.partial(kernel, n_chips)

    (own,) = call(
        prepare, [(OWN, LANES)], [velocity.shape, density.shape, source.shape],
        velocity, density, source,
        where=HBM, semaphores=3, grant=63,
    )
    gathered = gathered_over(own, chips)
    sent, sent_far, edge = call(bind(assemble), [plane(17), plane(2), plane(2)], [], gathered)
    near = lax.ppermute(sent, "slab", beside(1))
    far = lax.ppermute(sent_far, "slab", beside(2))
    species_near, species_beside, edge_low, edge_high = call(
        bind(species_edges), [(144, LANES), (144, LANES), (40, LANES), (40, LANES)], [], species
    )
    y_low = lax.ppermute(edge_high, "cross", upward)
    y_high = lax.ppermute(edge_low, "cross", downward)
    u_beside, v_rims = call(bind(flow_rims), [(BLOCK, LANES), (8, LANES)], [], gathered)
    mine = jnp.concatenate([near, far], 0)
    swapped = lax.ppermute(mine, "slab", within)
    mobile_w, weights, pressure, residual, coarse, outer, sent_two = call(
        bind(first_cycle),
        [
            padded(26), (8, *plane(24)), padded(24), plane(10), plane(12), PLANE, (272, LANES),
        ],
        [plane(24), padded(24)],
        sent, edge, mine, swapped, species_near,
    )
    near = gathered_over(sent_two, facing).reshape(544, LANES)
    sides = gathered_over(jnp.concatenate([near, species_beside], 0), cores)
    pressure, residual, coarse_weights, sent = call(
        bind(second_cycle),
        [padded(14), plane(6), (8, *plane(18)), plane(2)],
        [padded(20), plane(18), padded(18), padded(18), padded(24), padded(24)],
        weights, pressure, residual, coarse, sides,
    )
    near = gathered_over(sent, facing)
    swapped = gathered_over(near[:, 1], cores)
    return call(
        bind(finish),
        [velocity.shape, density.shape, species.shape],
        [plane(14), plane(16), padded(12), padded(12), padded(12), padded(12), padded(8)],
        mobile_w, weights, pressure, residual, coarse_weights, near, swapped,
        velocity, species, outer, u_beside, v_rims, sides, y_low, y_high,
    )


def solution(mesh):
    n_chips = mesh.shape["slab"] // 2
    block = P("slab", "cross", None)
    stack = P(None, "slab", "cross", None)

    def step(*arrays):
        return tuple(local(n_chips, *arrays))

    return jax.shard_map(
        step,
        mesh=mesh,
        in_specs=(stack, block, block, stack),
        out_specs=(stack, block, stack),
        check_vma=False,
    )
```

```python
import functools

import jax
import jax.numpy as jnp
from jax import lax
from jax.experimental import pallas as pl
from jax.experimental.pallas import tpu as pltpu
from jax.sharding import PartitionSpec as P


INTERPRET = False
HBM = pltpu.HBM
ROWS = 64
LANES = 128
BLOCK = 16
SPECIES = 9
EDGE = 160
OWN = EDGE + 8
damping = 0.8
time_step = 0.25


class Place:
    def __init__(self, counter, constant):
        self.counter = counter
        self.constant = constant

    def __add__(self, other):
        return Place(self.counter, self.constant + other)

    def __sub__(self, other):
        return Place(self.counter, self.constant - other)

    def __rmul__(self, factor):
        return Place(self.counter * factor, self.constant * factor)

    def index(self, shift=None):
        start = self.counter if shift is None else self.counter + shift
        return start + self.constant


def loop(low, high, body):
    count = high - low
    some = next(u for u in (4, 5, 6, 3, 7, 2, 1) if count % u == 0)

    def several(start):
        for u in range(some):
            body(Place(start, low + u))

    def step(i, carry):
        several(i * some)
        return carry

    if count == some:
        several(0)
    else:
        lax.fori_loop(0, count // some, step, 0)


def rows_of(shape):
    return lax.broadcasted_iota(jnp.int32, shape, 0)


def lanes_of(shape):
    return lax.broadcasted_iota(jnp.int32, shape, 1)


PLANE = (ROWS, LANES)


def roll_rows(x, by):
    return pltpu.roll(x, by % x.shape[0], 0)


def roll_lanes(x, by):
    return pltpu.roll(x, by % x.shape[1], 1)


PAD = 8
PADDED = (ROWS + 2 * PAD, LANES)


class Field:
    def __init__(self, ref, low, shift=None):
        self.ref = ref
        self.low = low
        self.shift = shift

    def __call__(self, i, rows=0):
        k = (i - self.low).index(self.shift)
        return self.ref[k, PAD + rows : PAD + rows + ROWS]

    def put(self, i, value):
        self.ref[(i - self.low).index(), PAD : PAD + ROWS] = value


def clear_pads(ref):
    nothing = jnp.zeros((PAD, LANES), jnp.float32)
    for k in range(ref.shape[0]):
        ref[k, 0:PAD] = nothing
        ref[k, PAD + ROWS :] = nothing


class Weights:
    def __init__(self, ref, step, low, shift=None, constant=None):
        self.ref = ref
        self.step = step
        self.low = low
        self.shift = shift
        self.constant = constant

    def place(self, i):
        return (i - self.low).index(self.shift)

    def fill(self, low, high, mobile, target, inside):
        s = self.step
        lane = lanes_of(PLANE)
        z_low, z_high = lane >= s, lane < LANES - s

        def body(i):
            m = mobile(i)
            x_m, x_p = mobile(i - 1), mobile(i + 1)
            y_m, y_p = mobile(i, -s), mobile(i, s)
            z_m = jnp.where(z_low, roll_lanes(m, s), 0.0)
            z_p = jnp.where(z_high, roll_lanes(m, -s), 0.0)
            diagonal = 3.0 * m + 0.5 * ((x_m + x_p) + (y_m + y_p) + (z_m + z_p))
            valid = inside(i)
            scaled = (damping * valid) / (diagonal + (1.0 - valid))
            half = 0.5 * scaled
            k = self.place(i)
            self.ref[0, k, 0:ROWS] = (m + x_m) * half
            self.ref[1, k, 0:ROWS] = (m + x_p) * half
            self.ref[2, k, 0:ROWS] = (m + y_m) * half
            self.ref[3, k, 0:ROWS] = (m + y_p) * half
            self.ref[4, k, 0:ROWS] = jnp.where(z_low, (m + z_m) * half, 0.0)
            self.ref[5, k, 0:ROWS] = jnp.where(z_high, (m + z_p) * half, 0.0)
            if s == 1:
                self.ref[6, k, 0:ROWS] = target(i) * scaled
                self.ref[7, k, 0:ROWS] = diagonal * (1.0 / damping)
            else:
                self.ref[6, k, 0:ROWS] = target(i) * (4.0 * scaled)
                self.ref[7, k, 0:ROWS] = 4.0 * scaled

        loop(low, high, body)

    def side(self, i):
        if self.constant is not None:
            return self.constant(i)
        return self.ref[6, self.place(i), 0:ROWS]

    def change(self, field, i):
        s = self.step
        k = self.place(i)
        p = field(i)
        total = self.ref[0, k, 0:ROWS] * field(i - 1) + self.ref[1, k, 0:ROWS] * field(i + 1)
        total = total + (self.ref[2, k, 0:ROWS] * field(i, -s) + self.ref[3, k, 0:ROWS] * field(i, s))
        total = total + (self.ref[4, k, 0:ROWS] * roll_lanes(p, s) + self.ref[5, k, 0:ROWS] * roll_lanes(p, -s))
        return p, (total - self.side(i)) - damping * p


def at(ref, origin, shift=None):
    return lambda i: ref[(i - origin).index(shift)]


def sweep(weights, source, result, low, high):
    def body(i):
        p, change = weights.change(source, i)
        result.put(i, p + change)

    loop(low, high, body)


def first_sweep(weights, result, low, high):
    def body(i):
        result.put(i, -weights.side(i))

    loop(low, high, body)


def pair_sum(q):
    row, lane = rows_of(PLANE), lanes_of(PLANE)
    q = q + jnp.where(lane % 2 == 0, roll_lanes(q, -1), roll_lanes(q, 1))
    return q + jnp.where(row % 2 == 0, roll_rows(q, -1), roll_rows(q, 1))


def packed(a, b, c, d):
    row, lane = rows_of(PLANE), lanes_of(PLANE)
    even = lane % 2 == 0
    return jnp.where(row % 2 == 0, jnp.where(even, a, b), jnp.where(even, c, d))


def unpacked(v):
    row, lane = rows_of(PLANE), lanes_of(PLANE)
    even, upper = lane % 2 == 0, row % 2 == 0
    first = jnp.where(even, v, roll_lanes(v, 1))
    second = jnp.where(even, roll_lanes(v, -1), v)

    def low_row(x):
        return jnp.where(upper, x, roll_rows(x, 1))

    def high_row(x):
        return jnp.where(upper, roll_rows(x, -1), x)

    return low_row(first), low_row(second), high_row(first), high_row(second)


def residual_planes(weights, field, result, result_low, low, high):
    def body(i):
        total = 0.0
        for half in range(2):
            _, change = weights.change(field, 2 * i + half)
            total = total - change * weights.ref[7, weights.place(2 * i + half), 0:ROWS]
        result[(i - result_low).index()] = 0.125 * pair_sum(total)

    loop(low, high, body)


def inside_of(first, count):
    def inside(i):
        place = i.index(first)
        return jnp.where((place >= 0) & (place < count), 1.0, 0.0)

    return inside


def whereabouts(n_chips):
    slab, cross = lax.axis_index("slab"), lax.axis_index("cross")
    chip = jnp.minimum(jnp.maximum(slab // 2, 0), n_chips - 1)
    return slab % 2 == 0, jnp.minimum(jnp.maximum(cross, 0), 3), chip


def prepare(velocity_in, density_in, source_in, out, velocity, density, source, semaphore):
    copies = [
        pltpu.make_async_copy(there, here, semaphore.at[k])
        for k, (there, here) in enumerate(
            [(density_in, density), (velocity_in, velocity), (source_in, source)]
        )
    ]
    for copy in copies:
        copy.start()
    lane = lanes_of((BLOCK, LANES))
    row = rows_of((BLOCK, LANES))
    copies[0].wait()
    for x in range(4):
        out[BLOCK * x : BLOCK * (x + 1)] = 1.0 / density[x]
    copies[1].wait()
    copies[2].wait()
    for x in range(4):
        u_p = velocity[0, x + 1] if x < 3 else 0.0
        u_m = velocity[0, x - 1] if x > 0 else 0.0
        v, w = velocity[1, x], velocity[2, x]
        v_p = jnp.where(row < BLOCK - 1, roll_rows(v, -1), 0.0)
        v_m = jnp.where(row > 0, roll_rows(v, 1), 0.0)
        w_p = jnp.where(lane < LANES - 1, roll_lanes(w, -1), 0.0)
        w_m = jnp.where(lane > 0, roll_lanes(w, 1), 0.0)
        moved = 0.5 * ((u_p - u_m) + (v_p - v_m) + (w_p - w_m))
        out[64 + BLOCK * x : 64 + BLOCK * (x + 1)] = moved - source[x]
        r = EDGE + x
        out[r : r + 1] = velocity[1, x, 0:1]
        out[r + 4 : r + 5] = velocity[1, x, BLOCK - 1 : BLOCK]
    out[128:144] = velocity[0, 0]
    out[144:160] = velocity[0, 3]


def assemble(n_chips, gathered, sent, sent_far, edge):
    north, _, _ = whereabouts(n_chips)
    row = rows_of((BLOCK, LANES))
    for c in range(4):
        rows = slice(BLOCK * c, BLOCK * (c + 1))
        for k in range(2):
            block = 2 * c + k
            for x in range(4):
                sent[4 * k + x, rows] = gathered[block, BLOCK * x : BLOCK * (x + 1)]
                t = gathered[block, 64 + BLOCK * x : 64 + BLOCK * (x + 1)]
                r = EDGE + x
                if c > 0:
                    t = t - jnp.where(row == 0, 0.5 * gathered[block - 2, r + 4 : r + 5], 0.0)
                if c < 3:
                    t = t + jnp.where(row == BLOCK - 1, 0.5 * gathered[block + 2, r : r + 1], 0.0)
                if k == 0 and x == 3:
                    t = t + 0.5 * gathered[block + 1, 128:144]
                if k == 1 and x == 0:
                    t = t - 0.5 * gathered[block - 1, 144:160]
                sent[8 + 4 * k + x, rows] = t
        edge[0, rows] = gathered[2 * c, 128:144]
        edge[1, rows] = gathered[2 * c + 1, 144:160]
    u = edge[jnp.where(north, 0, 1)]
    sent[16] = u
    sent_far[0] = sent[jnp.where(north, 0, 7)]
    sent_far[1] = u


def species_edges(n_chips, species, near, beside, edge_low, edge_high):
    north, _, _ = whereabouts(n_chips)
    outward, inward = jnp.where(north, 0, 3), jnp.where(north, 3, 0)
    for s in range(SPECIES):
        near[BLOCK * s : BLOCK * (s + 1)] = species[s, outward]
        beside[BLOCK * s : BLOCK * (s + 1)] = species[s, inward]
        for x in range(4):
            r = 4 * s + x
            edge_low[r : r + 1] = species[s, x, 0:1]
            edge_high[r : r + 1] = species[s, x, BLOCK - 1 : BLOCK]
    edge_low[36:40] = jnp.zeros((4, LANES), jnp.float32)
    edge_high[36:40] = jnp.zeros((4, LANES), jnp.float32)


def flow_rims(n_chips, gathered, u_beside, v_rims):
    north, cross, _ = whereabouts(n_chips)
    core = jnp.where(north, 0, 1)
    partner = 2 * cross + jnp.where(north, 1, 0)
    u_beside[...] = jnp.where(north, gathered[partner, 128:144], gathered[partner, 144:160])
    below = gathered[2 * jnp.maximum(cross - 1, 0) + core, EDGE:OWN]
    above = gathered[2 * jnp.minimum(cross + 1, 3) + core, EDGE:OWN]
    v_rims[0:4] = jnp.where(cross > 0, below[4:8], 0.0)
    v_rims[4:8] = jnp.where(cross < 3, above[0:4], 0.0)


def first_cycle(
    n_chips, own, edge, mine, swapped, species_near,
    mobile_ref, weights_ref, pressure_ref, residual, coarse, outer, sent,
    target_w, field_ref,
):
    north, _, chip = whereabouts(n_chips)
    clear_pads(mobile_ref)
    clear_pads(field_ref)
    clear_pads(pressure_ref)
    mobile_w, pressure = Field(mobile_ref, -9), Field(pressure_ref, -8)
    field = Field(field_ref, -8)

    def sides(k):
        a, b = mine[k], swapped[k]
        return jnp.where(north, a, b), jnp.where(north, b, a)

    def copy(i):
        k, later = i.index(), (i + 8).index()
        left, right = sides(k)
        mobile_w.put(i - 8, left)
        mobile_w.put(i, own[k])
        mobile_w.put(i + 8, right)
        left, right = sides(later)
        target_w[k] = left
        target_w[later] = own[later]
        target_w[(i + 16).index()] = right

    loop(0, 8, copy)
    left, right = sides(17)
    mobile_w.put(Place(0, -9), left)
    mobile_w.put(Place(0, 16), right)
    left, right = sides(18)
    target_w[0] = target_w[0] - 0.5 * left
    target_w[23] = target_w[23] + 0.5 * right
    left, right = sides(16)
    target_w[7] = target_w[7] + 0.5 * edge[0]
    target_w[8] = target_w[8] - 0.5 * left
    target_w[15] = target_w[15] + 0.5 * right
    target_w[16] = target_w[16] - 0.5 * edge[1]
    outer[...] = mine[16]

    weights = Weights(weights_ref, 1, -8)
    weights.fill(-8, 16, mobile_w, at(target_w, -8), inside_of(8 * chip, 8 * n_chips))
    first_sweep(weights, field, -8, 16)
    sweep(weights, field, pressure, -7, 15)
    residual_planes(weights, pressure, residual, -3, -3, 7)

    def restrict(i):
        pair = mobile_w(2 * i) + mobile_w(2 * i + 1)
        coarse[(i + 4).index()] = 0.125 * pair_sum(pair)

    loop(-4, 8, restrict)
    r = jnp.where(north, 6, 0)
    sent[0:64] = packed(residual[r], residual[r + 1], residual[r + 2], residual[r + 3])
    m = jnp.where(north, 8, 0)
    sent[64:128] = packed(coarse[m], coarse[m + 1], coarse[m + 2], coarse[m + 3])
    sent[128:272] = species_near[...]


def coarse_sweeps(weights, one, two, low, high):
    first_sweep(weights, one, low, high)
    sweep(weights, one, two, low + 1, high - 1)
    sweep(weights, two, one, low + 2, high - 2)
    sweep(weights, one, two, low + 3, high - 3)


def inner(n_chips, chip):
    return chip > 0, chip < n_chips - 1


def second_cycle(
    n_chips, weights_ref, pressure_ref, residual, coarse, got,
    pressure_new_ref, residual_new, coarse_weights_ref, sent,
    coarse_ref, residual_w, one_ref, two_ref, field_ref, other_ref,
):
    north, _, chip = whereabouts(n_chips)
    for ref in (pressure_new_ref, coarse_ref, one_ref, two_ref, field_ref, other_ref):
        clear_pads(ref)
    coarse_w, one, two = Field(coarse_ref, -8), Field(one_ref, -7), Field(two_ref, -7)
    field, other = Field(field_ref, -8), Field(other_ref, -8)
    pressure, pressure_new = Field(pressure_ref, -8), Field(pressure_new_ref, -3)

    left, right = unpacked(got[0, 0:64]), unpacked(got[1, 0:64])
    for i in range(4):
        residual_w[i] = left[i]
        residual_w[14 + i] = right[i]
    left, right = unpacked(got[0, 64:128]), unpacked(got[1, 64:128])
    for i in range(4):
        coarse_w.put(Place(0, i - 8), left[i])
        coarse_w.put(Place(0, i + 8), right[i])

    def copy_residual(i):
        residual_w[(i + 4).index()] = residual[i.index()]

    def copy_coarse(i):
        coarse_w.put(i - 4, coarse[i.index()])

    loop(0, 10, copy_residual)
    loop(0, 12, copy_coarse)

    coarse_weights = Weights(coarse_weights_ref, 2, -7)
    coarse_weights.fill(-7, 11, coarse_w, at(residual_w, -7), inside_of(4 * chip, 4 * n_chips))
    coarse_sweeps(coarse_weights, one, two, -7, 11)

    def prolong(i):
        correction = two(i)
        for half in range(2):
            k = 2 * i + half
            field.put(k, pressure(k) + correction)

    loop(-4, 8, prolong)

    weights = Weights(weights_ref, 1, -8)
    sweep(weights, field, other, -6, 14)
    sweep(weights, other, field, -5, 13)
    sweep(weights, field, other, -4, 12)
    sweep(weights, other, pressure_new, -3, 11)
    residual_planes(weights, pressure_new, residual_new, -1, -1, 5)
    sent[0] = pressure_new_ref[jnp.where(north, 6, 7), PAD : PAD + ROWS]
    r = jnp.where(north, 2, 0)
    sent[1] = packed(
        residual_new[r], residual_new[r + 1], residual_new[r + 2], residual_new[r + 3]
    )


def finish(
    n_chips, mobile_ref, weights_ref, pressure, residual, coarse_weights_ref, got, swapped,
    velocity, species, outer, u_beside, v_rims, sides, y_low, y_high,
    velocity_out, pressure_out, species_out,
    residual_w, pressure_w, one_ref, two_ref, field_ref, other_ref, final_pad,
):
    north, cross, chip = whereabouts(n_chips)
    before, after = inner(n_chips, chip)
    for ref in (one_ref, two_ref, field_ref, other_ref, final_pad):
        clear_pads(ref)
    one, two = Field(one_ref, -5), Field(two_ref, -5)
    field, other, final = Field(field_ref, -4), Field(other_ref, -4), Field(final_pad, -2)
    left = unpacked(jnp.where(before, swapped[0, 0], 0.0))
    right = unpacked(jnp.where(after, swapped[1, 1], 0.0))
    for i in range(4):
        residual_w[i] = left[i]
        residual_w[10 + i] = right[i]
    for i in range(6):
        residual_w[4 + i] = residual[i]
    pressure_w[0] = jnp.where(before, got[0, 0], 0.0)
    pressure_w[15] = jnp.where(after, got[1, 0], 0.0)
    known = Field(pressure, -3)

    def copy_pressure(i):
        pressure_w[(i + 4).index()] = known(i)

    loop(-3, 11, copy_pressure)

    shift, coarse_shift = jnp.where(north, 0, 4), jnp.where(north, 0, 2)
    coarse_weights = Weights(coarse_weights_ref, 2, -7, coarse_shift, at(residual_w, -5))

    def right_side(i):
        k = (i + 5).index()
        factor = coarse_weights_ref[7, coarse_weights.place(i), 0:ROWS]
        residual_w[k] = residual_w[(i + 5).index(coarse_shift)] * factor

    for k in range(12):
        right_side(Place(0, k - 5))
    coarse_sweeps(coarse_weights, one, two, -5, 7)

    def prolong(i):
        correction = two(i)
        for half in range(2):
            k = 2 * i + half
            field.put(k, pressure_w[(k + 4).index(shift)] + correction)

    loop(-2, 4, prolong)

    weights = Weights(weights_ref, 1, -8, shift)
    sweep(weights, field, other, -3, 7)
    sweep(weights, other, final, -2, 6)

    start = pl.multiple_of(cross * BLOCK, BLOCK)
    own = pl.ds(start + 8, BLOCK)
    row, lane = rows_of((BLOCK, LANES)), lanes_of((BLOCK, LANES))

    beyond = outer[pl.ds(start, BLOCK)]
    u_low = jnp.where(north, beyond, u_beside[...])
    u_high = jnp.where(north, u_beside[...], beyond)

    def u_out(x):
        if x < 0:
            u = u_low
        elif x > 3:
            u = u_high
        else:
            u = velocity[0, x]
        slope = 0.5 * (final_pad[x + 3, own] - final_pad[x + 1, own])
        return u - mobile_ref[shift + (x + 9), own] * slope

    u = [u_out(x) for x in range(-1, 5)]

    def species_beside(s, side):
        outside = sides[side, 128 + BLOCK * s : 144 + BLOCK * s]
        inside = sides[side, 272 + BLOCK * s : 288 + BLOCK * s]
        return jnp.where(north, outside, inside) if side == 0 else jnp.where(north, inside, outside)

    wide = pl.ds(start, 32)
    for x in range(4):
        p = final_pad[x + 2, wide]
        m = mobile_ref[shift + (x + 9), wide]
        p_own = p[8:24]
        v = velocity[1, x] - m[8:24] * (0.5 * (p[9:25] - p[7:23]))
        v_low = v_rims[x : x + 1] - m[7:8] * (0.5 * (p[8:9] - p[6:7]))
        v_high = v_rims[4 + x : 5 + x] - m[24:25] * (0.5 * (p[25:26] - p[23:24]))
        p_zp = jnp.where(lane < LANES - 1, roll_lanes(p_own, -1), 0.0)
        p_zm = jnp.where(lane > 0, roll_lanes(p_own, 1), 0.0)
        w = velocity[2, x] - m[8:24] * (0.5 * (p_zp - p_zm))
        velocity_out[0, x] = u[x + 1]
        velocity_out[1, x] = v
        velocity_out[2, x] = w
        pressure_out[x] = p_own

        flow_xm, flow_xp = 0.5 * (u[x] + u[x + 1]), 0.5 * (u[x + 1] + u[x + 2])
        v_m = jnp.where(row == 0, v_low, roll_rows(v, 1))
        v_p = jnp.where(row == BLOCK - 1, v_high, roll_rows(v, -1))
        flow_ym, flow_yp = 0.5 * (v_m + v), 0.5 * (v + v_p)
        w_m = jnp.where(lane > 0, roll_lanes(w, 1), 0.0)
        w_p = jnp.where(lane < LANES - 1, roll_lanes(w, -1), 0.0)
        flow_zm, flow_zp = 0.5 * (w_m + w), 0.5 * (w + w_p)

        def leaves(high, low):
            return jnp.maximum(high, 0.0) - jnp.minimum(low, 0.0)

        keep = 1.0 - time_step * (
            leaves(flow_xp, flow_xm) + leaves(flow_yp, flow_ym) + leaves(flow_zp, flow_zm)
        )
        from_xm, from_xp = (
            time_step * jnp.maximum(flow_xm, 0.0),
            -time_step * jnp.minimum(flow_xp, 0.0),
        )
        from_ym, from_yp = (
            time_step * jnp.maximum(flow_ym, 0.0),
            -time_step * jnp.minimum(flow_yp, 0.0),
        )
        from_zm = jnp.where(lane > 0, time_step * jnp.maximum(flow_zm, 0.0), 0.0)
        from_zp = jnp.where(lane < LANES - 1, -time_step * jnp.minimum(flow_zp, 0.0), 0.0)
        for s in range(SPECIES):
            c = species[s, x]
            if x > 0:
                c_xm = species[s, x - 1]
            else:
                c_xm = species_beside(s, 0)
            if x < 3:
                c_xp = species[s, x + 1]
            else:
                c_xp = species_beside(s, 1)
            r = 4 * s + x
            c_ym = jnp.where(row == 0, y_low[r : r + 1], roll_rows(c, 1))
            c_yp = jnp.where(row == BLOCK - 1, y_high[r : r + 1], roll_rows(c, -1))
            total = keep * c + (from_xm * c_xm + from_xp * c_xp)
            total = total + (from_ym * c_ym + from_yp * c_yp)
            total = total + (from_zm * roll_lanes(c, 1) + from_zp * roll_lanes(c, -1))
            species_out[s, x] = total


def call(kernel, outs, scratch, *operands, where=pltpu.VMEM, semaphores=0, grant=24):
    vmem = pl.BlockSpec(memory_space=pltpu.VMEM)
    shapes = [jax.ShapeDtypeStruct(shape, jnp.float32) for shape in outs]
    scratch = [pltpu.VMEM(shape, jnp.float32) for shape in scratch]
    if semaphores:
        scratch = [*scratch, pltpu.SemaphoreType.DMA((semaphores,))]
    return pl.pallas_call(
        kernel,
        out_shape=shapes,
        in_specs=[pl.BlockSpec(memory_space=where) for _ in operands],
        out_specs=[vmem for _ in outs],
        scratch_shapes=scratch,
        cost_estimate=pl.CostEstimate(flops=1000000, bytes_accessed=1000000, transcendentals=0),
        compiler_params=pltpu.CompilerParams(vmem_limit_bytes=grant * 2**20),
        interpret=INTERPRET,
    )(*operands)


def gathered_over(array, groups):
    return lax.all_gather(array, ("slab", "cross"), axis_index_groups=groups)


def local(n_chips, velocity, density, source, species):
    def device(slab, cross):
        return 4 * slab + cross

    chips = [[device(2 * j + k, c) for c in range(4) for k in range(2)] for j in range(n_chips)]
    cores = [
        [device(2 * j, c), device(2 * j + 1, c)] for j in range(n_chips) for c in range(4)
    ]
    facing = [
        [device(2 * j + 1, c), device(2 * j + 2, c)] for j in range(n_chips - 1) for c in range(4)
    ]
    for slab in (0, 2 * n_chips - 1):
        facing += [[device(slab, 0), device(slab, 1)], [device(slab, 2), device(slab, 3)]]

    def beside(distance):
        pairs = []
        for j in range(n_chips - distance):
            left, right = 2 * j + 1, 2 * (j + distance)
            pairs += [(left, right), (right, left)]
        return pairs

    within = [pair for j in range(n_chips) for pair in ((2 * j, 2 * j + 1), (2 * j + 1, 2 * j))]
    upward = [(c, c + 1) for c in range(3)]
    downward = [(c + 1, c) for c in range(3)]

    def plane(n):
        return (n, ROWS, LANES)

    def padded(n):
        return (n, *PADDED)

    def skewed(n):
        return (8, n + (1 - n) % 4, ROWS + 8, LANES)

    def bind(kernel):
        return functools.partial(kernel, n_chips)

    (own,) = call(
        prepare, [(OWN, LANES)], [velocity.shape, density.shape, source.shape],
        velocity, density, source,
        where=HBM, semaphores=3, grant=63,
    )
    gathered = gathered_over(own, chips)
    sent, sent_far, edge = call(bind(assemble), [plane(17), plane(2), plane(2)], [], gathered)
    near = lax.ppermute(sent, "slab", beside(1))
    far = lax.ppermute(sent_far, "slab", beside(2))
    species_near, species_beside, edge_low, edge_high = call(
        bind(species_edges), [(144, LANES), (144, LANES), (40, LANES), (40, LANES)], [], species
    )
    mine = jnp.concatenate([near, far], 0)
    swapped = lax.ppermute(mine, "slab", within)
    mobile_w, weights, pressure, residual, coarse, outer, sent_two = call(
        bind(first_cycle),
        [
            padded(26), skewed(24), padded(24), plane(10), plane(12), PLANE, (272, LANES),
        ],
        [plane(24), padded(24)],
        sent, edge, mine, swapped, species_near,
    )
    near = lax.ppermute(sent_two, "slab", beside(1))
    y_low = lax.ppermute(edge_high, "cross", upward)
    y_high = lax.ppermute(edge_low, "cross", downward)
    u_beside, v_rims = call(bind(flow_rims), [(BLOCK, LANES), (8, LANES)], [], gathered)
    sides = gathered_over(jnp.concatenate([near, species_beside], 0), cores)
    pressure, residual, coarse_weights, sent = call(
        bind(second_cycle),
        [padded(14), plane(6), skewed(18), plane(2)],
        [padded(20), plane(18), padded(18), padded(18), padded(24), padded(24)],
        weights, pressure, residual, coarse, sides,
    )
    near = gathered_over(sent, facing)
    swapped = gathered_over(near[:, 1], cores)
    return call(
        bind(finish),
        [velocity.shape, density.shape, species.shape],
        [plane(14), plane(16), padded(12), padded(12), padded(12), padded(12), padded(8)],
        mobile_w, weights, pressure, residual, coarse_weights, near, swapped,
        velocity, species, outer, u_beside, v_rims, sides, y_low, y_high,
    )


def solution(mesh):
    n_chips = mesh.shape["slab"] // 2
    block = P("slab", "cross", None)
    stack = P(None, "slab", "cross", None)

    def step(*arrays):
        return tuple(local(n_chips, *arrays))

    return jax.shard_map(
        step,
        mesh=mesh,
        in_specs=(stack, block, block, stack),
        out_specs=(stack, block, stack),
        check_vma=False,
    )
```

```python
import functools

import jax
import jax.numpy as jnp
from jax import lax
from jax.experimental import pallas as pl
from jax.experimental.pallas import tpu as pltpu
from jax.sharding import PartitionSpec as P


INTERPRET = False
HBM = pltpu.HBM
ROWS = 64
LANES = 128
BLOCK = 16
SPECIES = 9
EDGE = 160
OWN = EDGE + 8
damping = 0.8
time_step = 0.25


class Place:
    def __init__(self, counter, constant):
        self.counter = counter
        self.constant = constant

    def __add__(self, other):
        return Place(self.counter, self.constant + other)

    def __sub__(self, other):
        return Place(self.counter, self.constant - other)

    def __rmul__(self, factor):
        return Place(self.counter * factor, self.constant * factor)

    def index(self, shift=None):
        start = self.counter if shift is None else self.counter + shift
        return start + self.constant


def loop(low, high, body):
    for u in range(high - low):
        body(Place(0, low + u))


def rows_of(shape):
    return lax.broadcasted_iota(jnp.int32, shape, 0)


def lanes_of(shape):
    return lax.broadcasted_iota(jnp.int32, shape, 1)


PLANE = (ROWS, LANES)


def roll_rows(x, by):
    return pltpu.roll(x, by % x.shape[0], 0)


def roll_lanes(x, by):
    return pltpu.roll(x, by % x.shape[1], 1)


PAD = 8
PADDED = (ROWS + 2 * PAD, LANES)


class Field:
    def __init__(self, ref, low, shift=None):
        self.ref = ref
        self.low = low
        self.shift = shift

    def __call__(self, i, rows=0):
        k = (i - self.low).index(self.shift)
        return self.ref[k, PAD + rows : PAD + rows + ROWS]

    def put(self, i, value):
        self.ref[(i - self.low).index(), PAD : PAD + ROWS] = value


def clear_pads(ref):
    nothing = jnp.zeros((PAD, LANES), jnp.float32)
    for k in range(ref.shape[0]):
        ref[k, 0:PAD] = nothing
        ref[k, PAD + ROWS :] = nothing


class Weights:
    def __init__(self, ref, step, low, shift=None, constant=None):
        self.ref = ref
        self.step = step
        self.low = low
        self.shift = shift
        self.constant = constant

    def place(self, i):
        return (i - self.low).index(self.shift)

    def fill(self, low, high, mobile, target, inside):
        s = self.step
        lane = lanes_of(PLANE)
        z_low, z_high = lane >= s, lane < LANES - s

        def body(i):
            m = mobile(i)
            x_m, x_p = mobile(i - 1), mobile(i + 1)
            y_m, y_p = mobile(i, -s), mobile(i, s)
            z_m = jnp.where(z_low, roll_lanes(m, s), 0.0)
            z_p = jnp.where(z_high, roll_lanes(m, -s), 0.0)
            diagonal = 3.0 * m + 0.5 * ((x_m + x_p) + (y_m + y_p) + (z_m + z_p))
            valid = inside(i)
            scaled = (damping * valid) / (diagonal + (1.0 - valid))
            half = 0.5 * scaled
            k = self.place(i)
            self.ref[0, k] = (m + x_m) * half
            self.ref[1, k] = (m + x_p) * half
            self.ref[2, k] = (m + y_m) * half
            self.ref[3, k] = (m + y_p) * half
            self.ref[4, k] = jnp.where(z_low, (m + z_m) * half, 0.0)
            self.ref[5, k] = jnp.where(z_high, (m + z_p) * half, 0.0)
            if s == 1:
                self.ref[6, k] = target(i) * scaled
                self.ref[7, k] = diagonal * (1.0 / damping)
            else:
                self.ref[6, k] = target(i) * (4.0 * scaled)
                self.ref[7, k] = 4.0 * scaled

        loop(low, high, body)

    def side(self, i):
        if self.constant is not None:
            return self.constant(i)
        return self.ref[6, self.place(i)]

    def change(self, field, i):
        s = self.step
        k = self.place(i)
        p = field(i)
        total = self.ref[0, k] * field(i - 1) + self.ref[1, k] * field(i + 1)
        total = total + (self.ref[2, k] * field(i, -s) + self.ref[3, k] * field(i, s))
        total = total + (self.ref[4, k] * roll_lanes(p, s) + self.ref[5, k] * roll_lanes(p, -s))
        return p, (total - self.side(i)) - damping * p


def at(ref, origin, shift=None):
    return lambda i: ref[(i - origin).index(shift)]


def sweep(weights, source, result, low, high):
    def body(i):
        p, change = weights.change(source, i)
        result.put(i, p + change)

    loop(low, high, body)


def first_sweep(weights, result, low, high):
    def body(i):
        result.put(i, -weights.side(i))

    loop(low, high, body)


def pair_sum(q):
    row, lane = rows_of(PLANE), lanes_of(PLANE)
    q = q + jnp.where(lane % 2 == 0, roll_lanes(q, -1), roll_lanes(q, 1))
    return q + jnp.where(row % 2 == 0, roll_rows(q, -1), roll_rows(q, 1))


def packed(a, b, c, d):
    row, lane = rows_of(PLANE), lanes_of(PLANE)
    even = lane % 2 == 0
    return jnp.where(row % 2 == 0, jnp.where(even, a, b), jnp.where(even, c, d))


def unpacked(v):
    row, lane = rows_of(PLANE), lanes_of(PLANE)
    even, upper = lane % 2 == 0, row % 2 == 0
    first = jnp.where(even, v, roll_lanes(v, 1))
    second = jnp.where(even, roll_lanes(v, -1), v)

    def low_row(x):
        return jnp.where(upper, x, roll_rows(x, 1))

    def high_row(x):
        return jnp.where(upper, roll_rows(x, -1), x)

    return low_row(first), low_row(second), high_row(first), high_row(second)


def residual_planes(weights, field, result, result_low, low, high):
    def body(i):
        total = 0.0
        for half in range(2):
            _, change = weights.change(field, 2 * i + half)
            total = total - change * weights.ref[7, weights.place(2 * i + half)]
        result[(i - result_low).index()] = 0.125 * pair_sum(total)

    loop(low, high, body)


def inside_of(first, count):
    def inside(i):
        place = i.index(first)
        return jnp.where((place >= 0) & (place < count), 1.0, 0.0)

    return inside


def whereabouts(n_chips):
    slab, cross = lax.axis_index("slab"), lax.axis_index("cross")
    chip = jnp.minimum(jnp.maximum(slab // 2, 0), n_chips - 1)
    return slab % 2 == 0, jnp.minimum(jnp.maximum(cross, 0), 3), chip


def prepare(velocity_in, density_in, source_in, out, velocity, density, source, semaphore):
    copies = [
        pltpu.make_async_copy(there, here, semaphore.at[k])
        for k, (there, here) in enumerate(
            [(density_in, density), (velocity_in, velocity), (source_in, source)]
        )
    ]
    for copy in copies:
        copy.start()
    lane = lanes_of((BLOCK, LANES))
    row = rows_of((BLOCK, LANES))
    copies[0].wait()
    for x in range(4):
        out[BLOCK * x : BLOCK * (x + 1)] = 1.0 / density[x]
    copies[1].wait()
    copies[2].wait()
    for x in range(4):
        u_p = velocity[0, x + 1] if x < 3 else 0.0
        u_m = velocity[0, x - 1] if x > 0 else 0.0
        v, w = velocity[1, x], velocity[2, x]
        v_p = jnp.where(row < BLOCK - 1, roll_rows(v, -1), 0.0)
        v_m = jnp.where(row > 0, roll_rows(v, 1), 0.0)
        w_p = jnp.where(lane < LANES - 1, roll_lanes(w, -1), 0.0)
        w_m = jnp.where(lane > 0, roll_lanes(w, 1), 0.0)
        moved = 0.5 * ((u_p - u_m) + (v_p - v_m) + (w_p - w_m))
        out[64 + BLOCK * x : 64 + BLOCK * (x + 1)] = moved - source[x]
        r = EDGE + x
        out[r : r + 1] = velocity[1, x, 0:1]
        out[r + 4 : r + 5] = velocity[1, x, BLOCK - 1 : BLOCK]
    out[128:144] = velocity[0, 0]
    out[144:160] = velocity[0, 3]


def assemble(n_chips, gathered, sent, sent_far, edge):
    north, _, _ = whereabouts(n_chips)
    row = rows_of((BLOCK, LANES))
    for c in range(4):
        rows = slice(BLOCK * c, BLOCK * (c + 1))
        for k in range(2):
            block = 2 * c + k
            for x in range(4):
                sent[4 * k + x, rows] = gathered[block, BLOCK * x : BLOCK * (x + 1)]
                t = gathered[block, 64 + BLOCK * x : 64 + BLOCK * (x + 1)]
                r = EDGE + x
                if c > 0:
                    t = t - jnp.where(row == 0, 0.5 * gathered[block - 2, r + 4 : r + 5], 0.0)
                if c < 3:
                    t = t + jnp.where(row == BLOCK - 1, 0.5 * gathered[block + 2, r : r + 1], 0.0)
                if k == 0 and x == 3:
                    t = t + 0.5 * gathered[block + 1, 128:144]
                if k == 1 and x == 0:
                    t = t - 0.5 * gathered[block - 1, 144:160]
                sent[8 + 4 * k + x, rows] = t
        edge[0, rows] = gathered[2 * c, 128:144]
        edge[1, rows] = gathered[2 * c + 1, 144:160]
    u = edge[jnp.where(north, 0, 1)]
    sent[16] = u
    sent_far[0] = sent[jnp.where(north, 0, 7)]
    sent_far[1] = u


def species_edges(n_chips, species, near, beside, edge_low, edge_high):
    north, _, _ = whereabouts(n_chips)
    outward, inward = jnp.where(north, 0, 3), jnp.where(north, 3, 0)
    for s in range(SPECIES):
        near[BLOCK * s : BLOCK * (s + 1)] = species[s, outward]
        beside[BLOCK * s : BLOCK * (s + 1)] = species[s, inward]
        for x in range(4):
            r = 4 * s + x
            edge_low[r : r + 1] = species[s, x, 0:1]
            edge_high[r : r + 1] = species[s, x, BLOCK - 1 : BLOCK]
    edge_low[36:40] = jnp.zeros((4, LANES), jnp.float32)
    edge_high[36:40] = jnp.zeros((4, LANES), jnp.float32)


def flow_rims(n_chips, gathered, u_beside, v_rims):
    north, cross, _ = whereabouts(n_chips)
    core = jnp.where(north, 0, 1)
    partner = 2 * cross + jnp.where(north, 1, 0)
    u_beside[...] = jnp.where(north, gathered[partner, 128:144], gathered[partner, 144:160])
    below = gathered[2 * jnp.maximum(cross - 1, 0) + core, EDGE:OWN]
    above = gathered[2 * jnp.minimum(cross + 1, 3) + core, EDGE:OWN]
    v_rims[0:4] = jnp.where(cross > 0, below[4:8], 0.0)
    v_rims[4:8] = jnp.where(cross < 3, above[0:4], 0.0)


def first_cycle(
    n_chips, own, edge, mine, swapped, species_near,
    mobile_ref, weights_ref, pressure_ref, residual, coarse, outer, sent,
    target_w, field_ref,
):
    north, _, chip = whereabouts(n_chips)
    clear_pads(mobile_ref)
    clear_pads(field_ref)
    clear_pads(pressure_ref)
    mobile_w, pressure = Field(mobile_ref, -9), Field(pressure_ref, -8)
    field = Field(field_ref, -8)

    def sides(k):
        a, b = mine[k], swapped[k]
        return jnp.where(north, a, b), jnp.where(north, b, a)

    def copy(i):
        k, later = i.index(), (i + 8).index()
        left, right = sides(k)
        mobile_w.put(i - 8, left)
        mobile_w.put(i, own[k])
        mobile_w.put(i + 8, right)
        left, right = sides(later)
        target_w[k] = left
        target_w[later] = own[later]
        target_w[(i + 16).index()] = right

    loop(0, 8, copy)
    left, right = sides(17)
    mobile_w.put(Place(0, -9), left)
    mobile_w.put(Place(0, 16), right)
    left, right = sides(18)
    target_w[0] = target_w[0] - 0.5 * left
    target_w[23] = target_w[23] + 0.5 * right
    left, right = sides(16)
    target_w[7] = target_w[7] + 0.5 * edge[0]
    target_w[8] = target_w[8] - 0.5 * left
    target_w[15] = target_w[15] + 0.5 * right
    target_w[16] = target_w[16] - 0.5 * edge[1]
    outer[...] = mine[16]

    weights = Weights(weights_ref, 1, -8)
    weights.fill(-8, 16, mobile_w, at(target_w, -8), inside_of(8 * chip, 8 * n_chips))
    first_sweep(weights, field, -8, 16)
    sweep(weights, field, pressure, -7, 15)
    residual_planes(weights, pressure, residual, -3, -3, 7)

    def restrict(i):
        pair = mobile_w(2 * i) + mobile_w(2 * i + 1)
        coarse[(i + 4).index()] = 0.125 * pair_sum(pair)

    loop(-4, 8, restrict)
    r = jnp.where(north, 6, 0)
    sent[0:64] = packed(residual[r], residual[r + 1], residual[r + 2], residual[r + 3])
    m = jnp.where(north, 8, 0)
    sent[64:128] = packed(coarse[m], coarse[m + 1], coarse[m + 2], coarse[m + 3])
    sent[128:272] = species_near[...]


def coarse_sweeps(weights, one, two, low, high):
    first_sweep(weights, one, low, high)
    sweep(weights, one, two, low + 1, high - 1)
    sweep(weights, two, one, low + 2, high - 2)
    sweep(weights, one, two, low + 3, high - 3)


def inner(n_chips, chip):
    return chip > 0, chip < n_chips - 1


def second_cycle(
    n_chips, weights_ref, pressure_ref, residual, coarse, got,
    pressure_new_ref, residual_new, coarse_weights_ref, sent,
    coarse_ref, residual_w, one_ref, two_ref, field_ref, other_ref,
):
    north, _, chip = whereabouts(n_chips)
    before, after = inner(n_chips, chip)
    for ref in (pressure_new_ref, coarse_ref, one_ref, two_ref, field_ref, other_ref):
        clear_pads(ref)
    coarse_w, one, two = Field(coarse_ref, -8), Field(one_ref, -7), Field(two_ref, -7)
    field, other = Field(field_ref, -8), Field(other_ref, -8)
    pressure, pressure_new = Field(pressure_ref, -8), Field(pressure_new_ref, -3)

    left = unpacked(jnp.where(before, got[0, 0:64], 0.0))
    right = unpacked(jnp.where(after, got[1, 272:336], 0.0))
    for i in range(4):
        residual_w[i] = left[i]
        residual_w[14 + i] = right[i]
    left = unpacked(jnp.where(before, got[0, 64:128], 0.0))
    right = unpacked(jnp.where(after, got[1, 336:400], 0.0))
    for i in range(4):
        coarse_w.put(Place(0, i - 8), left[i])
        coarse_w.put(Place(0, i + 8), right[i])

    def copy_residual(i):
        residual_w[(i + 4).index()] = residual[i.index()]

    def copy_coarse(i):
        coarse_w.put(i - 4, coarse[i.index()])

    loop(0, 10, copy_residual)
    loop(0, 12, copy_coarse)

    coarse_weights = Weights(coarse_weights_ref, 2, -7)
    coarse_weights.fill(-7, 11, coarse_w, at(residual_w, -7), inside_of(4 * chip, 4 * n_chips))
    coarse_sweeps(coarse_weights, one, two, -7, 11)

    def prolong(i):
        correction = two(i)
        for half in range(2):
            k = 2 * i + half
            field.put(k, pressure(k) + correction)

    loop(-4, 8, prolong)

    weights = Weights(weights_ref, 1, -8)
    sweep(weights, field, other, -6, 14)
    sweep(weights, other, field, -5, 13)
    sweep(weights, field, other, -4, 12)
    sweep(weights, other, pressure_new, -3, 11)
    residual_planes(weights, pressure_new, residual_new, -1, -1, 5)
    sent[0] = pressure_new_ref[jnp.where(north, 6, 7), PAD : PAD + ROWS]
    r = jnp.where(north, 2, 0)
    sent[1] = packed(
        residual_new[r], residual_new[r + 1], residual_new[r + 2], residual_new[r + 3]
    )


def finish(
    n_chips, mobile_ref, weights_ref, pressure, residual, coarse_weights_ref, got, swapped,
    velocity, species, outer, u_beside, v_rims, sides, y_low, y_high,
    velocity_out, pressure_out, species_out,
    residual_w, pressure_w, one_ref, two_ref, field_ref, other_ref, final_pad,
):
    north, cross, chip = whereabouts(n_chips)
    before, after = inner(n_chips, chip)
    for ref in (one_ref, two_ref, field_ref, other_ref, final_pad):
        clear_pads(ref)
    one, two = Field(one_ref, -5), Field(two_ref, -5)
    field, other, final = Field(field_ref, -4), Field(other_ref, -4), Field(final_pad, -2)
    left = unpacked(jnp.where(before, swapped[0, 0], 0.0))
    right = unpacked(jnp.where(after, swapped[1, 1], 0.0))
    for i in range(4):
        residual_w[i] = left[i]
        residual_w[10 + i] = right[i]
    for i in range(6):
        residual_w[4 + i] = residual[i]
    pressure_w[0] = jnp.where(before, got[0, 0], 0.0)
    pressure_w[15] = jnp.where(after, got[1, 0], 0.0)
    known = Field(pressure, -3)

    def copy_pressure(i):
        pressure_w[(i + 4).index()] = known(i)

    loop(-3, 11, copy_pressure)

    shift, coarse_shift = jnp.where(north, 0, 4), jnp.where(north, 0, 2)
    coarse_weights = Weights(coarse_weights_ref, 2, -7, coarse_shift, at(residual_w, -5))

    def right_side(i):
        k = (i + 5).index()
        factor = coarse_weights_ref[7, coarse_weights.place(i)]
        residual_w[k] = residual_w[(i + 5).index(coarse_shift)] * factor

    for k in range(12):
        right_side(Place(0, k - 5))
    coarse_sweeps(coarse_weights, one, two, -5, 7)

    def prolong(i):
        correction = two(i)
        for half in range(2):
            k = 2 * i + half
            field.put(k, pressure_w[(k + 4).index(shift)] + correction)

    loop(-2, 4, prolong)

    weights = Weights(weights_ref, 1, -8, shift)
    sweep(weights, field, other, -3, 7)
    sweep(weights, other, final, -2, 6)

    start = pl.multiple_of(cross * BLOCK, BLOCK)
    own = pl.ds(start + 8, BLOCK)
    row, lane = rows_of((BLOCK, LANES)), lanes_of((BLOCK, LANES))

    beyond = outer[pl.ds(start, BLOCK)]
    u_low = jnp.where(north, beyond, u_beside[...])
    u_high = jnp.where(north, u_beside[...], beyond)

    def u_out(x):
        if x < 0:
            u = u_low
        elif x > 3:
            u = u_high
        else:
            u = velocity[0, x]
        slope = 0.5 * (final_pad[x + 3, own] - final_pad[x + 1, own])
        return u - mobile_ref[shift + (x + 9), own] * slope

    u = [u_out(x) for x in range(-1, 5)]

    def species_beside(s, side):
        at_rim = BLOCK * s + (128 if side == 0 else 400)
        outside = sides[side, at_rim : at_rim + BLOCK]
        outside = jnp.where(before if side == 0 else after, outside, 0.0)
        inside = sides[side, 544 + BLOCK * s : 560 + BLOCK * s]
        return jnp.where(north, outside, inside) if side == 0 else jnp.where(north, inside, outside)

    wide = pl.ds(start, 32)
    for x in range(4):
        p = final_pad[x + 2, wide]
        m = mobile_ref[shift + (x + 9), wide]
        p_own = p[8:24]
        v = velocity[1, x] - m[8:24] * (0.5 * (p[9:25] - p[7:23]))
        v_low = v_rims[x : x + 1] - m[7:8] * (0.5 * (p[8:9] - p[6:7]))
        v_high = v_rims[4 + x : 5 + x] - m[24:25] * (0.5 * (p[25:26] - p[23:24]))
        p_zp = jnp.where(lane < LANES - 1, roll_lanes(p_own, -1), 0.0)
        p_zm = jnp.where(lane > 0, roll_lanes(p_own, 1), 0.0)
        w = velocity[2, x] - m[8:24] * (0.5 * (p_zp - p_zm))
        velocity_out[0, x] = u[x + 1]
        velocity_out[1, x] = v
        velocity_out[2, x] = w
        pressure_out[x] = p_own

        flow_xm, flow_xp = 0.5 * (u[x] + u[x + 1]), 0.5 * (u[x + 1] + u[x + 2])
        v_m = jnp.where(row == 0, v_low, roll_rows(v, 1))
        v_p = jnp.where(row == BLOCK - 1, v_high, roll_rows(v, -1))
        flow_ym, flow_yp = 0.5 * (v_m + v), 0.5 * (v + v_p)
        w_m = jnp.where(lane > 0, roll_lanes(w, 1), 0.0)
        w_p = jnp.where(lane < LANES - 1, roll_lanes(w, -1), 0.0)
        flow_zm, flow_zp = 0.5 * (w_m + w), 0.5 * (w + w_p)

        def leaves(high, low):
            return jnp.maximum(high, 0.0) - jnp.minimum(low, 0.0)

        keep = 1.0 - time_step * (
            leaves(flow_xp, flow_xm) + leaves(flow_yp, flow_ym) + leaves(flow_zp, flow_zm)
        )
        from_xm, from_xp = (
            time_step * jnp.maximum(flow_xm, 0.0),
            -time_step * jnp.minimum(flow_xp, 0.0),
        )
        from_ym, from_yp = (
            time_step * jnp.maximum(flow_ym, 0.0),
            -time_step * jnp.minimum(flow_yp, 0.0),
        )
        from_zm = jnp.where(lane > 0, time_step * jnp.maximum(flow_zm, 0.0), 0.0)
        from_zp = jnp.where(lane < LANES - 1, -time_step * jnp.minimum(flow_zp, 0.0), 0.0)
        for s in range(SPECIES):
            c = species[s, x]
            if x > 0:
                c_xm = species[s, x - 1]
            else:
                c_xm = species_beside(s, 0)
            if x < 3:
                c_xp = species[s, x + 1]
            else:
                c_xp = species_beside(s, 1)
            r = 4 * s + x
            c_ym = jnp.where(row == 0, y_low[r : r + 1], roll_rows(c, 1))
            c_yp = jnp.where(row == BLOCK - 1, y_high[r : r + 1], roll_rows(c, -1))
            total = keep * c + (from_xm * c_xm + from_xp * c_xp)
            total = total + (from_ym * c_ym + from_yp * c_yp)
            total = total + (from_zm * roll_lanes(c, 1) + from_zp * roll_lanes(c, -1))
            species_out[s, x] = total


def call(kernel, outs, scratch, *operands, where=pltpu.VMEM, semaphores=0, grant=24):
    vmem = pl.BlockSpec(memory_space=pltpu.VMEM)
    shapes = [jax.ShapeDtypeStruct(shape, jnp.float32) for shape in outs]
    scratch = [pltpu.VMEM(shape, jnp.float32) for shape in scratch]
    if semaphores:
        scratch = [*scratch, pltpu.SemaphoreType.DMA((semaphores,))]
    return pl.pallas_call(
        kernel,
        out_shape=shapes,
        in_specs=[pl.BlockSpec(memory_space=where) for _ in operands],
        out_specs=[vmem for _ in outs],
        scratch_shapes=scratch,
        cost_estimate=pl.CostEstimate(flops=1000000, bytes_accessed=1000000, transcendentals=0),
        compiler_params=pltpu.CompilerParams(vmem_limit_bytes=grant * 2**20),
        interpret=INTERPRET,
    )(*operands)


def gathered_over(array, groups):
    return lax.all_gather(array, ("slab", "cross"), axis_index_groups=groups)


def local(n_chips, velocity, density, source, species):
    def device(slab, cross):
        return 4 * slab + cross

    chips = [[device(2 * j + k, c) for c in range(4) for k in range(2)] for j in range(n_chips)]
    cores = [
        [device(2 * j, c), device(2 * j + 1, c)] for j in range(n_chips) for c in range(4)
    ]
    facing = [
        [device(2 * j + 1, c), device(2 * j + 2, c)] for j in range(n_chips - 1) for c in range(4)
    ]
    for slab in (0, 2 * n_chips - 1):
        facing += [[device(slab, 0), device(slab, 1)], [device(slab, 2), device(slab, 3)]]

    def beside(distance):
        pairs = []
        for j in range(n_chips - distance):
            left, right = 2 * j + 1, 2 * (j + distance)
            pairs += [(left, right), (right, left)]
        return pairs

    within = [pair for j in range(n_chips) for pair in ((2 * j, 2 * j + 1), (2 * j + 1, 2 * j))]
    upward = [(c, c + 1) for c in range(3)]
    downward = [(c + 1, c) for c in range(3)]

    def plane(n):
        return (n, ROWS, LANES)

    def padded(n):
        return (n, *PADDED)

    def bind(kernel):
        return functools.partial(kernel, n_chips)

    (own,) = call(
        prepare, [(OWN, LANES)], [velocity.shape, density.shape, source.shape],
        velocity, density, source,
        where=HBM, semaphores=3, grant=63,
    )
    gathered = gathered_over(own, chips)
    sent, sent_far, edge = call(bind(assemble), [plane(17), plane(2), plane(2)], [], gathered)
    near = lax.ppermute(sent, "slab", beside(1))
    far = lax.ppermute(sent_far, "slab", beside(2))
    species_near, species_beside, edge_low, edge_high = call(
        bind(species_edges), [(144, LANES), (144, LANES), (40, LANES), (40, LANES)], [], species
    )
    y_low = lax.ppermute(edge_high, "cross", upward)
    y_high = lax.ppermute(edge_low, "cross", downward)
    u_beside, v_rims = call(bind(flow_rims), [(BLOCK, LANES), (8, LANES)], [], gathered)
    mine = jnp.concatenate([near, far], 0)
    swapped = lax.ppermute(mine, "slab", within)
    mobile_w, weights, pressure, residual, coarse, outer, sent_two = call(
        bind(first_cycle),
        [
            padded(26), (8, *plane(24)), padded(24), plane(10), plane(12), PLANE, (272, LANES),
        ],
        [plane(24), padded(24)],
        sent, edge, mine, swapped, species_near,
    )
    near = gathered_over(sent_two, facing).reshape(544, LANES)
    sides = gathered_over(jnp.concatenate([near, species_beside], 0), cores)
    pressure, residual, coarse_weights, sent = call(
        bind(second_cycle),
        [padded(14), plane(6), (8, *plane(18)), plane(2)],
        [padded(20), plane(18), padded(18), padded(18), padded(24), padded(24)],
        weights, pressure, residual, coarse, sides,
    )
    near = gathered_over(sent, facing)
    swapped = gathered_over(near[:, 1], cores)
    return call(
        bind(finish),
        [velocity.shape, density.shape, species.shape],
        [plane(14), plane(16), padded(12), padded(12), padded(12), padded(12), padded(8)],
        mobile_w, weights, pressure, residual, coarse_weights, near, swapped,
        velocity, species, outer, u_beside, v_rims, sides, y_low, y_high,
    )


def solution(mesh):
    n_chips = mesh.shape["slab"] // 2
    block = P("slab", "cross", None)
    stack = P(None, "slab", "cross", None)

    def step(*arrays):
        return tuple(local(n_chips, *arrays))

    return jax.shard_map(
        step,
        mesh=mesh,
        in_specs=(stack, block, block, stack),
        out_specs=(stack, block, stack),
        check_vma=False,
    )
```

```python
import functools

import jax
import jax.numpy as jnp
from jax import lax
from jax.experimental import pallas as pl
from jax.experimental.pallas import tpu as pltpu
from jax.sharding import PartitionSpec as P


INTERPRET = False
HBM = pltpu.HBM
ROWS = 64
LANES = 128
BLOCK = 16
SPECIES = 9
EDGE = 160
OWN = EDGE + 8
damping = 0.8
time_step = 0.25


class Place:
    def __init__(self, counter, constant):
        self.counter = counter
        self.constant = constant

    def __add__(self, other):
        return Place(self.counter, self.constant + other)

    def __sub__(self, other):
        return Place(self.counter, self.constant - other)

    def __rmul__(self, factor):
        return Place(self.counter * factor, self.constant * factor)

    def index(self, shift=None):
        start = self.counter if shift is None else self.counter + shift
        return start + self.constant


def loop(low, high, body):
    for u in range(high - low):
        body(Place(0, low + u))


def rows_of(shape):
    return lax.broadcasted_iota(jnp.int32, shape, 0)


def lanes_of(shape):
    return lax.broadcasted_iota(jnp.int32, shape, 1)


PLANE = (ROWS, LANES)


def roll_rows(x, by):
    return pltpu.roll(x, by % x.shape[0], 0)


def roll_lanes(x, by):
    return pltpu.roll(x, by % x.shape[1], 1)


PAD = 8
HALF = ROWS // 2


class Field:
    def __init__(self, ref, low, shift=None):
        self.ref = ref
        self.low = low
        self.shift = shift
        self.rows = ref.shape[1] - 2 * PAD

    def __call__(self, i, rows=0):
        k = (i - self.low).index(self.shift)
        return self.ref[k, PAD + rows : PAD + rows + self.rows]

    def put(self, i, value):
        self.ref[(i - self.low).index(), PAD : PAD + self.rows] = value

    def every_other(self, i, first):
        return self.ref[(i - self.low).index(), pl.ds(PAD + first, HALF, stride=2)]

    def put_every_other(self, i, first, value):
        self.ref[(i - self.low).index(), pl.ds(PAD + first, HALF, stride=2)] = value


def clear_pads(ref):
    nothing = jnp.zeros((PAD, LANES), jnp.float32)
    for k in range(ref.shape[0]):
        ref[k, 0:PAD] = nothing
        ref[k, ref.shape[1] - PAD :] = nothing


class Weights:
    def __init__(self, ref, step, low, shift=None, constant=None):
        self.ref = ref
        self.step = step
        self.low = low
        self.shift = shift
        self.constant = constant

    def place(self, i):
        return (i - self.low).index(self.shift)

    def fill(self, low, high, mobile, target, inside):
        s = self.step
        lane = lanes_of((mobile.rows, LANES))
        z_low, z_high = lane >= s, lane < LANES - s

        def body(i):
            m = mobile(i)
            x_m, x_p = mobile(i - 1), mobile(i + 1)
            y_m, y_p = mobile(i, -1), mobile(i, 1)
            z_m = jnp.where(z_low, roll_lanes(m, s), 0.0)
            z_p = jnp.where(z_high, roll_lanes(m, -s), 0.0)
            diagonal = 3.0 * m + 0.5 * ((x_m + x_p) + (y_m + y_p) + (z_m + z_p))
            valid = inside(i)
            scaled = (damping * valid) / (diagonal + (1.0 - valid))
            half = 0.5 * scaled
            k = self.place(i)
            self.ref[0, k] = (m + x_m) * half
            self.ref[1, k] = (m + x_p) * half
            self.ref[2, k] = (m + y_m) * half
            self.ref[3, k] = (m + y_p) * half
            self.ref[4, k] = jnp.where(z_low, (m + z_m) * half, 0.0)
            self.ref[5, k] = jnp.where(z_high, (m + z_p) * half, 0.0)
            if s == 1:
                self.ref[6, k] = target(i) * scaled
                self.ref[7, k] = diagonal * (1.0 / damping)
            else:
                self.ref[6, k] = target(i) * (4.0 * scaled)
                self.ref[7, k] = 4.0 * scaled

        loop(low, high, body)

    def side(self, i):
        if self.constant is not None:
            return self.constant(i)
        return self.ref[6, self.place(i)]

    def change(self, field, i):
        s = self.step
        k = self.place(i)
        p = field(i)
        total = self.ref[0, k] * field(i - 1) + self.ref[1, k] * field(i + 1)
        total = total + (self.ref[2, k] * field(i, -1) + self.ref[3, k] * field(i, 1))
        total = total + (self.ref[4, k] * roll_lanes(p, s) + self.ref[5, k] * roll_lanes(p, -s))
        return p, (total - self.side(i)) - damping * p


def at(ref, origin, shift=None):
    return lambda i: ref[(i - origin).index(shift)]


def sweep(weights, source, result, low, high):
    def body(i):
        p, change = weights.change(source, i)
        result.put(i, p + change)

    loop(low, high, body)


def first_sweep(weights, result, low, high):
    def body(i):
        result.put(i, -weights.side(i))

    loop(low, high, body)


def restricted(first, second):
    q = first + second
    even = lanes_of(q.shape) % 2 == 0
    return 0.125 * (q + jnp.where(even, roll_lanes(q, -1), roll_lanes(q, 1)))


def packed(planes):
    even = lanes_of((HALF, LANES)) % 2 == 0
    a, b, c, d = planes
    return jnp.where(even, a, b), jnp.where(even, c, d)


def unpacked(v):
    even = lanes_of((HALF, LANES)) % 2 == 0
    planes = []
    for half in (v[:HALF], v[HALF:]):
        planes.append(jnp.where(even, half, roll_lanes(half, 1)))
        planes.append(jnp.where(even, roll_lanes(half, -1), half))
    return planes


def residual_planes(weights, field, result, result_low, low, high, scratch):
    def body(i):
        total = 0.0
        for half in range(2):
            _, change = weights.change(field, 2 * i + half)
            total = total - change * weights.ref[7, weights.place(2 * i + half)]
        k = (i - low).index()
        scratch[k] = total
        odd = scratch[k, pl.ds(1, HALF, stride=2)]
        result[(i - result_low).index()] = restricted(scratch[k, pl.ds(0, HALF, stride=2)], odd)

    loop(low, high, body)


def prolong(correction, known, result, low, high):
    def body(i):
        added = correction(i)
        for half in range(2):
            for first in range(2):
                k = 2 * i + half
                result.put_every_other(k, first, known(k, first) + added)

    loop(low, high, body)


def inside_of(first, count):
    def inside(i):
        place = i.index(first)
        return jnp.where((place >= 0) & (place < count), 1.0, 0.0)

    return inside


def whereabouts(n_chips):
    slab, cross = lax.axis_index("slab"), lax.axis_index("cross")
    chip = jnp.minimum(jnp.maximum(slab // 2, 0), n_chips - 1)
    return slab % 2 == 0, jnp.minimum(jnp.maximum(cross, 0), 3), chip


def prepare(velocity_in, density_in, source_in, out, velocity, density, source, semaphore):
    copies = [
        pltpu.make_async_copy(there, here, semaphore.at[k])
        for k, (there, here) in enumerate(
            [(density_in, density), (velocity_in, velocity), (source_in, source)]
        )
    ]
    for copy in copies:
        copy.start()
    lane = lanes_of((BLOCK, LANES))
    row = rows_of((BLOCK, LANES))
    copies[0].wait()
    for x in range(4):
        out[BLOCK * x : BLOCK * (x + 1)] = 1.0 / density[x]
    copies[1].wait()
    copies[2].wait()
    for x in range(4):
        u_p = velocity[0, x + 1] if x < 3 else 0.0
        u_m = velocity[0, x - 1] if x > 0 else 0.0
        v, w = velocity[1, x], velocity[2, x]
        v_p = jnp.where(row < BLOCK - 1, roll_rows(v, -1), 0.0)
        v_m = jnp.where(row > 0, roll_rows(v, 1), 0.0)
        w_p = jnp.where(lane < LANES - 1, roll_lanes(w, -1), 0.0)
        w_m = jnp.where(lane > 0, roll_lanes(w, 1), 0.0)
        moved = 0.5 * ((u_p - u_m) + (v_p - v_m) + (w_p - w_m))
        out[64 + BLOCK * x : 64 + BLOCK * (x + 1)] = moved - source[x]
        r = EDGE + x
        out[r : r + 1] = velocity[1, x, 0:1]
        out[r + 4 : r + 5] = velocity[1, x, BLOCK - 1 : BLOCK]
    out[128:144] = velocity[0, 0]
    out[144:160] = velocity[0, 3]


def assemble(n_chips, gathered, sent, sent_far, edge):
    north, _, _ = whereabouts(n_chips)
    row = rows_of((BLOCK, LANES))
    for c in range(4):
        rows = slice(BLOCK * c, BLOCK * (c + 1))
        for k in range(2):
            block = 2 * c + k
            for x in range(4):
                sent[4 * k + x, rows] = gathered[block, BLOCK * x : BLOCK * (x + 1)]
                t = gathered[block, 64 + BLOCK * x : 64 + BLOCK * (x + 1)]
                r = EDGE + x
                if c > 0:
                    t = t - jnp.where(row == 0, 0.5 * gathered[block - 2, r + 4 : r + 5], 0.0)
                if c < 3:
                    t = t + jnp.where(row == BLOCK - 1, 0.5 * gathered[block + 2, r : r + 1], 0.0)
                if k == 0 and x == 3:
                    t = t + 0.5 * gathered[block + 1, 128:144]
                if k == 1 and x == 0:
                    t = t - 0.5 * gathered[block - 1, 144:160]
                sent[8 + 4 * k + x, rows] = t
        edge[0, rows] = gathered[2 * c, 128:144]
        edge[1, rows] = gathered[2 * c + 1, 144:160]
    u = edge[jnp.where(north, 0, 1)]
    sent[16] = u
    sent_far[0] = sent[jnp.where(north, 0, 7)]
    sent_far[1] = u


def species_edges(n_chips, species, near, beside, edge_low, edge_high):
    north, _, _ = whereabouts(n_chips)
    outward, inward = jnp.where(north, 0, 3), jnp.where(north, 3, 0)
    for s in range(SPECIES):
        near[BLOCK * s : BLOCK * (s + 1)] = species[s, outward]
        beside[BLOCK * s : BLOCK * (s + 1)] = species[s, inward]
        for x in range(4):
            r = 4 * s + x
            edge_low[r : r + 1] = species[s, x, 0:1]
            edge_high[r : r + 1] = species[s, x, BLOCK - 1 : BLOCK]
    edge_low[36:40] = jnp.zeros((4, LANES), jnp.float32)
    edge_high[36:40] = jnp.zeros((4, LANES), jnp.float32)


def flow_rims(n_chips, gathered, u_beside, v_rims):
    north, cross, _ = whereabouts(n_chips)
    core = jnp.where(north, 0, 1)
    partner = 2 * cross + jnp.where(north, 1, 0)
    u_beside[...] = jnp.where(north, gathered[partner, 128:144], gathered[partner, 144:160])
    below = gathered[2 * jnp.maximum(cross - 1, 0) + core, EDGE:OWN]
    above = gathered[2 * jnp.minimum(cross + 1, 3) + core, EDGE:OWN]
    v_rims[0:4] = jnp.where(cross > 0, below[4:8], 0.0)
    v_rims[4:8] = jnp.where(cross < 3, above[0:4], 0.0)


def first_cycle(
    n_chips, own, edge, mine, swapped, species_near,
    mobile_ref, weights_ref, pressure_ref, residual, coarse, outer, sent,
    target_w, field_ref, rows_ref,
):
    north, _, chip = whereabouts(n_chips)
    clear_pads(mobile_ref)
    clear_pads(field_ref)
    clear_pads(pressure_ref)
    mobile_w, pressure = Field(mobile_ref, -9), Field(pressure_ref, -8)
    field = Field(field_ref, -8)

    def sides(k):
        a, b = mine[k], swapped[k]
        return jnp.where(north, a, b), jnp.where(north, b, a)

    def copy(i):
        k, later = i.index(), (i + 8).index()
        left, right = sides(k)
        mobile_w.put(i - 8, left)
        mobile_w.put(i, own[k])
        mobile_w.put(i + 8, right)
        left, right = sides(later)
        target_w[k] = left
        target_w[later] = own[later]
        target_w[(i + 16).index()] = right

    loop(0, 8, copy)
    left, right = sides(17)
    mobile_w.put(Place(0, -9), left)
    mobile_w.put(Place(0, 16), right)
    left, right = sides(18)
    target_w[0] = target_w[0] - 0.5 * left
    target_w[23] = target_w[23] + 0.5 * right
    left, right = sides(16)
    target_w[7] = target_w[7] + 0.5 * edge[0]
    target_w[8] = target_w[8] - 0.5 * left
    target_w[15] = target_w[15] + 0.5 * right
    target_w[16] = target_w[16] - 0.5 * edge[1]
    outer[...] = mine[16]

    weights = Weights(weights_ref, 1, -8)
    weights.fill(-8, 16, mobile_w, at(target_w, -8), inside_of(8 * chip, 8 * n_chips))
    first_sweep(weights, field, -8, 16)
    sweep(weights, field, pressure, -7, 15)
    residual_planes(weights, pressure, residual, -3, -3, 7, rows_ref)

    def restrict(i):
        rows = [
            mobile_w.every_other(2 * i, first) + mobile_w.every_other(2 * i + 1, first)
            for first in range(2)
        ]
        coarse[(i + 4).index()] = restricted(*rows)

    loop(-4, 8, restrict)
    r = jnp.where(north, 6, 0)
    sent[0:32], sent[32:64] = packed([residual[r + k] for k in range(4)])
    m = jnp.where(north, 8, 0)
    sent[64:96], sent[96:128] = packed([coarse[m + k] for k in range(4)])
    sent[128:272] = species_near[...]


def coarse_sweeps(weights, one, two, low, high):
    first_sweep(weights, one, low, high)
    sweep(weights, one, two, low + 1, high - 1)
    sweep(weights, two, one, low + 2, high - 2)
    sweep(weights, one, two, low + 3, high - 3)


def inner(n_chips, chip):
    return chip > 0, chip < n_chips - 1


def second_cycle(
    n_chips, weights_ref, pressure_ref, residual, coarse, got,
    pressure_new_ref, residual_new, coarse_weights_ref, sent,
    coarse_ref, residual_w, one_ref, two_ref, field_ref, other_ref, rows_ref,
):
    north, _, chip = whereabouts(n_chips)
    before, after = inner(n_chips, chip)
    for ref in (pressure_new_ref, coarse_ref, one_ref, two_ref, field_ref, other_ref):
        clear_pads(ref)
    coarse_w, one, two = Field(coarse_ref, -8), Field(one_ref, -7), Field(two_ref, -7)
    field, other = Field(field_ref, -8), Field(other_ref, -8)
    pressure, pressure_new = Field(pressure_ref, -8), Field(pressure_new_ref, -3)

    left = unpacked(jnp.where(before, got[0, 0:64], 0.0))
    right = unpacked(jnp.where(after, got[1, 272:336], 0.0))
    for i in range(4):
        residual_w[i] = left[i]
        residual_w[14 + i] = right[i]
    left = unpacked(jnp.where(before, got[0, 64:128], 0.0))
    right = unpacked(jnp.where(after, got[1, 336:400], 0.0))
    for i in range(4):
        coarse_w.put(Place(0, i - 8), left[i])
        coarse_w.put(Place(0, i + 8), right[i])

    def copy_residual(i):
        residual_w[(i + 4).index()] = residual[i.index()]

    def copy_coarse(i):
        coarse_w.put(i - 4, coarse[i.index()])

    loop(0, 10, copy_residual)
    loop(0, 12, copy_coarse)

    coarse_weights = Weights(coarse_weights_ref, 2, -7)
    coarse_weights.fill(-7, 11, coarse_w, at(residual_w, -7), inside_of(4 * chip, 4 * n_chips))
    coarse_sweeps(coarse_weights, one, two, -7, 11)

    prolong(two, pressure.every_other, field, -4, 8)

    weights = Weights(weights_ref, 1, -8)
    sweep(weights, field, other, -6, 14)
    sweep(weights, other, field, -5, 13)
    sweep(weights, field, other, -4, 12)
    sweep(weights, other, pressure_new, -3, 11)
    residual_planes(weights, pressure_new, residual_new, -1, -1, 5, rows_ref)
    sent[0] = pressure_new_ref[jnp.where(north, 6, 7), PAD : PAD + ROWS]
    r = jnp.where(north, 2, 0)
    sent[1, 0:32], sent[1, 32:64] = packed([residual_new[r + k] for k in range(4)])


def finish(
    n_chips, mobile_ref, weights_ref, pressure, residual, coarse_weights_ref, got, swapped,
    velocity, species, outer, u_beside, v_rims, sides, y_low, y_high,
    velocity_out, pressure_out, species_out,
    residual_w, pressure_w, one_ref, two_ref, field_ref, other_ref, final_pad,
):
    north, cross, chip = whereabouts(n_chips)
    before, after = inner(n_chips, chip)
    for ref in (one_ref, two_ref, field_ref, other_ref, final_pad):
        clear_pads(ref)
    one, two = Field(one_ref, -5), Field(two_ref, -5)
    field, other, final = Field(field_ref, -4), Field(other_ref, -4), Field(final_pad, -2)
    left = unpacked(jnp.where(before, swapped[0, 0], 0.0))
    right = unpacked(jnp.where(after, swapped[1, 1], 0.0))
    for i in range(4):
        residual_w[i] = left[i]
        residual_w[10 + i] = right[i]
    for i in range(6):
        residual_w[4 + i] = residual[i]
    pressure_w[0] = jnp.where(before, got[0, 0], 0.0)
    pressure_w[15] = jnp.where(after, got[1, 0], 0.0)
    known = Field(pressure, -3)

    def copy_pressure(i):
        pressure_w[(i + 4).index()] = known(i)

    loop(-3, 11, copy_pressure)

    shift, coarse_shift = jnp.where(north, 0, 4), jnp.where(north, 0, 2)
    coarse_weights = Weights(coarse_weights_ref, 2, -7, coarse_shift, at(residual_w, -5))

    def right_side(i):
        k = (i + 5).index()
        factor = coarse_weights_ref[7, coarse_weights.place(i)]
        residual_w[k] = residual_w[(i + 5).index(coarse_shift)] * factor

    for k in range(12):
        right_side(Place(0, k - 5))
    coarse_sweeps(coarse_weights, one, two, -5, 7)

    def known_rows(i, first):
        return pressure_w[(i + 4).index(shift), pl.ds(first, HALF, stride=2)]

    prolong(two, known_rows, field, -2, 4)

    weights = Weights(weights_ref, 1, -8, shift)
    sweep(weights, field, other, -3, 7)
    sweep(weights, other, final, -2, 6)

    start = pl.multiple_of(cross * BLOCK, BLOCK)
    own = pl.ds(start + 8, BLOCK)
    row, lane = rows_of((BLOCK, LANES)), lanes_of((BLOCK, LANES))

    beyond = outer[pl.ds(start, BLOCK)]
    u_low = jnp.where(north, beyond, u_beside[...])
    u_high = jnp.where(north, u_beside[...], beyond)

    def u_out(x):
        if x < 0:
            u = u_low
        elif x > 3:
            u = u_high
        else:
            u = velocity[0, x]
        slope = 0.5 * (final_pad[x + 3, own] - final_pad[x + 1, own])
        return u - mobile_ref[shift + (x + 9), own] * slope

    u = [u_out(x) for x in range(-1, 5)]

    def species_beside(s, side):
        at_rim = BLOCK * s + (128 if side == 0 else 400)
        outside = sides[side, at_rim : at_rim + BLOCK]
        outside = jnp.where(before if side == 0 else after, outside, 0.0)
        inside = sides[side, 544 + BLOCK * s : 560 + BLOCK * s]
        return jnp.where(north, outside, inside) if side == 0 else jnp.where(north, inside, outside)

    wide = pl.ds(start, 32)
    for x in range(4):
        p = final_pad[x + 2, wide]
        m = mobile_ref[shift + (x + 9), wide]
        p_own = p[8:24]
        v = velocity[1, x] - m[8:24] * (0.5 * (p[9:25] - p[7:23]))
        v_low = v_rims[x : x + 1] - m[7:8] * (0.5 * (p[8:9] - p[6:7]))
        v_high = v_rims[4 + x : 5 + x] - m[24:25] * (0.5 * (p[25:26] - p[23:24]))
        p_zp = jnp.where(lane < LANES - 1, roll_lanes(p_own, -1), 0.0)
        p_zm = jnp.where(lane > 0, roll_lanes(p_own, 1), 0.0)
        w = velocity[2, x] - m[8:24] * (0.5 * (p_zp - p_zm))
        velocity_out[0, x] = u[x + 1]
        velocity_out[1, x] = v
        velocity_out[2, x] = w
        pressure_out[x] = p_own

        flow_xm, flow_xp = 0.5 * (u[x] + u[x + 1]), 0.5 * (u[x + 1] + u[x + 2])
        v_m = jnp.where(row == 0, v_low, roll_rows(v, 1))
        v_p = jnp.where(row == BLOCK - 1, v_high, roll_rows(v, -1))
        flow_ym, flow_yp = 0.5 * (v_m + v), 0.5 * (v + v_p)
        w_m = jnp.where(lane > 0, roll_lanes(w, 1), 0.0)
        w_p = jnp.where(lane < LANES - 1, roll_lanes(w, -1), 0.0)
        flow_zm, flow_zp = 0.5 * (w_m + w), 0.5 * (w + w_p)

        def leaves(high, low):
            return jnp.maximum(high, 0.0) - jnp.minimum(low, 0.0)

        keep = 1.0 - time_step * (
            leaves(flow_xp, flow_xm) + leaves(flow_yp, flow_ym) + leaves(flow_zp, flow_zm)
        )
        from_xm, from_xp = (
            time_step * jnp.maximum(flow_xm, 0.0),
            -time_step * jnp.minimum(flow_xp, 0.0),
        )
        from_ym, from_yp = (
            time_step * jnp.maximum(flow_ym, 0.0),
            -time_step * jnp.minimum(flow_yp, 0.0),
        )
        from_zm = jnp.where(lane > 0, time_step * jnp.maximum(flow_zm, 0.0), 0.0)
        from_zp = jnp.where(lane < LANES - 1, -time_step * jnp.minimum(flow_zp, 0.0), 0.0)
        for s in range(SPECIES):
            c = species[s, x]
            if x > 0:
                c_xm = species[s, x - 1]
            else:
                c_xm = species_beside(s, 0)
            if x < 3:
                c_xp = species[s, x + 1]
            else:
                c_xp = species_beside(s, 1)
            r = 4 * s + x
            c_ym = jnp.where(row == 0, y_low[r : r + 1], roll_rows(c, 1))
            c_yp = jnp.where(row == BLOCK - 1, y_high[r : r + 1], roll_rows(c, -1))
            total = keep * c + (from_xm * c_xm + from_xp * c_xp)
            total = total + (from_ym * c_ym + from_yp * c_yp)
            total = total + (from_zm * roll_lanes(c, 1) + from_zp * roll_lanes(c, -1))
            species_out[s, x] = total


def call(kernel, outs, scratch, *operands, where=pltpu.VMEM, semaphores=0, grant=24):
    vmem = pl.BlockSpec(memory_space=pltpu.VMEM)
    shapes = [jax.ShapeDtypeStruct(shape, jnp.float32) for shape in outs]
    scratch = [pltpu.VMEM(shape, jnp.float32) for shape in scratch]
    if semaphores:
        scratch = [*scratch, pltpu.SemaphoreType.DMA((semaphores,))]
    return pl.pallas_call(
        kernel,
        out_shape=shapes,
        in_specs=[pl.BlockSpec(memory_space=where) for _ in operands],
        out_specs=[vmem for _ in outs],
        scratch_shapes=scratch,
        cost_estimate=pl.CostEstimate(flops=1000000, bytes_accessed=1000000, transcendentals=0),
        compiler_params=pltpu.CompilerParams(vmem_limit_bytes=grant * 2**20),
        interpret=INTERPRET,
    )(*operands)


def gathered_over(array, groups):
    return lax.all_gather(array, ("slab", "cross"), axis_index_groups=groups)


def local(n_chips, velocity, density, source, species):
    def device(slab, cross):
        return 4 * slab + cross

    chips = [[device(2 * j + k, c) for c in range(4) for k in range(2)] for j in range(n_chips)]
    cores = [
        [device(2 * j, c), device(2 * j + 1, c)] for j in range(n_chips) for c in range(4)
    ]
    facing = [
        [device(2 * j + 1, c), device(2 * j + 2, c)] for j in range(n_chips - 1) for c in range(4)
    ]
    for slab in (0, 2 * n_chips - 1):
        facing += [[device(slab, 0), device(slab, 1)], [device(slab, 2), device(slab, 3)]]

    def beside(distance):
        pairs = []
        for j in range(n_chips - distance):
            left, right = 2 * j + 1, 2 * (j + distance)
            pairs += [(left, right), (right, left)]
        return pairs

    within = [pair for j in range(n_chips) for pair in ((2 * j, 2 * j + 1), (2 * j + 1, 2 * j))]
    upward = [(c, c + 1) for c in range(3)]
    downward = [(c + 1, c) for c in range(3)]

    def plane(n):
        return (n, ROWS, LANES)

    def padded(n, rows=ROWS):
        return (n, rows + 2 * PAD, LANES)

    def halved(n):
        return (n, HALF, LANES)

    def bind(kernel):
        return functools.partial(kernel, n_chips)

    (own,) = call(
        prepare, [(OWN, LANES)], [velocity.shape, density.shape, source.shape],
        velocity, density, source,
        where=HBM, semaphores=3, grant=63,
    )
    gathered = gathered_over(own, chips)
    sent, sent_far, edge = call(bind(assemble), [plane(17), plane(2), plane(2)], [], gathered)
    near = lax.ppermute(sent, "slab", beside(1))
    far = lax.ppermute(sent_far, "slab", beside(2))
    species_near, species_beside, edge_low, edge_high = call(
        bind(species_edges), [(144, LANES), (144, LANES), (40, LANES), (40, LANES)], [], species
    )
    y_low = lax.ppermute(edge_high, "cross", upward)
    y_high = lax.ppermute(edge_low, "cross", downward)
    u_beside, v_rims = call(bind(flow_rims), [(BLOCK, LANES), (8, LANES)], [], gathered)
    mine = jnp.concatenate([near, far], 0)
    swapped = lax.ppermute(mine, "slab", within)
    mobile_w, weights, pressure, residual, coarse, outer, sent_two = call(
        bind(first_cycle),
        [
            padded(26), (8, *plane(24)), padded(24), halved(10), halved(12), PLANE, (272, LANES),
        ],
        [plane(24), padded(24), plane(10)],
        sent, edge, mine, swapped, species_near,
    )
    near = gathered_over(sent_two, facing).reshape(544, LANES)
    sides = gathered_over(jnp.concatenate([near, species_beside], 0), cores)
    pressure, residual, coarse_weights, sent = call(
        bind(second_cycle),
        [padded(14), halved(6), (8, *halved(18)), plane(2)],
        [
            padded(20, HALF), halved(18), padded(18, HALF), padded(18, HALF), padded(24), padded(24),
            plane(6),
        ],
        weights, pressure, residual, coarse, sides,
    )
    near = gathered_over(sent, facing)
    swapped = gathered_over(near[:, 1], cores)
    return call(
        bind(finish),
        [velocity.shape, density.shape, species.shape],
        [
            halved(14), plane(16), padded(12, HALF), padded(12, HALF), padded(12), padded(12),
            padded(8),
        ],
        mobile_w, weights, pressure, residual, coarse_weights, near, swapped,
        velocity, species, outer, u_beside, v_rims, sides, y_low, y_high,
    )


def solution(mesh):
    n_chips = mesh.shape["slab"] // 2
    block = P("slab", "cross", None)
    stack = P(None, "slab", "cross", None)

    def step(*arrays):
        return tuple(local(n_chips, *arrays))

    return jax.shard_map(
        step,
        mesh=mesh,
        in_specs=(stack, block, block, stack),
        out_specs=(stack, block, stack),
        check_vma=False,
    )
```

```python
import functools

import jax
import jax.numpy as jnp
from jax import lax
from jax.experimental import pallas as pl
from jax.experimental.pallas import tpu as pltpu
from jax.sharding import PartitionSpec as P


INTERPRET = False
HBM = pltpu.HBM
ROWS = 64
LANES = 128
BLOCK = 16
SPECIES = 9
EDGE = 160
OWN = EDGE + 80
damping = 0.8
time_step = 0.25


class Place:
    def __init__(self, counter, constant):
        self.counter = counter
        self.constant = constant

    def __add__(self, other):
        return Place(self.counter, self.constant + other)

    def __sub__(self, other):
        return Place(self.counter, self.constant - other)

    def __rmul__(self, factor):
        return Place(self.counter * factor, self.constant * factor)

    def index(self, shift=None):
        start = self.counter if shift is None else self.counter + shift
        return start + self.constant


def loop(low, high, body):
    for u in range(high - low):
        body(Place(0, low + u))


def rows_of(shape):
    return lax.broadcasted_iota(jnp.int32, shape, 0)


def lanes_of(shape):
    return lax.broadcasted_iota(jnp.int32, shape, 1)


PLANE = (ROWS, LANES)


def roll_rows(x, by):
    return pltpu.roll(x, by % x.shape[0], 0)


def roll_lanes(x, by):
    return pltpu.roll(x, by % x.shape[1], 1)


PAD = 8
HALF = ROWS // 2


class Field:
    def __init__(self, ref, low, shift=None):
        self.ref = ref
        self.low = low
        self.shift = shift
        self.rows = ref.shape[1] - 2 * PAD

    def __call__(self, i, rows=0):
        k = (i - self.low).index(self.shift)
        return self.ref[k, PAD + rows : PAD + rows + self.rows]

    def put(self, i, value):
        self.ref[(i - self.low).index(), PAD : PAD + self.rows] = value

    def every_other(self, i, first):
        return self.ref[(i - self.low).index(), pl.ds(PAD + first, HALF, stride=2)]

    def put_every_other(self, i, first, value):
        self.ref[(i - self.low).index(), pl.ds(PAD + first, HALF, stride=2)] = value


def clear_pads(ref):
    nothing = jnp.zeros((PAD, LANES), jnp.float32)
    for k in range(ref.shape[0]):
        ref[k, 0:PAD] = nothing
        ref[k, ref.shape[1] - PAD :] = nothing


class Weights:
    def __init__(self, ref, step, low, shift=None, constant=None):
        self.ref = ref
        self.step = step
        self.low = low
        self.shift = shift
        self.constant = constant

    def place(self, i):
        return (i - self.low).index(self.shift)

    def fill(self, low, high, mobile, target, inside):
        s = self.step
        lane = lanes_of((mobile.rows, LANES))
        z_low, z_high = lane >= s, lane < LANES - s

        def body(i):
            m = mobile(i)
            x_m, x_p = mobile(i - 1), mobile(i + 1)
            y_m, y_p = mobile(i, -1), mobile(i, 1)
            z_m = jnp.where(z_low, roll_lanes(m, s), 0.0)
            z_p = jnp.where(z_high, roll_lanes(m, -s), 0.0)
            diagonal = 3.0 * m + 0.5 * ((x_m + x_p) + (y_m + y_p) + (z_m + z_p))
            valid = inside(i)
            scaled = (damping * valid) / (diagonal + (1.0 - valid))
            half = 0.5 * scaled
            k = self.place(i)
            self.ref[0, k] = (m + x_m) * half
            self.ref[1, k] = (m + x_p) * half
            self.ref[2, k] = (m + y_m) * half
            self.ref[3, k] = (m + y_p) * half
            self.ref[4, k] = jnp.where(z_low, (m + z_m) * half, 0.0)
            self.ref[5, k] = jnp.where(z_high, (m + z_p) * half, 0.0)
            if s == 1:
                self.ref[6, k] = target(i) * scaled
                self.ref[7, k] = diagonal * (1.0 / damping)
            else:
                self.ref[6, k] = target(i) * (4.0 * scaled)
                self.ref[7, k] = 4.0 * scaled

        loop(low, high, body)

    def side(self, i):
        if self.constant is not None:
            return self.constant(i)
        return self.ref[6, self.place(i)]

    def change(self, field, i):
        s = self.step
        k = self.place(i)
        p = field(i)
        total = self.ref[0, k] * field(i - 1) + self.ref[1, k] * field(i + 1)
        total = total + (self.ref[2, k] * field(i, -1) + self.ref[3, k] * field(i, 1))
        total = total + (self.ref[4, k] * roll_lanes(p, s) + self.ref[5, k] * roll_lanes(p, -s))
        return p, (total - self.side(i)) - damping * p


def at(ref, origin, shift=None):
    return lambda i: ref[(i - origin).index(shift)]


def sweep(weights, source, result, low, high):
    def body(i):
        p, change = weights.change(source, i)
        result.put(i, p + change)

    loop(low, high, body)


def first_sweep(weights, result, low, high):
    def body(i):
        result.put(i, -weights.side(i))

    loop(low, high, body)


def restricted(first, second):
    q = first + second
    even = lanes_of(q.shape) % 2 == 0
    return 0.125 * (q + jnp.where(even, roll_lanes(q, -1), roll_lanes(q, 1)))


def packed(planes):
    even = lanes_of((HALF, LANES)) % 2 == 0
    a, b, c, d = planes
    return jnp.where(even, a, b), jnp.where(even, c, d)


def unpacked(v):
    even = lanes_of((HALF, LANES)) % 2 == 0
    planes = []
    for half in (v[:HALF], v[HALF:]):
        planes.append(jnp.where(even, half, roll_lanes(half, 1)))
        planes.append(jnp.where(even, roll_lanes(half, -1), half))
    return planes


def residual_planes(weights, field, result, result_low, low, high, scratch):
    def body(i):
        total = 0.0
        for half in range(2):
            _, change = weights.change(field, 2 * i + half)
            total = total - change * weights.ref[7, weights.place(2 * i + half)]
        k = (i - low).index()
        scratch[k] = total
        odd = scratch[k, pl.ds(1, HALF, stride=2)]
        result[(i - result_low).index()] = restricted(scratch[k, pl.ds(0, HALF, stride=2)], odd)

    loop(low, high, body)


def prolong(correction, known, result, low, high):
    def body(i):
        added = correction(i)
        for half in range(2):
            for first in range(2):
                k = 2 * i + half
                result.put_every_other(k, first, known(k, first) + added)

    loop(low, high, body)


def inside_of(first, count):
    def inside(i):
        place = i.index(first)
        return jnp.where((place >= 0) & (place < count), 1.0, 0.0)

    return inside


def whereabouts(n_chips):
    slab, cross = lax.axis_index("slab"), lax.axis_index("cross")
    chip = jnp.minimum(jnp.maximum(slab // 2, 0), n_chips - 1)
    return slab % 2 == 0, jnp.minimum(jnp.maximum(cross, 0), 3), chip


def prepare(
    velocity_in, density_in, source_in, species_in, out,
    velocity, density, source, species, semaphore,
):
    copies = [
        pltpu.make_async_copy(there, here, semaphore.at[k])
        for k, (there, here) in enumerate(
            [
                (density_in, density), (velocity_in, velocity), (source_in, source),
                (species_in, species),
            ]
        )
    ]
    for copy in copies:
        copy.start()
    lane = lanes_of((BLOCK, LANES))
    row = rows_of((BLOCK, LANES))
    copies[0].wait()
    for x in range(4):
        out[BLOCK * x : BLOCK * (x + 1)] = 1.0 / density[x]
    copies[1].wait()
    copies[2].wait()
    for x in range(4):
        u_p = velocity[0, x + 1] if x < 3 else 0.0
        u_m = velocity[0, x - 1] if x > 0 else 0.0
        v, w = velocity[1, x], velocity[2, x]
        v_p = jnp.where(row < BLOCK - 1, roll_rows(v, -1), 0.0)
        v_m = jnp.where(row > 0, roll_rows(v, 1), 0.0)
        w_p = jnp.where(lane < LANES - 1, roll_lanes(w, -1), 0.0)
        w_m = jnp.where(lane > 0, roll_lanes(w, 1), 0.0)
        moved = 0.5 * ((u_p - u_m) + (v_p - v_m) + (w_p - w_m))
        out[64 + BLOCK * x : 64 + BLOCK * (x + 1)] = moved - source[x]
        r = EDGE + x
        out[r : r + 1] = velocity[1, x, 0:1]
        out[r + 4 : r + 5] = velocity[1, x, BLOCK - 1 : BLOCK]
    out[128:144] = velocity[0, 0]
    out[144:160] = velocity[0, 3]
    copies[3].wait()
    for s in range(SPECIES):
        for x in range(4):
            r = EDGE + 8 + 4 * s + x
            out[r : r + 1] = species[s, x, 0:1]
            out[r + 36 : r + 37] = species[s, x, BLOCK - 1 : BLOCK]


def assemble(n_chips, gathered, sent, sent_far, edge):
    north, _, _ = whereabouts(n_chips)
    row = rows_of((BLOCK, LANES))
    for c in range(4):
        rows = slice(BLOCK * c, BLOCK * (c + 1))
        for k in range(2):
            block = 2 * c + k
            for x in range(4):
                sent[4 * k + x, rows] = gathered[block, BLOCK * x : BLOCK * (x + 1)]
                t = gathered[block, 64 + BLOCK * x : 64 + BLOCK * (x + 1)]
                r = EDGE + x
                if c > 0:
                    t = t - jnp.where(row == 0, 0.5 * gathered[block - 2, r + 4 : r + 5], 0.0)
                if c < 3:
                    t = t + jnp.where(row == BLOCK - 1, 0.5 * gathered[block + 2, r : r + 1], 0.0)
                if k == 0 and x == 3:
                    t = t + 0.5 * gathered[block + 1, 128:144]
                if k == 1 and x == 0:
                    t = t - 0.5 * gathered[block - 1, 144:160]
                sent[8 + 4 * k + x, rows] = t
        edge[0, rows] = gathered[2 * c, 128:144]
        edge[1, rows] = gathered[2 * c + 1, 144:160]
    u = edge[jnp.where(north, 0, 1)]
    sent[16] = u
    sent_far[0] = sent[jnp.where(north, 0, 7)]
    sent_far[1] = u


def species_edges(n_chips, species, near, beside):
    north, _, _ = whereabouts(n_chips)
    outward, inward = jnp.where(north, 0, 3), jnp.where(north, 3, 0)
    for s in range(SPECIES):
        near[BLOCK * s : BLOCK * (s + 1)] = species[s, outward]
        beside[BLOCK * s : BLOCK * (s + 1)] = species[s, inward]


def flow_rims(n_chips, gathered, u_beside, v_rims, y_low, y_high):
    north, cross, _ = whereabouts(n_chips)
    core = jnp.where(north, 0, 1)
    partner = 2 * cross + jnp.where(north, 1, 0)
    u_beside[...] = jnp.where(north, gathered[partner, 128:144], gathered[partner, 144:160])
    below = gathered[2 * jnp.maximum(cross - 1, 0) + core, EDGE:OWN]
    above = gathered[2 * jnp.minimum(cross + 1, 3) + core, EDGE:OWN]
    v_rims[0:4] = jnp.where(cross > 0, below[4:8], 0.0)
    v_rims[4:8] = jnp.where(cross < 3, above[0:4], 0.0)
    y_low[...] = jnp.where(cross > 0, below[44:80], 0.0)
    y_high[...] = jnp.where(cross < 3, above[8:44], 0.0)


def first_cycle(
    n_chips, own, edge, mine, swapped,
    mobile_ref, weights_ref, pressure_ref, residual, coarse, outer, sent,
    target_w, field_ref, rows_ref,
):
    north, _, chip = whereabouts(n_chips)
    clear_pads(mobile_ref)
    clear_pads(field_ref)
    clear_pads(pressure_ref)
    mobile_w, pressure = Field(mobile_ref, -9), Field(pressure_ref, -8)
    field = Field(field_ref, -8)

    def sides(k):
        a, b = mine[k], swapped[k]
        return jnp.where(north, a, b), jnp.where(north, b, a)

    def copy(i):
        k, later = i.index(), (i + 8).index()
        left, right = sides(k)
        mobile_w.put(i - 8, left)
        mobile_w.put(i, own[k])
        mobile_w.put(i + 8, right)
        left, right = sides(later)
        target_w[k] = left
        target_w[later] = own[later]
        target_w[(i + 16).index()] = right

    loop(0, 8, copy)
    left, right = sides(17)
    mobile_w.put(Place(0, -9), left)
    mobile_w.put(Place(0, 16), right)
    left, right = sides(18)
    target_w[0] = target_w[0] - 0.5 * left
    target_w[23] = target_w[23] + 0.5 * right
    left, right = sides(16)
    target_w[7] = target_w[7] + 0.5 * edge[0]
    target_w[8] = target_w[8] - 0.5 * left
    target_w[15] = target_w[15] + 0.5 * right
    target_w[16] = target_w[16] - 0.5 * edge[1]
    outer[...] = mine[16]

    weights = Weights(weights_ref, 1, -8)
    weights.fill(-8, 16, mobile_w, at(target_w, -8), inside_of(8 * chip, 8 * n_chips))
    first_sweep(weights, field, -8, 16)
    sweep(weights, field, pressure, -7, 15)
    residual_planes(weights, pressure, residual, -3, -3, 7, rows_ref)

    def restrict(i):
        rows = [
            mobile_w.every_other(2 * i, first) + mobile_w.every_other(2 * i + 1, first)
            for first in range(2)
        ]
        coarse[(i + 4).index()] = restricted(*rows)

    loop(-4, 8, restrict)
    r = jnp.where(north, 6, 0)
    sent[0:32], sent[32:64] = packed([residual[r + k] for k in range(4)])
    m = jnp.where(north, 8, 0)
    sent[64:96], sent[96:128] = packed([coarse[m + k] for k in range(4)])


def coarse_sweeps(weights, one, two, low, high):
    first_sweep(weights, one, low, high)
    sweep(weights, one, two, low + 1, high - 1)
    sweep(weights, two, one, low + 2, high - 2)
    sweep(weights, one, two, low + 3, high - 3)


def inner(n_chips, chip):
    return chip > 0, chip < n_chips - 1


def second_cycle(
    n_chips, weights_ref, pressure_ref, residual, coarse, got,
    pressure_new_ref, residual_new, coarse_weights_ref, sent,
    coarse_ref, residual_w, one_ref, two_ref, field_ref, other_ref, rows_ref,
):
    north, _, chip = whereabouts(n_chips)
    before, after = inner(n_chips, chip)
    for ref in (pressure_new_ref, coarse_ref, one_ref, two_ref, field_ref, other_ref):
        clear_pads(ref)
    coarse_w, one, two = Field(coarse_ref, -8), Field(one_ref, -7), Field(two_ref, -7)
    field, other = Field(field_ref, -8), Field(other_ref, -8)
    pressure, pressure_new = Field(pressure_ref, -8), Field(pressure_new_ref, -3)

    left = unpacked(jnp.where(before, got[0, 0:64], 0.0))
    right = unpacked(jnp.where(after, got[1, 128:192], 0.0))
    for i in range(4):
        residual_w[i] = left[i]
        residual_w[14 + i] = right[i]
    left = unpacked(jnp.where(before, got[0, 64:128], 0.0))
    right = unpacked(jnp.where(after, got[1, 192:256], 0.0))
    for i in range(4):
        coarse_w.put(Place(0, i - 8), left[i])
        coarse_w.put(Place(0, i + 8), right[i])

    def copy_residual(i):
        residual_w[(i + 4).index()] = residual[i.index()]

    def copy_coarse(i):
        coarse_w.put(i - 4, coarse[i.index()])

    loop(0, 10, copy_residual)
    loop(0, 12, copy_coarse)

    coarse_weights = Weights(coarse_weights_ref, 2, -7)
    coarse_weights.fill(-7, 11, coarse_w, at(residual_w, -7), inside_of(4 * chip, 4 * n_chips))
    coarse_sweeps(coarse_weights, one, two, -7, 11)

    prolong(two, pressure.every_other, field, -4, 8)

    weights = Weights(weights_ref, 1, -8)
    sweep(weights, field, other, -6, 14)
    sweep(weights, other, field, -5, 13)
    sweep(weights, field, other, -4, 12)
    sweep(weights, other, pressure_new, -3, 11)
    residual_planes(weights, pressure_new, residual_new, -1, -1, 5, rows_ref)
    sent[0] = pressure_new_ref[jnp.where(north, 6, 7), PAD : PAD + ROWS]
    r = jnp.where(north, 2, 0)
    sent[1, 0:32], sent[1, 32:64] = packed([residual_new[r + k] for k in range(4)])


def finish(
    n_chips, mobile_ref, weights_ref, pressure, residual, coarse_weights_ref, got, swapped,
    velocity, species, outer, u_beside, v_rims, outer_rim, sides, y_low, y_high,
    velocity_out, pressure_out, species_out,
    residual_w, pressure_w, one_ref, two_ref, field_ref, other_ref, final_pad,
):
    north, cross, chip = whereabouts(n_chips)
    before, after = inner(n_chips, chip)
    for ref in (one_ref, two_ref, field_ref, other_ref, final_pad):
        clear_pads(ref)
    one, two = Field(one_ref, -5), Field(two_ref, -5)
    field, other, final = Field(field_ref, -4), Field(other_ref, -4), Field(final_pad, -2)
    left = unpacked(jnp.where(before, swapped[0, 0], 0.0))
    right = unpacked(jnp.where(after, swapped[1, 1], 0.0))
    for i in range(4):
        residual_w[i] = left[i]
        residual_w[10 + i] = right[i]
    for i in range(6):
        residual_w[4 + i] = residual[i]
    pressure_w[0] = jnp.where(before, got[0, 0], 0.0)
    pressure_w[15] = jnp.where(after, got[1, 0], 0.0)
    known = Field(pressure, -3)

    def copy_pressure(i):
        pressure_w[(i + 4).index()] = known(i)

    loop(-3, 11, copy_pressure)

    shift, coarse_shift = jnp.where(north, 0, 4), jnp.where(north, 0, 2)
    coarse_weights = Weights(coarse_weights_ref, 2, -7, coarse_shift, at(residual_w, -5))

    def right_side(i):
        k = (i + 5).index()
        factor = coarse_weights_ref[7, coarse_weights.place(i)]
        residual_w[k] = residual_w[(i + 5).index(coarse_shift)] * factor

    for k in range(12):
        right_side(Place(0, k - 5))
    coarse_sweeps(coarse_weights, one, two, -5, 7)

    def known_rows(i, first):
        return pressure_w[(i + 4).index(shift), pl.ds(first, HALF, stride=2)]

    prolong(two, known_rows, field, -2, 4)

    weights = Weights(weights_ref, 1, -8, shift)
    sweep(weights, field, other, -3, 7)
    sweep(weights, other, final, -2, 6)

    start = pl.multiple_of(cross * BLOCK, BLOCK)
    own = pl.ds(start + 8, BLOCK)
    row, lane = rows_of((BLOCK, LANES)), lanes_of((BLOCK, LANES))

    beyond = outer[pl.ds(start, BLOCK)]
    u_low = jnp.where(north, beyond, u_beside[...])
    u_high = jnp.where(north, u_beside[...], beyond)

    def u_out(x):
        if x < 0:
            u = u_low
        elif x > 3:
            u = u_high
        else:
            u = velocity[0, x]
        slope = 0.5 * (final_pad[x + 3, own] - final_pad[x + 1, own])
        return u - mobile_ref[shift + (x + 9), own] * slope

    u = [u_out(x) for x in range(-1, 5)]

    def species_beside(s, side):
        outside = outer_rim[BLOCK * s : BLOCK * (s + 1)]
        inside = sides[side, 256 + BLOCK * s : 272 + BLOCK * s]
        return jnp.where(north, outside, inside) if side == 0 else jnp.where(north, inside, outside)

    wide = pl.ds(start, 32)
    for x in range(4):
        p = final_pad[x + 2, wide]
        m = mobile_ref[shift + (x + 9), wide]
        p_own = p[8:24]
        v = velocity[1, x] - m[8:24] * (0.5 * (p[9:25] - p[7:23]))
        v_low = v_rims[x : x + 1] - m[7:8] * (0.5 * (p[8:9] - p[6:7]))
        v_high = v_rims[4 + x : 5 + x] - m[24:25] * (0.5 * (p[25:26] - p[23:24]))
        p_zp = jnp.where(lane < LANES - 1, roll_lanes(p_own, -1), 0.0)
        p_zm = jnp.where(lane > 0, roll_lanes(p_own, 1), 0.0)
        w = velocity[2, x] - m[8:24] * (0.5 * (p_zp - p_zm))
        velocity_out[0, x] = u[x + 1]
        velocity_out[1, x] = v
        velocity_out[2, x] = w
        pressure_out[x] = p_own

        flow_xm, flow_xp = 0.5 * (u[x] + u[x + 1]), 0.5 * (u[x + 1] + u[x + 2])
        v_m = jnp.where(row == 0, v_low, roll_rows(v, 1))
        v_p = jnp.where(row == BLOCK - 1, v_high, roll_rows(v, -1))
        flow_ym, flow_yp = 0.5 * (v_m + v), 0.5 * (v + v_p)
        w_m = jnp.where(lane > 0, roll_lanes(w, 1), 0.0)
        w_p = jnp.where(lane < LANES - 1, roll_lanes(w, -1), 0.0)
        flow_zm, flow_zp = 0.5 * (w_m + w), 0.5 * (w + w_p)

        def leaves(high, low):
            return jnp.maximum(high, 0.0) - jnp.minimum(low, 0.0)

        keep = 1.0 - time_step * (
            leaves(flow_xp, flow_xm) + leaves(flow_yp, flow_ym) + leaves(flow_zp, flow_zm)
        )
        from_xm, from_xp = (
            time_step * jnp.maximum(flow_xm, 0.0),
            -time_step * jnp.minimum(flow_xp, 0.0),
        )
        from_ym, from_yp = (
            time_step * jnp.maximum(flow_ym, 0.0),
            -time_step * jnp.minimum(flow_yp, 0.0),
        )
        from_zm = jnp.where(lane > 0, time_step * jnp.maximum(flow_zm, 0.0), 0.0)
        from_zp = jnp.where(lane < LANES - 1, -time_step * jnp.minimum(flow_zp, 0.0), 0.0)
        for s in range(SPECIES):
            c = species[s, x]
            if x > 0:
                c_xm = species[s, x - 1]
            else:
                c_xm = species_beside(s, 0)
            if x < 3:
                c_xp = species[s, x + 1]
            else:
                c_xp = species_beside(s, 1)
            r = 4 * s + x
            c_ym = jnp.where(row == 0, y_low[r : r + 1], roll_rows(c, 1))
            c_yp = jnp.where(row == BLOCK - 1, y_high[r : r + 1], roll_rows(c, -1))
            total = keep * c + (from_xm * c_xm + from_xp * c_xp)
            total = total + (from_ym * c_ym + from_yp * c_yp)
            total = total + (from_zm * roll_lanes(c, 1) + from_zp * roll_lanes(c, -1))
            species_out[s, x] = total


def call(kernel, outs, scratch, *operands, where=pltpu.VMEM, semaphores=0, grant=24):
    vmem = pl.BlockSpec(memory_space=pltpu.VMEM)
    shapes = [jax.ShapeDtypeStruct(shape, jnp.float32) for shape in outs]
    scratch = [pltpu.VMEM(shape, jnp.float32) for shape in scratch]
    if semaphores:
        scratch = [*scratch, pltpu.SemaphoreType.DMA((semaphores,))]
    return pl.pallas_call(
        kernel,
        out_shape=shapes,
        in_specs=[pl.BlockSpec(memory_space=where) for _ in operands],
        out_specs=[vmem for _ in outs],
        scratch_shapes=scratch,
        cost_estimate=pl.CostEstimate(flops=1000000, bytes_accessed=1000000, transcendentals=0),
        compiler_params=pltpu.CompilerParams(vmem_limit_bytes=grant * 2**20),
        interpret=INTERPRET,
    )(*operands)


def gathered_over(array, groups):
    return lax.all_gather(array, ("slab", "cross"), axis_index_groups=groups)


def local(n_chips, velocity, density, source, species):
    def device(slab, cross):
        return 4 * slab + cross

    chips = [[device(2 * j + k, c) for c in range(4) for k in range(2)] for j in range(n_chips)]
    cores = [
        [device(2 * j, c), device(2 * j + 1, c)] for j in range(n_chips) for c in range(4)
    ]
    facing = [
        [device(2 * j + 1, c), device(2 * j + 2, c)] for j in range(n_chips - 1) for c in range(4)
    ]
    for slab in (0, 2 * n_chips - 1):
        facing += [[device(slab, 0), device(slab, 1)], [device(slab, 2), device(slab, 3)]]

    def beside(distance):
        pairs = []
        for j in range(n_chips - distance):
            left, right = 2 * j + 1, 2 * (j + distance)
            pairs += [(left, right), (right, left)]
        return pairs

    within = [pair for j in range(n_chips) for pair in ((2 * j, 2 * j + 1), (2 * j + 1, 2 * j))]

    def plane(n):
        return (n, ROWS, LANES)

    def padded(n, rows=ROWS):
        return (n, rows + 2 * PAD, LANES)

    def halved(n):
        return (n, HALF, LANES)

    def bind(kernel):
        return functools.partial(kernel, n_chips)

    (own,) = call(
        prepare, [(OWN, LANES)], [velocity.shape, density.shape, source.shape, species.shape],
        velocity, density, source, species,
        where=HBM, semaphores=4, grant=63,
    )
    gathered = gathered_over(own, chips)
    sent, sent_far, edge = call(bind(assemble), [plane(17), plane(2), plane(2)], [], gathered)
    near = lax.ppermute(sent, "slab", beside(1))
    far = lax.ppermute(sent_far, "slab", beside(2))
    species_near, species_beside = call(
        bind(species_edges), [(144, LANES), (144, LANES)], [], species
    )
    outer_rim = lax.ppermute(species_near, "slab", beside(1))
    u_beside, v_rims, y_low, y_high = call(
        bind(flow_rims), [(BLOCK, LANES), (8, LANES), (36, LANES), (36, LANES)], [], gathered
    )
    mine = jnp.concatenate([near, far], 0)
    swapped = lax.ppermute(mine, "slab", within)
    mobile_w, weights, pressure, residual, coarse, outer, sent_two = call(
        bind(first_cycle),
        [
            padded(26), (8, *plane(24)), padded(24), halved(10), halved(12), PLANE, (128, LANES),
        ],
        [plane(24), padded(24), plane(10)],
        sent, edge, mine, swapped,
    )
    near = gathered_over(sent_two, facing).reshape(256, LANES)
    sides = gathered_over(jnp.concatenate([near, species_beside], 0), cores)
    pressure, residual, coarse_weights, sent = call(
        bind(second_cycle),
        [padded(14), halved(6), (8, *halved(18)), plane(2)],
        [
            padded(20, HALF), halved(18), padded(18, HALF), padded(18, HALF), padded(24), padded(24),
            plane(6),
        ],
        weights, pressure, residual, coarse, sides,
    )
    near = gathered_over(sent, facing)
    swapped = gathered_over(near[:, 1], cores)
    return call(
        bind(finish),
        [velocity.shape, density.shape, species.shape],
        [
            halved(14), plane(16), padded(12, HALF), padded(12, HALF), padded(12), padded(12),
            padded(8),
        ],
        mobile_w, weights, pressure, residual, coarse_weights, near, swapped,
        velocity, species, outer, u_beside, v_rims, outer_rim, sides, y_low, y_high,
    )


def solution(mesh):
    n_chips = mesh.shape["slab"] // 2
    block = P("slab", "cross", None)
    stack = P(None, "slab", "cross", None)

    def step(*arrays):
        return tuple(local(n_chips, *arrays))

    return jax.shard_map(
        step,
        mesh=mesh,
        in_specs=(stack, block, block, stack),
        out_specs=(stack, block, stack),
        check_vma=False,
    )
```

```python
import functools

import jax
import jax.numpy as jnp
from jax import lax
from jax.experimental import pallas as pl
from jax.experimental.pallas import tpu as pltpu
from jax.sharding import PartitionSpec as P


INTERPRET = False
HBM = pltpu.HBM
ROWS = 64
LANES = 128
BLOCK = 16
SPECIES = 9
EDGE = 160
OWN = EDGE + 80
damping = 0.8
time_step = 0.25


class Place:
    def __init__(self, counter, constant):
        self.counter = counter
        self.constant = constant

    def __add__(self, other):
        return Place(self.counter, self.constant + other)

    def __sub__(self, other):
        return Place(self.counter, self.constant - other)

    def __rmul__(self, factor):
        return Place(self.counter * factor, self.constant * factor)

    def index(self, shift=None):
        start = self.counter if shift is None else self.counter + shift
        return start + self.constant


def loop(low, high, body):
    for u in range(high - low):
        body(Place(0, low + u))


def rows_of(shape):
    return lax.broadcasted_iota(jnp.int32, shape, 0)


def lanes_of(shape):
    return lax.broadcasted_iota(jnp.int32, shape, 1)


PLANE = (ROWS, LANES)


def roll_rows(x, by):
    return pltpu.roll(x, by % x.shape[0], 0)


def roll_lanes(x, by):
    return pltpu.roll(x, by % x.shape[1], 1)


PAD = 8
HALF = ROWS // 2


class Field:
    def __init__(self, ref, low, shift=None):
        self.ref = ref
        self.low = low
        self.shift = shift
        self.rows = ref.shape[1] - 2 * PAD

    def __call__(self, i, rows=0):
        k = (i - self.low).index(self.shift)
        return self.ref[k, PAD + rows : PAD + rows + self.rows]

    def put(self, i, value):
        self.ref[(i - self.low).index(), PAD : PAD + self.rows] = value

    def every_other(self, i, first):
        return self.ref[(i - self.low).index(), pl.ds(PAD + first, HALF, stride=2)]

    def put_every_other(self, i, first, value):
        self.ref[(i - self.low).index(), pl.ds(PAD + first, HALF, stride=2)] = value


def clear_pads(ref):
    nothing = jnp.zeros((PAD, LANES), jnp.float32)
    for k in range(ref.shape[0]):
        ref[k, 0:PAD] = nothing
        ref[k, ref.shape[1] - PAD :] = nothing


class Weights:
    def __init__(self, ref, step, low, shift=None, constant=None):
        self.ref = ref
        self.step = step
        self.low = low
        self.shift = shift
        self.constant = constant

    def place(self, i):
        return (i - self.low).index(self.shift)

    def fill(self, low, high, mobile, target, inside):
        s = self.step
        lane = lanes_of((mobile.rows, LANES))
        z_low, z_high = lane >= s, lane < LANES - s

        def body(i):
            m = mobile(i)
            x_m, x_p = mobile(i - 1), mobile(i + 1)
            y_m, y_p = mobile(i, -1), mobile(i, 1)
            z_m = jnp.where(z_low, roll_lanes(m, s), 0.0)
            z_p = jnp.where(z_high, roll_lanes(m, -s), 0.0)
            diagonal = 3.0 * m + 0.5 * ((x_m + x_p) + (y_m + y_p) + (z_m + z_p))
            valid = inside(i)
            scaled = (damping * valid) / (diagonal + (1.0 - valid))
            half = 0.5 * scaled
            k = self.place(i)
            self.ref[0, k] = (m + x_m) * half
            self.ref[1, k] = (m + x_p) * half
            self.ref[2, k] = (m + y_m) * half
            self.ref[3, k] = (m + y_p) * half
            self.ref[4, k] = jnp.where(z_low, (m + z_m) * half, 0.0)
            self.ref[5, k] = jnp.where(z_high, (m + z_p) * half, 0.0)
            if s == 1:
                self.ref[6, k] = target(i) * scaled
                self.ref[7, k] = diagonal * (1.0 / damping)
            else:
                self.ref[6, k] = target(i) * (4.0 * scaled)
                self.ref[7, k] = 4.0 * scaled

        loop(low, high, body)

    def side(self, i):
        if self.constant is not None:
            return self.constant(i)
        return self.ref[6, self.place(i)]

    def change(self, field, i):
        s = self.step
        k = self.place(i)
        p = field(i)
        total = self.ref[0, k] * field(i - 1) + self.ref[1, k] * field(i + 1)
        total = total + (self.ref[2, k] * field(i, -1) + self.ref[3, k] * field(i, 1))
        total = total + (self.ref[4, k] * roll_lanes(p, s) + self.ref[5, k] * roll_lanes(p, -s))
        return p, (total - self.side(i)) - damping * p


def at(ref, origin, shift=None):
    return lambda i: ref[(i - origin).index(shift)]


def sweep(weights, source, result, low, high):
    def body(i):
        p, change = weights.change(source, i)
        result.put(i, p + change)

    loop(low, high, body)


def first_sweep(weights, result, low, high):
    def body(i):
        result.put(i, -weights.side(i))

    loop(low, high, body)


def restricted(first, second):
    q = first + second
    even = lanes_of(q.shape) % 2 == 0
    return 0.125 * (q + jnp.where(even, roll_lanes(q, -1), roll_lanes(q, 1)))


def packed(planes):
    even = lanes_of((HALF, LANES)) % 2 == 0
    a, b, c, d = planes
    return jnp.where(even, a, b), jnp.where(even, c, d)


def unpacked(v):
    even = lanes_of((HALF, LANES)) % 2 == 0
    planes = []
    for half in (v[:HALF], v[HALF:]):
        planes.append(jnp.where(even, half, roll_lanes(half, 1)))
        planes.append(jnp.where(even, roll_lanes(half, -1), half))
    return planes


def residual_planes(weights, field, result, result_low, low, high, scratch):
    def body(i):
        total = 0.0
        for half in range(2):
            _, change = weights.change(field, 2 * i + half)
            total = total - change * weights.ref[7, weights.place(2 * i + half)]
        k = (i - low).index()
        scratch[k] = total
        odd = scratch[k, pl.ds(1, HALF, stride=2)]
        result[(i - result_low).index()] = restricted(scratch[k, pl.ds(0, HALF, stride=2)], odd)

    loop(low, high, body)


def prolong(correction, known, result, low, high):
    def body(i):
        added = correction(i)
        for half in range(2):
            for first in range(2):
                k = 2 * i + half
                result.put_every_other(k, first, known(k, first) + added)

    loop(low, high, body)


def inside_of(first, count):
    def inside(i):
        place = i.index(first)
        return jnp.where((place >= 0) & (place < count), 1.0, 0.0)

    return inside


def whereabouts(n_chips):
    slab, cross = lax.axis_index("slab"), lax.axis_index("cross")
    chip = jnp.minimum(jnp.maximum(slab // 2, 0), n_chips - 1)
    return slab % 2 == 0, jnp.minimum(jnp.maximum(cross, 0), 3), chip


def prepare(
    velocity_in, density_in, source_in, species_in, out,
    velocity, density, source, species, semaphore,
):
    copies = [
        pltpu.make_async_copy(there, here, semaphore.at[k])
        for k, (there, here) in enumerate(
            [
                (density_in, density), (velocity_in, velocity), (source_in, source),
                (species_in, species),
            ]
        )
    ]
    for copy in copies:
        copy.start()
    lane = lanes_of((BLOCK, LANES))
    row = rows_of((BLOCK, LANES))
    copies[0].wait()
    for x in range(4):
        out[BLOCK * x : BLOCK * (x + 1)] = 1.0 / density[x]
    copies[1].wait()
    copies[2].wait()
    for x in range(4):
        u_p = velocity[0, x + 1] if x < 3 else 0.0
        u_m = velocity[0, x - 1] if x > 0 else 0.0
        v, w = velocity[1, x], velocity[2, x]
        v_p = jnp.where(row < BLOCK - 1, roll_rows(v, -1), 0.0)
        v_m = jnp.where(row > 0, roll_rows(v, 1), 0.0)
        w_p = jnp.where(lane < LANES - 1, roll_lanes(w, -1), 0.0)
        w_m = jnp.where(lane > 0, roll_lanes(w, 1), 0.0)
        moved = 0.5 * ((u_p - u_m) + (v_p - v_m) + (w_p - w_m))
        out[64 + BLOCK * x : 64 + BLOCK * (x + 1)] = moved - source[x]
        r = EDGE + x
        out[r : r + 1] = velocity[1, x, 0:1]
        out[r + 4 : r + 5] = velocity[1, x, BLOCK - 1 : BLOCK]
    out[128:144] = velocity[0, 0]
    out[144:160] = velocity[0, 3]
    copies[3].wait()
    for s in range(SPECIES):
        for x in range(4):
            r = EDGE + 8 + 4 * s + x
            out[r : r + 1] = species[s, x, 0:1]
            out[r + 36 : r + 37] = species[s, x, BLOCK - 1 : BLOCK]


def assemble(n_chips, gathered, sent, sent_far, edge):
    north, _, _ = whereabouts(n_chips)
    row = rows_of((BLOCK, LANES))
    for c in range(4):
        rows = slice(BLOCK * c, BLOCK * (c + 1))
        for k in range(2):
            block = 2 * c + k
            for x in range(4):
                sent[4 * k + x, rows] = gathered[block, BLOCK * x : BLOCK * (x + 1)]
                t = gathered[block, 64 + BLOCK * x : 64 + BLOCK * (x + 1)]
                r = EDGE + x
                if c > 0:
                    t = t - jnp.where(row == 0, 0.5 * gathered[block - 2, r + 4 : r + 5], 0.0)
                if c < 3:
                    t = t + jnp.where(row == BLOCK - 1, 0.5 * gathered[block + 2, r : r + 1], 0.0)
                if k == 0 and x == 3:
                    t = t + 0.5 * gathered[block + 1, 128:144]
                if k == 1 and x == 0:
                    t = t - 0.5 * gathered[block - 1, 144:160]
                sent[8 + 4 * k + x, rows] = t
        edge[0, rows] = gathered[2 * c, 128:144]
        edge[1, rows] = gathered[2 * c + 1, 144:160]
    sent[16] = edge[jnp.where(north, 0, 1)]
    sent_far[0] = sent[jnp.where(north, 7, 0)]
    sent_far[1] = edge[jnp.where(north, 1, 0)]


def species_edges(n_chips, species, near, beside):
    north, _, _ = whereabouts(n_chips)
    outward, inward = jnp.where(north, 0, 3), jnp.where(north, 3, 0)
    for s in range(SPECIES):
        near[BLOCK * s : BLOCK * (s + 1)] = species[s, outward]
        beside[BLOCK * s : BLOCK * (s + 1)] = species[s, inward]


def flow_rims(n_chips, gathered, u_beside, v_rims, y_low, y_high):
    north, cross, _ = whereabouts(n_chips)
    core = jnp.where(north, 0, 1)
    partner = 2 * cross + jnp.where(north, 1, 0)
    u_beside[...] = jnp.where(north, gathered[partner, 128:144], gathered[partner, 144:160])
    below = gathered[2 * jnp.maximum(cross - 1, 0) + core, EDGE:OWN]
    above = gathered[2 * jnp.minimum(cross + 1, 3) + core, EDGE:OWN]
    v_rims[0:4] = jnp.where(cross > 0, below[4:8], 0.0)
    v_rims[4:8] = jnp.where(cross < 3, above[0:4], 0.0)
    y_low[...] = jnp.where(cross > 0, below[44:80], 0.0)
    y_high[...] = jnp.where(cross < 3, above[8:44], 0.0)


def first_cycle(
    n_chips, own, edge, mine, swapped,
    mobile_ref, weights_ref, pressure_ref, residual, coarse, outer, sent,
    target_w, field_ref, rows_ref,
):
    north, _, chip = whereabouts(n_chips)
    clear_pads(mobile_ref)
    clear_pads(field_ref)
    clear_pads(pressure_ref)
    mobile_w, pressure = Field(mobile_ref, -9), Field(pressure_ref, -8)
    field = Field(field_ref, -8)

    def sides(k):
        a, b = mine[k], swapped[k]
        return jnp.where(north, a, b), jnp.where(north, b, a)

    def copy(i):
        k, later = i.index(), (i + 8).index()
        left, right = sides(k)
        mobile_w.put(i - 8, left)
        mobile_w.put(i, own[k])
        mobile_w.put(i + 8, right)
        left, right = sides(later)
        target_w[k] = left
        target_w[later] = own[later]
        target_w[(i + 16).index()] = right

    loop(0, 8, copy)
    right, left = sides(17)
    mobile_w.put(Place(0, -9), left)
    mobile_w.put(Place(0, 16), right)
    right, left = sides(18)
    target_w[0] = target_w[0] - 0.5 * left
    target_w[23] = target_w[23] + 0.5 * right
    left, right = sides(16)
    target_w[7] = target_w[7] + 0.5 * edge[0]
    target_w[8] = target_w[8] - 0.5 * left
    target_w[15] = target_w[15] + 0.5 * right
    target_w[16] = target_w[16] - 0.5 * edge[1]
    outer[...] = mine[16]

    weights = Weights(weights_ref, 1, -8)
    weights.fill(-8, 16, mobile_w, at(target_w, -8), inside_of(8 * chip, 8 * n_chips))
    first_sweep(weights, field, -8, 16)
    sweep(weights, field, pressure, -7, 15)
    residual_planes(weights, pressure, residual, -3, -3, 7, rows_ref)

    def restrict(i):
        rows = [
            mobile_w.every_other(2 * i, first) + mobile_w.every_other(2 * i + 1, first)
            for first in range(2)
        ]
        coarse[(i + 4).index()] = restricted(*rows)

    loop(-4, 8, restrict)
    r = jnp.where(north, 6, 0)
    sent[0:32], sent[32:64] = packed([residual[r + k] for k in range(4)])
    m = jnp.where(north, 8, 0)
    sent[64:96], sent[96:128] = packed([coarse[m + k] for k in range(4)])


def coarse_sweeps(weights, one, two, low, high):
    first_sweep(weights, one, low, high)
    sweep(weights, one, two, low + 1, high - 1)
    sweep(weights, two, one, low + 2, high - 2)
    sweep(weights, one, two, low + 3, high - 3)


def inner(n_chips, chip):
    return chip > 0, chip < n_chips - 1


def second_cycle(
    n_chips, weights_ref, pressure_ref, residual, coarse, got,
    pressure_new_ref, residual_new, coarse_weights_ref, sent,
    coarse_ref, residual_w, one_ref, two_ref, field_ref, other_ref, rows_ref,
):
    north, _, chip = whereabouts(n_chips)
    before, after = inner(n_chips, chip)
    for ref in (pressure_new_ref, coarse_ref, one_ref, two_ref, field_ref, other_ref):
        clear_pads(ref)
    coarse_w, one, two = Field(coarse_ref, -8), Field(one_ref, -7), Field(two_ref, -7)
    field, other = Field(field_ref, -8), Field(other_ref, -8)
    pressure, pressure_new = Field(pressure_ref, -8), Field(pressure_new_ref, -3)

    left = unpacked(jnp.where(before, got[0, 0:64], 0.0))
    right = unpacked(jnp.where(after, got[1, 128:192], 0.0))
    for i in range(4):
        residual_w[i] = left[i]
        residual_w[14 + i] = right[i]
    left = unpacked(jnp.where(before, got[0, 64:128], 0.0))
    right = unpacked(jnp.where(after, got[1, 192:256], 0.0))
    for i in range(4):
        coarse_w.put(Place(0, i - 8), left[i])
        coarse_w.put(Place(0, i + 8), right[i])

    def copy_residual(i):
        residual_w[(i + 4).index()] = residual[i.index()]

    def copy_coarse(i):
        coarse_w.put(i - 4, coarse[i.index()])

    loop(0, 10, copy_residual)
    loop(0, 12, copy_coarse)

    coarse_weights = Weights(coarse_weights_ref, 2, -7)
    coarse_weights.fill(-7, 11, coarse_w, at(residual_w, -7), inside_of(4 * chip, 4 * n_chips))
    coarse_sweeps(coarse_weights, one, two, -7, 11)

    prolong(two, pressure.every_other, field, -4, 8)

    weights = Weights(weights_ref, 1, -8)
    sweep(weights, field, other, -6, 14)
    sweep(weights, other, field, -5, 13)
    sweep(weights, field, other, -4, 12)
    sweep(weights, other, pressure_new, -3, 11)
    residual_planes(weights, pressure_new, residual_new, -1, -1, 5, rows_ref)
    sent[0] = pressure_new_ref[jnp.where(north, 6, 7), PAD : PAD + ROWS]
    r = jnp.where(north, 2, 0)
    sent[1, 0:32], sent[1, 32:64] = packed([residual_new[r + k] for k in range(4)])


def finish(
    n_chips, mobile_ref, weights_ref, pressure, residual, coarse_weights_ref, got, swapped,
    velocity, species, outer, u_beside, v_rims, outer_rim, sides, y_low, y_high,
    velocity_out, pressure_out, species_out,
    residual_w, pressure_w, one_ref, two_ref, field_ref, other_ref, final_pad,
):
    north, cross, chip = whereabouts(n_chips)
    before, after = inner(n_chips, chip)
    for ref in (one_ref, two_ref, field_ref, other_ref, final_pad):
        clear_pads(ref)
    one, two = Field(one_ref, -5), Field(two_ref, -5)
    field, other, final = Field(field_ref, -4), Field(other_ref, -4), Field(final_pad, -2)
    left = unpacked(jnp.where(before, swapped[0, 0], 0.0))
    right = unpacked(jnp.where(after, swapped[1, 1], 0.0))
    for i in range(4):
        residual_w[i] = left[i]
        residual_w[10 + i] = right[i]
    for i in range(6):
        residual_w[4 + i] = residual[i]
    pressure_w[0] = jnp.where(before, got[0, 0], 0.0)
    pressure_w[15] = jnp.where(after, got[1, 0], 0.0)
    known = Field(pressure, -3)

    def copy_pressure(i):
        pressure_w[(i + 4).index()] = known(i)

    loop(-3, 11, copy_pressure)

    shift, coarse_shift = jnp.where(north, 0, 4), jnp.where(north, 0, 2)
    coarse_weights = Weights(coarse_weights_ref, 2, -7, coarse_shift, at(residual_w, -5))

    def right_side(i):
        k = (i + 5).index()
        factor = coarse_weights_ref[7, coarse_weights.place(i)]
        residual_w[k] = residual_w[(i + 5).index(coarse_shift)] * factor

    for k in range(12):
        right_side(Place(0, k - 5))
    coarse_sweeps(coarse_weights, one, two, -5, 7)

    def known_rows(i, first):
        return pressure_w[(i + 4).index(shift), pl.ds(first, HALF, stride=2)]

    prolong(two, known_rows, field, -2, 4)

    weights = Weights(weights_ref, 1, -8, shift)
    sweep(weights, field, other, -3, 7)
    sweep(weights, other, final, -2, 6)

    start = pl.multiple_of(cross * BLOCK, BLOCK)
    own = pl.ds(start + 8, BLOCK)
    row, lane = rows_of((BLOCK, LANES)), lanes_of((BLOCK, LANES))

    beyond = outer[pl.ds(start, BLOCK)]
    u_low = jnp.where(north, beyond, u_beside[...])
    u_high = jnp.where(north, u_beside[...], beyond)

    def u_out(x):
        if x < 0:
            u = u_low
        elif x > 3:
            u = u_high
        else:
            u = velocity[0, x]
        slope = 0.5 * (final_pad[x + 3, own] - final_pad[x + 1, own])
        return u - mobile_ref[shift + (x + 9), own] * slope

    u = [u_out(x) for x in range(-1, 5)]

    def species_beside(s, side):
        outside = outer_rim[BLOCK * s : BLOCK * (s + 1)]
        inside = sides[side, 256 + BLOCK * s : 272 + BLOCK * s]
        return jnp.where(north, outside, inside) if side == 0 else jnp.where(north, inside, outside)

    wide = pl.ds(start, 32)
    for x in range(4):
        p = final_pad[x + 2, wide]
        m = mobile_ref[shift + (x + 9), wide]
        p_own = p[8:24]
        v = velocity[1, x] - m[8:24] * (0.5 * (p[9:25] - p[7:23]))
        v_low = v_rims[x : x + 1] - m[7:8] * (0.5 * (p[8:9] - p[6:7]))
        v_high = v_rims[4 + x : 5 + x] - m[24:25] * (0.5 * (p[25:26] - p[23:24]))
        p_zp = jnp.where(lane < LANES - 1, roll_lanes(p_own, -1), 0.0)
        p_zm = jnp.where(lane > 0, roll_lanes(p_own, 1), 0.0)
        w = velocity[2, x] - m[8:24] * (0.5 * (p_zp - p_zm))
        velocity_out[0, x] = u[x + 1]
        velocity_out[1, x] = v
        velocity_out[2, x] = w
        pressure_out[x] = p_own

        flow_xm, flow_xp = 0.5 * (u[x] + u[x + 1]), 0.5 * (u[x + 1] + u[x + 2])
        v_m = jnp.where(row == 0, v_low, roll_rows(v, 1))
        v_p = jnp.where(row == BLOCK - 1, v_high, roll_rows(v, -1))
        flow_ym, flow_yp = 0.5 * (v_m + v), 0.5 * (v + v_p)
        w_m = jnp.where(lane > 0, roll_lanes(w, 1), 0.0)
        w_p = jnp.where(lane < LANES - 1, roll_lanes(w, -1), 0.0)
        flow_zm, flow_zp = 0.5 * (w_m + w), 0.5 * (w + w_p)

        def leaves(high, low):
            return jnp.maximum(high, 0.0) - jnp.minimum(low, 0.0)

        keep = 1.0 - time_step * (
            leaves(flow_xp, flow_xm) + leaves(flow_yp, flow_ym) + leaves(flow_zp, flow_zm)
        )
        from_xm, from_xp = (
            time_step * jnp.maximum(flow_xm, 0.0),
            -time_step * jnp.minimum(flow_xp, 0.0),
        )
        from_ym, from_yp = (
            time_step * jnp.maximum(flow_ym, 0.0),
            -time_step * jnp.minimum(flow_yp, 0.0),
        )
        from_zm = jnp.where(lane > 0, time_step * jnp.maximum(flow_zm, 0.0), 0.0)
        from_zp = jnp.where(lane < LANES - 1, -time_step * jnp.minimum(flow_zp, 0.0), 0.0)
        for s in range(SPECIES):
            c = species[s, x]
            if x > 0:
                c_xm = species[s, x - 1]
            else:
                c_xm = species_beside(s, 0)
            if x < 3:
                c_xp = species[s, x + 1]
            else:
                c_xp = species_beside(s, 1)
            r = 4 * s + x
            c_ym = jnp.where(row == 0, y_low[r : r + 1], roll_rows(c, 1))
            c_yp = jnp.where(row == BLOCK - 1, y_high[r : r + 1], roll_rows(c, -1))
            total = keep * c + (from_xm * c_xm + from_xp * c_xp)
            total = total + (from_ym * c_ym + from_yp * c_yp)
            total = total + (from_zm * roll_lanes(c, 1) + from_zp * roll_lanes(c, -1))
            species_out[s, x] = total


def call(kernel, outs, scratch, *operands, where=pltpu.VMEM, semaphores=0, grant=24):
    vmem = pl.BlockSpec(memory_space=pltpu.VMEM)
    shapes = [jax.ShapeDtypeStruct(shape, jnp.float32) for shape in outs]
    scratch = [pltpu.VMEM(shape, jnp.float32) for shape in scratch]
    if semaphores:
        scratch = [*scratch, pltpu.SemaphoreType.DMA((semaphores,))]
    return pl.pallas_call(
        kernel,
        out_shape=shapes,
        in_specs=[pl.BlockSpec(memory_space=where) for _ in operands],
        out_specs=[vmem for _ in outs],
        scratch_shapes=scratch,
        cost_estimate=pl.CostEstimate(flops=1000000, bytes_accessed=1000000, transcendentals=0),
        compiler_params=pltpu.CompilerParams(vmem_limit_bytes=grant * 2**20),
        interpret=INTERPRET,
    )(*operands)


def gathered_over(array, groups):
    return lax.all_gather(array, ("slab", "cross"), axis_index_groups=groups)


def local(n_chips, velocity, density, source, species):
    def device(slab, cross):
        return 4 * slab + cross

    chips = [[device(2 * j + k, c) for c in range(4) for k in range(2)] for j in range(n_chips)]
    cores = [
        [device(2 * j, c), device(2 * j + 1, c)] for j in range(n_chips) for c in range(4)
    ]
    facing = [
        [device(2 * j + 1, c), device(2 * j + 2, c)] for j in range(n_chips - 1) for c in range(4)
    ]
    for slab in (0, 2 * n_chips - 1):
        facing += [[device(slab, 0), device(slab, 1)], [device(slab, 2), device(slab, 3)]]

    def both_ways(pairs):
        return [pair for left, right in pairs for pair in ((left, right), (right, left))]

    beside = both_ways([(2 * j + 1, 2 * j + 2) for j in range(n_chips - 1)])
    two_away = both_ways([(2 * j, 2 * j + 5) for j in range(n_chips - 2)])

    within = [pair for j in range(n_chips) for pair in ((2 * j, 2 * j + 1), (2 * j + 1, 2 * j))]

    def plane(n):
        return (n, ROWS, LANES)

    def padded(n, rows=ROWS):
        return (n, rows + 2 * PAD, LANES)

    def halved(n):
        return (n, HALF, LANES)

    def bind(kernel):
        return functools.partial(kernel, n_chips)

    (own,) = call(
        prepare, [(OWN, LANES)], [velocity.shape, density.shape, source.shape, species.shape],
        velocity, density, source, species,
        where=HBM, semaphores=4, grant=63,
    )
    gathered = gathered_over(own, chips)
    sent, sent_far, edge = call(bind(assemble), [plane(17), plane(2), plane(2)], [], gathered)
    near = lax.ppermute(sent, "slab", beside)
    far = lax.ppermute(sent_far, "slab", two_away)
    species_near, species_beside = call(
        bind(species_edges), [(144, LANES), (144, LANES)], [], species
    )
    outer_rim = lax.ppermute(species_near, "slab", beside)
    u_beside, v_rims, y_low, y_high = call(
        bind(flow_rims), [(BLOCK, LANES), (8, LANES), (36, LANES), (36, LANES)], [], gathered
    )
    mine = jnp.concatenate([near, far], 0)
    swapped = lax.ppermute(mine, "slab", within)
    mobile_w, weights, pressure, residual, coarse, outer, sent_two = call(
        bind(first_cycle),
        [
            padded(26), (8, *plane(24)), padded(24), halved(10), halved(12), PLANE, (128, LANES),
        ],
        [plane(24), padded(24), plane(10)],
        sent, edge, mine, swapped,
    )
    near = gathered_over(sent_two, facing).reshape(256, LANES)
    sides = gathered_over(jnp.concatenate([near, species_beside], 0), cores)
    pressure, residual, coarse_weights, sent = call(
        bind(second_cycle),
        [padded(14), halved(6), (8, *halved(18)), plane(2)],
        [
            padded(20, HALF), halved(18), padded(18, HALF), padded(18, HALF), padded(24), padded(24),
            plane(6),
        ],
        weights, pressure, residual, coarse, sides,
    )
    near = gathered_over(sent, facing)
    swapped = gathered_over(near[:, 1], cores)
    return call(
        bind(finish),
        [velocity.shape, density.shape, species.shape],
        [
            halved(14), plane(16), padded(12, HALF), padded(12, HALF), padded(12), padded(12),
            padded(8),
        ],
        mobile_w, weights, pressure, residual, coarse_weights, near, swapped,
        velocity, species, outer, u_beside, v_rims, outer_rim, sides, y_low, y_high,
    )


def solution(mesh):
    n_chips = mesh.shape["slab"] // 2
    block = P("slab", "cross", None)
    stack = P(None, "slab", "cross", None)

    def step(*arrays):
        return tuple(local(n_chips, *arrays))

    return jax.shard_map(
        step,
        mesh=mesh,
        in_specs=(stack, block, block, stack),
        out_specs=(stack, block, stack),
        check_vma=False,
    )
```

```python
import functools

import jax
import jax.numpy as jnp
from jax import lax
from jax.experimental import pallas as pl
from jax.experimental.pallas import tpu as pltpu
from jax.sharding import PartitionSpec as P


INTERPRET = False
HBM = pltpu.HBM
ROWS = 64
LANES = 128
BLOCK = 16
SPECIES = 9
EDGE = 160
OWN = EDGE + 8
damping = 0.8
time_step = 0.25


class Place:
    def __init__(self, counter, constant):
        self.counter = counter
        self.constant = constant

    def __add__(self, other):
        return Place(self.counter, self.constant + other)

    def __sub__(self, other):
        return Place(self.counter, self.constant - other)

    def __rmul__(self, factor):
        return Place(self.counter * factor, self.constant * factor)

    def index(self, shift=None):
        start = self.counter if shift is None else self.counter + shift
        return start + self.constant


def loop(low, high, body):
    for u in range(high - low):
        body(Place(0, low + u))


def rows_of(shape):
    return lax.broadcasted_iota(jnp.int32, shape, 0)


def lanes_of(shape):
    return lax.broadcasted_iota(jnp.int32, shape, 1)


PLANE = (ROWS, LANES)


def roll_rows(x, by):
    return pltpu.roll(x, by % x.shape[0], 0)


def roll_lanes(x, by):
    return pltpu.roll(x, by % x.shape[1], 1)


PAD = 8
HALF = ROWS // 2


class Field:
    def __init__(self, ref, low, shift=None):
        self.ref = ref
        self.low = low
        self.shift = shift
        self.rows = ref.shape[1] - 2 * PAD

    def __call__(self, i, rows=0):
        k = (i - self.low).index(self.shift)
        return self.ref[k, PAD + rows : PAD + rows + self.rows]

    def put(self, i, value):
        self.ref[(i - self.low).index(), PAD : PAD + self.rows] = value

    def every_other(self, i, first):
        return self.ref[(i - self.low).index(), pl.ds(PAD + first, HALF, stride=2)]

    def put_every_other(self, i, first, value):
        self.ref[(i - self.low).index(), pl.ds(PAD + first, HALF, stride=2)] = value


def clear_pads(ref):
    nothing = jnp.zeros((PAD, LANES), jnp.float32)
    for k in range(ref.shape[0]):
        ref[k, 0:PAD] = nothing
        ref[k, ref.shape[1] - PAD :] = nothing


class Weights:
    def __init__(self, ref, step, low, shift=None, constant=None):
        self.ref = ref
        self.step = step
        self.low = low
        self.shift = shift
        self.constant = constant

    def place(self, i):
        return (i - self.low).index(self.shift)

    def fill(self, low, high, mobile, target, inside):
        s = self.step
        lane = lanes_of((mobile.rows, LANES))
        z_low, z_high = lane >= s, lane < LANES - s

        def body(i):
            m = mobile(i)
            x_m, x_p = mobile(i - 1), mobile(i + 1)
            y_m, y_p = mobile(i, -1), mobile(i, 1)
            z_m = jnp.where(z_low, roll_lanes(m, s), 0.0)
            z_p = jnp.where(z_high, roll_lanes(m, -s), 0.0)
            diagonal = 3.0 * m + 0.5 * ((x_m + x_p) + (y_m + y_p) + (z_m + z_p))
            valid = inside(i)
            scaled = (damping * valid) / (diagonal + (1.0 - valid))
            half = 0.5 * scaled
            k = self.place(i)
            self.ref[0, k] = (m + x_m) * half
            self.ref[1, k] = (m + x_p) * half
            self.ref[2, k] = (m + y_m) * half
            self.ref[3, k] = (m + y_p) * half
            self.ref[4, k] = jnp.where(z_low, (m + z_m) * half, 0.0)
            self.ref[5, k] = jnp.where(z_high, (m + z_p) * half, 0.0)
            if s == 1:
                self.ref[6, k] = target(i) * scaled
                self.ref[7, k] = diagonal * (1.0 / damping)
            else:
                self.ref[6, k] = target(i) * (4.0 * scaled)
                self.ref[7, k] = 4.0 * scaled

        loop(low, high, body)

    def side(self, i):
        if self.constant is not None:
            return self.constant(i)
        return self.ref[6, self.place(i)]

    def change(self, field, i):
        s = self.step
        k = self.place(i)
        p = field(i)
        total = self.ref[0, k] * field(i - 1) + self.ref[1, k] * field(i + 1)
        total = total + (self.ref[2, k] * field(i, -1) + self.ref[3, k] * field(i, 1))
        total = total + (self.ref[4, k] * roll_lanes(p, s) + self.ref[5, k] * roll_lanes(p, -s))
        return p, (total - self.side(i)) - damping * p


def at(ref, origin, shift=None):
    return lambda i: ref[(i - origin).index(shift)]


def sweep(weights, source, result, low, high):
    def body(i):
        p, change = weights.change(source, i)
        result.put(i, p + change)

    loop(low, high, body)


def first_sweep(weights, result, low, high):
    def body(i):
        result.put(i, -weights.side(i))

    loop(low, high, body)


def restricted(first, second):
    q = first + second
    even = lanes_of(q.shape) % 2 == 0
    return 0.125 * (q + jnp.where(even, roll_lanes(q, -1), roll_lanes(q, 1)))


def packed(planes):
    even = lanes_of((HALF, LANES)) % 2 == 0
    a, b, c, d = planes
    return jnp.where(even, a, b), jnp.where(even, c, d)


def unpacked(v):
    even = lanes_of((HALF, LANES)) % 2 == 0
    planes = []
    for half in (v[:HALF], v[HALF:]):
        planes.append(jnp.where(even, half, roll_lanes(half, 1)))
        planes.append(jnp.where(even, roll_lanes(half, -1), half))
    return planes


def residual_planes(weights, field, result, result_low, low, high, scratch):
    def body(i):
        total = 0.0
        for half in range(2):
            _, change = weights.change(field, 2 * i + half)
            total = total - change * weights.ref[7, weights.place(2 * i + half)]
        k = (i - low).index()
        scratch[k] = total
        odd = scratch[k, pl.ds(1, HALF, stride=2)]
        result[(i - result_low).index()] = restricted(scratch[k, pl.ds(0, HALF, stride=2)], odd)

    loop(low, high, body)


def prolong(correction, known, result, low, high):
    def body(i):
        added = correction(i)
        for half in range(2):
            for first in range(2):
                k = 2 * i + half
                result.put_every_other(k, first, known(k, first) + added)

    loop(low, high, body)


def inside_of(first, count):
    def inside(i):
        place = i.index(first)
        return jnp.where((place >= 0) & (place < count), 1.0, 0.0)

    return inside


def whereabouts(n_chips):
    slab, cross = lax.axis_index("slab"), lax.axis_index("cross")
    chip = jnp.minimum(jnp.maximum(slab // 2, 0), n_chips - 1)
    return slab % 2 == 0, jnp.minimum(jnp.maximum(cross, 0), 3), chip


def prepare(
    velocity_in, density_in, source_in, out, velocity, density, source, semaphore
):
    copies = [
        pltpu.make_async_copy(there, here, semaphore.at[k])
        for k, (there, here) in enumerate(
            [
                (density_in, density), (velocity_in, velocity), (source_in, source),
            ]
        )
    ]
    for copy in copies:
        copy.start()
    lane = lanes_of((BLOCK, LANES))
    row = rows_of((BLOCK, LANES))
    copies[0].wait()
    for x in range(4):
        out[BLOCK * x : BLOCK * (x + 1)] = 1.0 / density[x]
    copies[1].wait()
    copies[2].wait()
    for x in range(4):
        u_p = velocity[0, x + 1] if x < 3 else 0.0
        u_m = velocity[0, x - 1] if x > 0 else 0.0
        v, w = velocity[1, x], velocity[2, x]
        v_p = jnp.where(row < BLOCK - 1, roll_rows(v, -1), 0.0)
        v_m = jnp.where(row > 0, roll_rows(v, 1), 0.0)
        w_p = jnp.where(lane < LANES - 1, roll_lanes(w, -1), 0.0)
        w_m = jnp.where(lane > 0, roll_lanes(w, 1), 0.0)
        moved = 0.5 * ((u_p - u_m) + (v_p - v_m) + (w_p - w_m))
        out[64 + BLOCK * x : 64 + BLOCK * (x + 1)] = moved - source[x]
        r = EDGE + x
        out[r : r + 1] = velocity[1, x, 0:1]
        out[r + 4 : r + 5] = velocity[1, x, BLOCK - 1 : BLOCK]
    out[128:144] = velocity[0, 0]
    out[144:160] = velocity[0, 3]


def assemble(n_chips, gathered, sent, sent_far, edge):
    north, _, _ = whereabouts(n_chips)
    row = rows_of((BLOCK, LANES))
    for c in range(4):
        rows = slice(BLOCK * c, BLOCK * (c + 1))
        for k in range(2):
            block = 2 * c + k
            for x in range(4):
                sent[4 * k + x, rows] = gathered[block, BLOCK * x : BLOCK * (x + 1)]
                t = gathered[block, 64 + BLOCK * x : 64 + BLOCK * (x + 1)]
                r = EDGE + x
                if c > 0:
                    t = t - jnp.where(row == 0, 0.5 * gathered[block - 2, r + 4 : r + 5], 0.0)
                if c < 3:
                    t = t + jnp.where(row == BLOCK - 1, 0.5 * gathered[block + 2, r : r + 1], 0.0)
                if k == 0 and x == 3:
                    t = t + 0.5 * gathered[block + 1, 128:144]
                if k == 1 and x == 0:
                    t = t - 0.5 * gathered[block - 1, 144:160]
                sent[8 + 4 * k + x, rows] = t
        edge[0, rows] = gathered[2 * c, 128:144]
        edge[1, rows] = gathered[2 * c + 1, 144:160]
    sent[16] = edge[jnp.where(north, 0, 1)]
    sent_far[0] = sent[jnp.where(north, 7, 0)]
    sent_far[1] = edge[jnp.where(north, 1, 0)]


def species_edges(n_chips, species, near, beside, edge_low, edge_high):
    north, _, _ = whereabouts(n_chips)
    outward, inward = jnp.where(north, 0, 3), jnp.where(north, 3, 0)
    for s in range(SPECIES):
        near[BLOCK * s : BLOCK * (s + 1)] = species[s, outward]
        beside[BLOCK * s : BLOCK * (s + 1)] = species[s, inward]
        for x in range(4):
            r = 4 * s + x
            edge_low[r : r + 1] = species[s, x, 0:1]
            edge_high[r : r + 1] = species[s, x, BLOCK - 1 : BLOCK]


def flow_rims(n_chips, gathered, u_beside, v_rims):
    north, cross, _ = whereabouts(n_chips)
    core = jnp.where(north, 0, 1)
    partner = 2 * cross + jnp.where(north, 1, 0)
    u_beside[...] = jnp.where(north, gathered[partner, 128:144], gathered[partner, 144:160])
    below = gathered[2 * jnp.maximum(cross - 1, 0) + core, EDGE:OWN]
    above = gathered[2 * jnp.minimum(cross + 1, 3) + core, EDGE:OWN]
    v_rims[0:4] = jnp.where(cross > 0, below[4:8], 0.0)
    v_rims[4:8] = jnp.where(cross < 3, above[0:4], 0.0)


def first_cycle(
    n_chips, own, edge, mine, swapped,
    mobile_ref, weights_ref, pressure_ref, residual, coarse, outer, sent,
    target_w, field_ref, rows_ref,
):
    north, _, chip = whereabouts(n_chips)
    clear_pads(mobile_ref)
    clear_pads(field_ref)
    clear_pads(pressure_ref)
    mobile_w, pressure = Field(mobile_ref, -9), Field(pressure_ref, -8)
    field = Field(field_ref, -8)

    def sides(k):
        a, b = mine[k], swapped[k]
        return jnp.where(north, a, b), jnp.where(north, b, a)

    def copy(i):
        k, later = i.index(), (i + 8).index()
        left, right = sides(k)
        mobile_w.put(i - 8, left)
        mobile_w.put(i, own[k])
        mobile_w.put(i + 8, right)
        left, right = sides(later)
        target_w[k] = left
        target_w[later] = own[later]
        target_w[(i + 16).index()] = right

    loop(0, 8, copy)
    right, left = sides(17)
    mobile_w.put(Place(0, -9), left)
    mobile_w.put(Place(0, 16), right)
    right, left = sides(18)
    target_w[0] = target_w[0] - 0.5 * left
    target_w[23] = target_w[23] + 0.5 * right
    left, right = sides(16)
    target_w[7] = target_w[7] + 0.5 * edge[0]
    target_w[8] = target_w[8] - 0.5 * left
    target_w[15] = target_w[15] + 0.5 * right
    target_w[16] = target_w[16] - 0.5 * edge[1]
    outer[...] = mine[16]

    weights = Weights(weights_ref, 1, -8)
    weights.fill(-8, 16, mobile_w, at(target_w, -8), inside_of(8 * chip, 8 * n_chips))
    first_sweep(weights, field, -8, 16)
    sweep(weights, field, pressure, -7, 15)
    residual_planes(weights, pressure, residual, -3, -3, 7, rows_ref)

    def restrict(i):
        rows = [
            mobile_w.every_other(2 * i, first) + mobile_w.every_other(2 * i + 1, first)
            for first in range(2)
        ]
        coarse[(i + 4).index()] = restricted(*rows)

    loop(-4, 8, restrict)
    r = jnp.where(north, 6, 0)
    sent[0:32], sent[32:64] = packed([residual[r + k] for k in range(4)])
    m = jnp.where(north, 8, 0)
    sent[64:96], sent[96:128] = packed([coarse[m + k] for k in range(4)])


def coarse_sweeps(weights, one, two, low, high):
    first_sweep(weights, one, low, high)
    sweep(weights, one, two, low + 1, high - 1)
    sweep(weights, two, one, low + 2, high - 2)
    sweep(weights, one, two, low + 3, high - 3)


def inner(n_chips, chip):
    return chip > 0, chip < n_chips - 1


def second_cycle(
    n_chips, weights_ref, pressure_ref, residual, coarse, got,
    pressure_new_ref, residual_new, coarse_weights_ref, sent,
    coarse_ref, residual_w, one_ref, two_ref, field_ref, other_ref, rows_ref,
):
    north, _, chip = whereabouts(n_chips)
    before, after = inner(n_chips, chip)
    for ref in (pressure_new_ref, coarse_ref, one_ref, two_ref, field_ref, other_ref):
        clear_pads(ref)
    coarse_w, one, two = Field(coarse_ref, -8), Field(one_ref, -7), Field(two_ref, -7)
    field, other = Field(field_ref, -8), Field(other_ref, -8)
    pressure, pressure_new = Field(pressure_ref, -8), Field(pressure_new_ref, -3)

    left = unpacked(jnp.where(before, got[0, 0:64], 0.0))
    right = unpacked(jnp.where(after, got[1, 128:192], 0.0))
    for i in range(4):
        residual_w[i] = left[i]
        residual_w[14 + i] = right[i]
    left = unpacked(jnp.where(before, got[0, 64:128], 0.0))
    right = unpacked(jnp.where(after, got[1, 192:256], 0.0))
    for i in range(4):
        coarse_w.put(Place(0, i - 8), left[i])
        coarse_w.put(Place(0, i + 8), right[i])

    def copy_residual(i):
        residual_w[(i + 4).index()] = residual[i.index()]

    def copy_coarse(i):
        coarse_w.put(i - 4, coarse[i.index()])

    loop(0, 10, copy_residual)
    loop(0, 12, copy_coarse)

    coarse_weights = Weights(coarse_weights_ref, 2, -7)
    coarse_weights.fill(-7, 11, coarse_w, at(residual_w, -7), inside_of(4 * chip, 4 * n_chips))
    coarse_sweeps(coarse_weights, one, two, -7, 11)

    prolong(two, pressure.every_other, field, -4, 8)

    weights = Weights(weights_ref, 1, -8)
    sweep(weights, field, other, -6, 14)
    sweep(weights, other, field, -5, 13)
    sweep(weights, field, other, -4, 12)
    sweep(weights, other, pressure_new, -3, 11)
    residual_planes(weights, pressure_new, residual_new, -1, -1, 5, rows_ref)
    sent[0] = pressure_new_ref[jnp.where(north, 6, 7), PAD : PAD + ROWS]
    r = jnp.where(north, 2, 0)
    sent[1, 0:32], sent[1, 32:64] = packed([residual_new[r + k] for k in range(4)])


def finish(
    n_chips, mobile_ref, weights_ref, pressure, residual, coarse_weights_ref, got, swapped,
    velocity, species, outer, u_beside, v_rims, outer_rim, sides, y_low, y_high,
    velocity_out, pressure_out, species_out,
    residual_w, pressure_w, one_ref, two_ref, field_ref, other_ref, final_pad,
):
    north, cross, chip = whereabouts(n_chips)
    before, after = inner(n_chips, chip)
    for ref in (one_ref, two_ref, field_ref, other_ref, final_pad):
        clear_pads(ref)
    one, two = Field(one_ref, -5), Field(two_ref, -5)
    field, other, final = Field(field_ref, -4), Field(other_ref, -4), Field(final_pad, -2)
    left = unpacked(jnp.where(before, swapped[0, 0], 0.0))
    right = unpacked(jnp.where(after, swapped[1, 1], 0.0))
    for i in range(4):
        residual_w[i] = left[i]
        residual_w[10 + i] = right[i]
    for i in range(6):
        residual_w[4 + i] = residual[i]
    pressure_w[0] = jnp.where(before, got[0, 0], 0.0)
    pressure_w[15] = jnp.where(after, got[1, 0], 0.0)
    known = Field(pressure, -3)

    def copy_pressure(i):
        pressure_w[(i + 4).index()] = known(i)

    loop(-3, 11, copy_pressure)

    shift, coarse_shift = jnp.where(north, 0, 4), jnp.where(north, 0, 2)
    coarse_weights = Weights(coarse_weights_ref, 2, -7, coarse_shift, at(residual_w, -5))

    def right_side(i):
        k = (i + 5).index()
        factor = coarse_weights_ref[7, coarse_weights.place(i)]
        residual_w[k] = residual_w[(i + 5).index(coarse_shift)] * factor

    for k in range(12):
        right_side(Place(0, k - 5))
    coarse_sweeps(coarse_weights, one, two, -5, 7)

    def known_rows(i, first):
        return pressure_w[(i + 4).index(shift), pl.ds(first, HALF, stride=2)]

    prolong(two, known_rows, field, -2, 4)

    weights = Weights(weights_ref, 1, -8, shift)
    sweep(weights, field, other, -3, 7)
    sweep(weights, other, final, -2, 6)

    start = pl.multiple_of(cross * BLOCK, BLOCK)
    own = pl.ds(start + 8, BLOCK)
    row, lane = rows_of((BLOCK, LANES)), lanes_of((BLOCK, LANES))

    beyond = outer[pl.ds(start, BLOCK)]
    u_low = jnp.where(north, beyond, u_beside[...])
    u_high = jnp.where(north, u_beside[...], beyond)

    def u_out(x):
        if x < 0:
            u = u_low
        elif x > 3:
            u = u_high
        else:
            u = velocity[0, x]
        slope = 0.5 * (final_pad[x + 3, own] - final_pad[x + 1, own])
        return u - mobile_ref[shift + (x + 9), own] * slope

    u = [u_out(x) for x in range(-1, 5)]

    def species_beside(s, side):
        outside = outer_rim[BLOCK * s : BLOCK * (s + 1)]
        inside = sides[side, 256 + BLOCK * s : 272 + BLOCK * s]
        return jnp.where(north, outside, inside) if side == 0 else jnp.where(north, inside, outside)

    wide = pl.ds(start, 32)
    for x in range(4):
        p = final_pad[x + 2, wide]
        m = mobile_ref[shift + (x + 9), wide]
        p_own = p[8:24]
        v = velocity[1, x] - m[8:24] * (0.5 * (p[9:25] - p[7:23]))
        v_low = v_rims[x : x + 1] - m[7:8] * (0.5 * (p[8:9] - p[6:7]))
        v_high = v_rims[4 + x : 5 + x] - m[24:25] * (0.5 * (p[25:26] - p[23:24]))
        p_zp = jnp.where(lane < LANES - 1, roll_lanes(p_own, -1), 0.0)
        p_zm = jnp.where(lane > 0, roll_lanes(p_own, 1), 0.0)
        w = velocity[2, x] - m[8:24] * (0.5 * (p_zp - p_zm))
        velocity_out[0, x] = u[x + 1]
        velocity_out[1, x] = v
        velocity_out[2, x] = w
        pressure_out[x] = p_own

        flow_xm, flow_xp = 0.5 * (u[x] + u[x + 1]), 0.5 * (u[x + 1] + u[x + 2])
        v_m = jnp.where(row == 0, v_low, roll_rows(v, 1))
        v_p = jnp.where(row == BLOCK - 1, v_high, roll_rows(v, -1))
        flow_ym, flow_yp = 0.5 * (v_m + v), 0.5 * (v + v_p)
        w_m = jnp.where(lane > 0, roll_lanes(w, 1), 0.0)
        w_p = jnp.where(lane < LANES - 1, roll_lanes(w, -1), 0.0)
        flow_zm, flow_zp = 0.5 * (w_m + w), 0.5 * (w + w_p)

        def leaves(high, low):
            return jnp.maximum(high, 0.0) - jnp.minimum(low, 0.0)

        keep = 1.0 - time_step * (
            leaves(flow_xp, flow_xm) + leaves(flow_yp, flow_ym) + leaves(flow_zp, flow_zm)
        )
        from_xm, from_xp = (
            time_step * jnp.maximum(flow_xm, 0.0),
            -time_step * jnp.minimum(flow_xp, 0.0),
        )
        from_ym, from_yp = (
            time_step * jnp.maximum(flow_ym, 0.0),
            -time_step * jnp.minimum(flow_yp, 0.0),
        )
        from_zm = jnp.where(lane > 0, time_step * jnp.maximum(flow_zm, 0.0), 0.0)
        from_zp = jnp.where(lane < LANES - 1, -time_step * jnp.minimum(flow_zp, 0.0), 0.0)
        for s in range(SPECIES):
            c = species[s, x]
            if x > 0:
                c_xm = species[s, x - 1]
            else:
                c_xm = species_beside(s, 0)
            if x < 3:
                c_xp = species[s, x + 1]
            else:
                c_xp = species_beside(s, 1)
            r = 4 * s + x
            c_ym = jnp.where(row == 0, y_low[r : r + 1], roll_rows(c, 1))
            c_yp = jnp.where(row == BLOCK - 1, y_high[r : r + 1], roll_rows(c, -1))
            total = keep * c + (from_xm * c_xm + from_xp * c_xp)
            total = total + (from_ym * c_ym + from_yp * c_yp)
            total = total + (from_zm * roll_lanes(c, 1) + from_zp * roll_lanes(c, -1))
            species_out[s, x] = total


def call(kernel, outs, scratch, *operands, where=pltpu.VMEM, semaphores=0, grant=24):
    vmem = pl.BlockSpec(memory_space=pltpu.VMEM)
    shapes = [jax.ShapeDtypeStruct(shape, jnp.float32) for shape in outs]
    scratch = [pltpu.VMEM(shape, jnp.float32) for shape in scratch]
    if semaphores:
        scratch = [*scratch, pltpu.SemaphoreType.DMA((semaphores,))]
    return pl.pallas_call(
        kernel,
        out_shape=shapes,
        in_specs=[pl.BlockSpec(memory_space=where) for _ in operands],
        out_specs=[vmem for _ in outs],
        scratch_shapes=scratch,
        cost_estimate=pl.CostEstimate(flops=1000000, bytes_accessed=1000000, transcendentals=0),
        compiler_params=pltpu.CompilerParams(vmem_limit_bytes=grant * 2**20),
        interpret=INTERPRET,
    )(*operands)


def gathered_over(array, groups):
    return lax.all_gather(array, ("slab", "cross"), axis_index_groups=groups)


def local(n_chips, velocity, density, source, species):
    def device(slab, cross):
        return 4 * slab + cross

    chips = [[device(2 * j + k, c) for c in range(4) for k in range(2)] for j in range(n_chips)]
    cores = [
        [device(2 * j, c), device(2 * j + 1, c)] for j in range(n_chips) for c in range(4)
    ]
    facing = [
        [device(2 * j + 1, c), device(2 * j + 2, c)] for j in range(n_chips - 1) for c in range(4)
    ]
    for slab in (0, 2 * n_chips - 1):
        facing += [[device(slab, 0), device(slab, 1)], [device(slab, 2), device(slab, 3)]]

    def both_ways(pairs):
        return [pair for left, right in pairs for pair in ((left, right), (right, left))]

    beside = both_ways([(2 * j + 1, 2 * j + 2) for j in range(n_chips - 1)])
    two_away = both_ways([(2 * j, 2 * j + 5) for j in range(n_chips - 2)])

    within = [pair for j in range(n_chips) for pair in ((2 * j, 2 * j + 1), (2 * j + 1, 2 * j))]

    def plane(n):
        return (n, ROWS, LANES)

    def padded(n, rows=ROWS):
        return (n, rows + 2 * PAD, LANES)

    def halved(n):
        return (n, HALF, LANES)

    def bind(kernel):
        return functools.partial(kernel, n_chips)

    (own,) = call(
        prepare, [(OWN, LANES)], [velocity.shape, density.shape, source.shape],
        velocity, density, source,
        where=HBM, semaphores=3, grant=63,
    )
    gathered = gathered_over(own, chips)
    sent, sent_far, edge = call(bind(assemble), [plane(17), plane(2), plane(2)], [], gathered)
    near = lax.ppermute(sent, "slab", beside)
    far = lax.ppermute(sent_far, "slab", two_away)
    species_near, species_beside, edge_low, edge_high = call(
        bind(species_edges), [(144, LANES), (144, LANES), (36, LANES), (36, LANES)], [], species
    )
    y_low = lax.ppermute(edge_high, "cross", [(c, c + 1) for c in range(3)])
    y_high = lax.ppermute(edge_low, "cross", [(c + 1, c) for c in range(3)])
    outer_rim = lax.ppermute(species_near, "slab", beside)
    u_beside, v_rims = call(bind(flow_rims), [(BLOCK, LANES), (8, LANES)], [], gathered)
    mine = jnp.concatenate([near, far], 0)
    swapped = lax.ppermute(mine, "slab", within)
    mobile_w, weights, pressure, residual, coarse, outer, sent_two = call(
        bind(first_cycle),
        [
            padded(26), (8, *plane(24)), padded(24), halved(10), halved(12), PLANE, (128, LANES),
        ],
        [plane(24), padded(24), plane(10)],
        sent, edge, mine, swapped,
    )
    near = gathered_over(sent_two, facing).reshape(256, LANES)
    sides = gathered_over(jnp.concatenate([near, species_beside], 0), cores)
    pressure, residual, coarse_weights, sent = call(
        bind(second_cycle),
        [padded(14), halved(6), (8, *halved(18)), plane(2)],
        [
            padded(20, HALF), halved(18), padded(18, HALF), padded(18, HALF), padded(24), padded(24),
            plane(6),
        ],
        weights, pressure, residual, coarse, sides,
    )
    near = gathered_over(sent, facing)
    swapped = gathered_over(near[:, 1], cores)
    return call(
        bind(finish),
        [velocity.shape, density.shape, species.shape],
        [
            halved(14), plane(16), padded(12, HALF), padded(12, HALF), padded(12), padded(12),
            padded(8),
        ],
        mobile_w, weights, pressure, residual, coarse_weights, near, swapped,
        velocity, species, outer, u_beside, v_rims, outer_rim, sides, y_low, y_high,
    )


def solution(mesh):
    n_chips = mesh.shape["slab"] // 2
    block = P("slab", "cross", None)
    stack = P(None, "slab", "cross", None)

    def step(*arrays):
        return tuple(local(n_chips, *arrays))

    return jax.shard_map(
        step,
        mesh=mesh,
        in_specs=(stack, block, block, stack),
        out_specs=(stack, block, stack),
        check_vma=False,
    )
```

```python
import functools

import jax
import jax.numpy as jnp
from jax import lax
from jax.experimental import pallas as pl
from jax.experimental.pallas import tpu as pltpu
from jax.sharding import PartitionSpec as P


INTERPRET = False
HBM = pltpu.HBM
ROWS = 64
LANES = 128
BLOCK = 16
SPECIES = 9
EDGE = 160
OWN = EDGE + 8
damping = 0.8
time_step = 0.25


class Place:
    def __init__(self, counter, constant):
        self.counter = counter
        self.constant = constant

    def __add__(self, other):
        return Place(self.counter, self.constant + other)

    def __sub__(self, other):
        return Place(self.counter, self.constant - other)

    def __rmul__(self, factor):
        return Place(self.counter * factor, self.constant * factor)

    def index(self, shift=None):
        start = self.counter if shift is None else self.counter + shift
        return start + self.constant


def loop(low, high, body):
    for u in range(high - low):
        body(Place(0, low + u))


def rows_of(shape):
    return lax.broadcasted_iota(jnp.int32, shape, 0)


def lanes_of(shape):
    return lax.broadcasted_iota(jnp.int32, shape, 1)


PLANE = (ROWS, LANES)


def roll_rows(x, by):
    return pltpu.roll(x, by % x.shape[0], 0)


def roll_lanes(x, by):
    return pltpu.roll(x, by % x.shape[1], 1)


PAD = 8
HALF = ROWS // 2


class Field:
    def __init__(self, ref, low, shift=None):
        self.ref = ref
        self.low = low
        self.shift = shift
        self.rows = ref.shape[1] - 2 * PAD

    def __call__(self, i, rows=0):
        k = (i - self.low).index(self.shift)
        return self.ref[k, PAD + rows : PAD + rows + self.rows]

    def put(self, i, value):
        self.ref[(i - self.low).index(), PAD : PAD + self.rows] = value

    def every_other(self, i, first):
        return self.ref[(i - self.low).index(), pl.ds(PAD + first, HALF, stride=2)]

    def put_every_other(self, i, first, value):
        self.ref[(i - self.low).index(), pl.ds(PAD + first, HALF, stride=2)] = value


def clear_pads(ref):
    nothing = jnp.zeros((PAD, LANES), jnp.float32)
    for k in range(ref.shape[0]):
        ref[k, 0:PAD] = nothing
        ref[k, ref.shape[1] - PAD :] = nothing


class Weights:
    def __init__(self, ref, step, low, shift=None, constant=None):
        self.ref = ref
        self.step = step
        self.low = low
        self.shift = shift
        self.constant = constant

    def place(self, i):
        return (i - self.low).index(self.shift)

    def fill(self, low, high, mobile, target, inside):
        s = self.step
        lane = lanes_of((mobile.rows, LANES))
        z_low, z_high = lane >= s, lane < LANES - s

        def body(i):
            m = mobile(i)
            x_m, x_p = mobile(i - 1), mobile(i + 1)
            y_m, y_p = mobile(i, -1), mobile(i, 1)
            z_m = jnp.where(z_low, roll_lanes(m, s), 0.0)
            z_p = jnp.where(z_high, roll_lanes(m, -s), 0.0)
            diagonal = 3.0 * m + 0.5 * ((x_m + x_p) + (y_m + y_p) + (z_m + z_p))
            valid = inside(i)
            scaled = (damping * valid) / (diagonal + (1.0 - valid))
            half = 0.5 * scaled
            k = self.place(i)
            self.ref[0, k] = (m + x_m) * half
            self.ref[1, k] = (m + x_p) * half
            self.ref[2, k] = (m + y_m) * half
            self.ref[3, k] = (m + y_p) * half
            self.ref[4, k] = jnp.where(z_low, (m + z_m) * half, 0.0)
            self.ref[5, k] = jnp.where(z_high, (m + z_p) * half, 0.0)
            if s == 1:
                self.ref[6, k] = target(i) * scaled
                self.ref[7, k] = diagonal * (1.0 / damping)
            else:
                self.ref[6, k] = target(i) * (4.0 * scaled)
                self.ref[7, k] = 4.0 * scaled

        loop(low, high, body)

    def side(self, i):
        if self.constant is not None:
            return self.constant(i)
        return self.ref[6, self.place(i)]

    def change(self, field, i):
        s = self.step
        k = self.place(i)
        p = field(i)
        total = self.ref[0, k] * field(i - 1) + self.ref[1, k] * field(i + 1)
        total = total + (self.ref[2, k] * field(i, -1) + self.ref[3, k] * field(i, 1))
        total = total + (self.ref[4, k] * roll_lanes(p, s) + self.ref[5, k] * roll_lanes(p, -s))
        return p, (total - self.side(i)) - damping * p


def at(ref, origin, shift=None):
    return lambda i: ref[(i - origin).index(shift)]


def sweep(weights, source, result, low, high):
    def body(i):
        p, change = weights.change(source, i)
        result.put(i, p + change)

    loop(low, high, body)


def first_sweep(weights, result, low, high):
    def body(i):
        result.put(i, -weights.side(i))

    loop(low, high, body)


def restricted(first, second):
    q = first + second
    even = lanes_of(q.shape) % 2 == 0
    return 0.125 * (q + jnp.where(even, roll_lanes(q, -1), roll_lanes(q, 1)))


def packed(planes):
    even = lanes_of((HALF, LANES)) % 2 == 0
    a, b, c, d = planes
    return jnp.where(even, a, b), jnp.where(even, c, d)


def unpacked(v):
    even = lanes_of((HALF, LANES)) % 2 == 0
    planes = []
    for half in (v[:HALF], v[HALF:]):
        planes.append(jnp.where(even, half, roll_lanes(half, 1)))
        planes.append(jnp.where(even, roll_lanes(half, -1), half))
    return planes


def residual_planes(weights, field, result, result_low, low, high, scratch):
    def body(i):
        total = 0.0
        for half in range(2):
            _, change = weights.change(field, 2 * i + half)
            total = total - change * weights.ref[7, weights.place(2 * i + half)]
        k = (i - low).index()
        scratch[k] = total
        odd = scratch[k, pl.ds(1, HALF, stride=2)]
        result[(i - result_low).index()] = restricted(scratch[k, pl.ds(0, HALF, stride=2)], odd)

    loop(low, high, body)


def prolong(correction, known, result, low, high):
    def body(i):
        added = correction(i)
        for half in range(2):
            for first in range(2):
                k = 2 * i + half
                result.put_every_other(k, first, known(k, first) + added)

    loop(low, high, body)


def inside_of(first, count):
    def inside(i):
        place = i.index(first)
        return jnp.where((place >= 0) & (place < count), 1.0, 0.0)

    return inside


def whereabouts(n_chips):
    slab, cross = lax.axis_index("slab"), lax.axis_index("cross")
    chip = jnp.minimum(jnp.maximum(slab // 2, 0), n_chips - 1)
    return slab % 2 == 0, jnp.minimum(jnp.maximum(cross, 0), 3), chip


def prepare(velocity_in, density_in, source_in, out, velocity, density, source, semaphore):
    copies = [
        pltpu.make_async_copy(there, here, semaphore.at[k])
        for k, (there, here) in enumerate(
            [(density_in, density), (velocity_in, velocity), (source_in, source)]
        )
    ]
    for copy in copies:
        copy.start()
    lane = lanes_of((BLOCK, LANES))
    row = rows_of((BLOCK, LANES))
    copies[0].wait()
    for x in range(4):
        out[BLOCK * x : BLOCK * (x + 1)] = 1.0 / density[x]
    copies[1].wait()
    copies[2].wait()
    for x in range(4):
        u_p = velocity[0, x + 1] if x < 3 else 0.0
        u_m = velocity[0, x - 1] if x > 0 else 0.0
        v, w = velocity[1, x], velocity[2, x]
        v_p = jnp.where(row < BLOCK - 1, roll_rows(v, -1), 0.0)
        v_m = jnp.where(row > 0, roll_rows(v, 1), 0.0)
        w_p = jnp.where(lane < LANES - 1, roll_lanes(w, -1), 0.0)
        w_m = jnp.where(lane > 0, roll_lanes(w, 1), 0.0)
        moved = 0.5 * ((u_p - u_m) + (v_p - v_m) + (w_p - w_m))
        out[64 + BLOCK * x : 64 + BLOCK * (x + 1)] = moved - source[x]
        r = EDGE + x
        out[r : r + 1] = velocity[1, x, 0:1]
        out[r + 4 : r + 5] = velocity[1, x, BLOCK - 1 : BLOCK]
    out[128:144] = velocity[0, 0]
    out[144:160] = velocity[0, 3]


def assemble(n_chips, gathered, sent, sent_far, edge):
    north, _, _ = whereabouts(n_chips)
    row = rows_of((BLOCK, LANES))
    for c in range(4):
        rows = slice(BLOCK * c, BLOCK * (c + 1))
        for k in range(2):
            block = 2 * c + k
            for x in range(4):
                sent[4 * k + x, rows] = gathered[block, BLOCK * x : BLOCK * (x + 1)]
                t = gathered[block, 64 + BLOCK * x : 64 + BLOCK * (x + 1)]
                r = EDGE + x
                if c > 0:
                    t = t - jnp.where(row == 0, 0.5 * gathered[block - 2, r + 4 : r + 5], 0.0)
                if c < 3:
                    t = t + jnp.where(row == BLOCK - 1, 0.5 * gathered[block + 2, r : r + 1], 0.0)
                if k == 0 and x == 3:
                    t = t + 0.5 * gathered[block + 1, 128:144]
                if k == 1 and x == 0:
                    t = t - 0.5 * gathered[block - 1, 144:160]
                sent[8 + 4 * k + x, rows] = t
        edge[0, rows] = gathered[2 * c, 128:144]
        edge[1, rows] = gathered[2 * c + 1, 144:160]
    sent[16] = edge[jnp.where(north, 0, 1)]
    sent_far[0] = sent[jnp.where(north, 7, 0)]
    sent_far[1] = edge[jnp.where(north, 1, 0)]


def species_edges(n_chips, species, near, beside, edge_low, edge_high):
    north, _, _ = whereabouts(n_chips)
    outward, inward = jnp.where(north, 0, 3), jnp.where(north, 3, 0)
    for s in range(SPECIES):
        near[BLOCK * s : BLOCK * (s + 1)] = species[s, outward]
        beside[BLOCK * s : BLOCK * (s + 1)] = species[s, inward]
        for x in range(4):
            r = 4 * s + x
            edge_low[r : r + 1] = species[s, x, 0:1]
            edge_high[r : r + 1] = species[s, x, BLOCK - 1 : BLOCK]
    edge_low[36:40] = jnp.zeros((4, LANES), jnp.float32)
    edge_high[36:40] = jnp.zeros((4, LANES), jnp.float32)


def flow_rims(n_chips, gathered, u_beside, v_rims):
    north, cross, _ = whereabouts(n_chips)
    core = jnp.where(north, 0, 1)
    partner = 2 * cross + jnp.where(north, 1, 0)
    u_beside[...] = jnp.where(north, gathered[partner, 128:144], gathered[partner, 144:160])
    below = gathered[2 * jnp.maximum(cross - 1, 0) + core, EDGE:OWN]
    above = gathered[2 * jnp.minimum(cross + 1, 3) + core, EDGE:OWN]
    v_rims[0:4] = jnp.where(cross > 0, below[4:8], 0.0)
    v_rims[4:8] = jnp.where(cross < 3, above[0:4], 0.0)


def first_cycle(
    n_chips, own, edge, mine, swapped, species_near,
    mobile_ref, weights_ref, pressure_ref, residual, coarse, outer, sent,
    target_w, field_ref, rows_ref,
):
    north, _, chip = whereabouts(n_chips)
    clear_pads(mobile_ref)
    clear_pads(field_ref)
    clear_pads(pressure_ref)
    mobile_w, pressure = Field(mobile_ref, -9), Field(pressure_ref, -8)
    field = Field(field_ref, -8)

    def sides(k):
        a, b = mine[k], swapped[k]
        return jnp.where(north, a, b), jnp.where(north, b, a)

    def copy(i):
        k, later = i.index(), (i + 8).index()
        left, right = sides(k)
        mobile_w.put(i - 8, left)
        mobile_w.put(i, own[k])
        mobile_w.put(i + 8, right)
        left, right = sides(later)
        target_w[k] = left
        target_w[later] = own[later]
        target_w[(i + 16).index()] = right

    loop(0, 8, copy)
    right, left = sides(17)
    mobile_w.put(Place(0, -9), left)
    mobile_w.put(Place(0, 16), right)
    right, left = sides(18)
    target_w[0] = target_w[0] - 0.5 * left
    target_w[23] = target_w[23] + 0.5 * right
    left, right = sides(16)
    target_w[7] = target_w[7] + 0.5 * edge[0]
    target_w[8] = target_w[8] - 0.5 * left
    target_w[15] = target_w[15] + 0.5 * right
    target_w[16] = target_w[16] - 0.5 * edge[1]
    outer[...] = mine[16]

    weights = Weights(weights_ref, 1, -8)
    weights.fill(-8, 16, mobile_w, at(target_w, -8), inside_of(8 * chip, 8 * n_chips))
    first_sweep(weights, field, -8, 16)
    sweep(weights, field, pressure, -7, 15)
    residual_planes(weights, pressure, residual, -3, -3, 7, rows_ref)

    def restrict(i):
        rows = [
            mobile_w.every_other(2 * i, first) + mobile_w.every_other(2 * i + 1, first)
            for first in range(2)
        ]
        coarse[(i + 4).index()] = restricted(*rows)

    loop(-4, 8, restrict)
    r = jnp.where(north, 6, 0)
    sent[0:32], sent[32:64] = packed([residual[r + k] for k in range(4)])
    m = jnp.where(north, 8, 0)
    sent[64:96], sent[96:128] = packed([coarse[m + k] for k in range(4)])
    sent[128:272] = species_near[...]


def coarse_sweeps(weights, one, two, low, high):
    first_sweep(weights, one, low, high)
    sweep(weights, one, two, low + 1, high - 1)
    sweep(weights, two, one, low + 2, high - 2)
    sweep(weights, one, two, low + 3, high - 3)


def inner(n_chips, chip):
    return chip > 0, chip < n_chips - 1


def second_cycle(
    n_chips, weights_ref, pressure_ref, residual, coarse, got,
    pressure_new_ref, residual_new, coarse_weights_ref, sent,
    coarse_ref, residual_w, one_ref, two_ref, field_ref, other_ref, rows_ref,
):
    north, _, chip = whereabouts(n_chips)
    before, after = inner(n_chips, chip)
    for ref in (pressure_new_ref, coarse_ref, one_ref, two_ref, field_ref, other_ref):
        clear_pads(ref)
    coarse_w, one, two = Field(coarse_ref, -8), Field(one_ref, -7), Field(two_ref, -7)
    field, other = Field(field_ref, -8), Field(other_ref, -8)
    pressure, pressure_new = Field(pressure_ref, -8), Field(pressure_new_ref, -3)

    left = unpacked(jnp.where(before, got[0, 0:64], 0.0))
    right = unpacked(jnp.where(after, got[1, 272:336], 0.0))
    for i in range(4):
        residual_w[i] = left[i]
        residual_w[14 + i] = right[i]
    left = unpacked(jnp.where(before, got[0, 64:128], 0.0))
    right = unpacked(jnp.where(after, got[1, 336:400], 0.0))
    for i in range(4):
        coarse_w.put(Place(0, i - 8), left[i])
        coarse_w.put(Place(0, i + 8), right[i])

    def copy_residual(i):
        residual_w[(i + 4).index()] = residual[i.index()]

    def copy_coarse(i):
        coarse_w.put(i - 4, coarse[i.index()])

    loop(0, 10, copy_residual)
    loop(0, 12, copy_coarse)

    coarse_weights = Weights(coarse_weights_ref, 2, -7)
    coarse_weights.fill(-7, 11, coarse_w, at(residual_w, -7), inside_of(4 * chip, 4 * n_chips))
    coarse_sweeps(coarse_weights, one, two, -7, 11)

    prolong(two, pressure.every_other, field, -4, 8)

    weights = Weights(weights_ref, 1, -8)
    sweep(weights, field, other, -6, 14)
    sweep(weights, other, field, -5, 13)
    sweep(weights, field, other, -4, 12)
    sweep(weights, other, pressure_new, -3, 11)
    residual_planes(weights, pressure_new, residual_new, -1, -1, 5, rows_ref)
    sent[0] = pressure_new_ref[jnp.where(north, 6, 7), PAD : PAD + ROWS]
    r = jnp.where(north, 2, 0)
    sent[1, 0:32], sent[1, 32:64] = packed([residual_new[r + k] for k in range(4)])


def finish(
    n_chips, mobile_ref, weights_ref, pressure, residual, coarse_weights_ref, got, swapped,
    velocity, species, outer, u_beside, v_rims, sides, y_low, y_high,
    velocity_out, pressure_out, species_out,
    residual_w, pressure_w, one_ref, two_ref, field_ref, other_ref, final_pad,
):
    north, cross, chip = whereabouts(n_chips)
    before, after = inner(n_chips, chip)
    for ref in (one_ref, two_ref, field_ref, other_ref, final_pad):
        clear_pads(ref)
    one, two = Field(one_ref, -5), Field(two_ref, -5)
    field, other, final = Field(field_ref, -4), Field(other_ref, -4), Field(final_pad, -2)
    left = unpacked(jnp.where(before, swapped[0, 0], 0.0))
    right = unpacked(jnp.where(after, swapped[1, 1], 0.0))
    for i in range(4):
        residual_w[i] = left[i]
        residual_w[10 + i] = right[i]
    for i in range(6):
        residual_w[4 + i] = residual[i]
    pressure_w[0] = jnp.where(before, got[0, 0], 0.0)
    pressure_w[15] = jnp.where(after, got[1, 0], 0.0)
    known = Field(pressure, -3)

    def copy_pressure(i):
        pressure_w[(i + 4).index()] = known(i)

    loop(-3, 11, copy_pressure)

    shift, coarse_shift = jnp.where(north, 0, 4), jnp.where(north, 0, 2)
    coarse_weights = Weights(coarse_weights_ref, 2, -7, coarse_shift, at(residual_w, -5))

    def right_side(i):
        k = (i + 5).index()
        factor = coarse_weights_ref[7, coarse_weights.place(i)]
        residual_w[k] = residual_w[(i + 5).index(coarse_shift)] * factor

    for k in range(12):
        right_side(Place(0, k - 5))
    coarse_sweeps(coarse_weights, one, two, -5, 7)

    def known_rows(i, first):
        return pressure_w[(i + 4).index(shift), pl.ds(first, HALF, stride=2)]

    prolong(two, known_rows, field, -2, 4)

    weights = Weights(weights_ref, 1, -8, shift)
    sweep(weights, field, other, -3, 7)
    sweep(weights, other, final, -2, 6)

    start = pl.multiple_of(cross * BLOCK, BLOCK)
    own = pl.ds(start + 8, BLOCK)
    row, lane = rows_of((BLOCK, LANES)), lanes_of((BLOCK, LANES))

    beyond = outer[pl.ds(start, BLOCK)]
    u_low = jnp.where(north, beyond, u_beside[...])
    u_high = jnp.where(north, u_beside[...], beyond)

    def u_out(x):
        if x < 0:
            u = u_low
        elif x > 3:
            u = u_high
        else:
            u = velocity[0, x]
        slope = 0.5 * (final_pad[x + 3, own] - final_pad[x + 1, own])
        return u - mobile_ref[shift + (x + 9), own] * slope

    u = [u_out(x) for x in range(-1, 5)]

    def species_beside(s, side):
        at_rim = BLOCK * s + (128 if side == 0 else 400)
        outside = sides[side, at_rim : at_rim + BLOCK]
        outside = jnp.where(before if side == 0 else after, outside, 0.0)
        inside = sides[side, 544 + BLOCK * s : 560 + BLOCK * s]
        return jnp.where(north, outside, inside) if side == 0 else jnp.where(north, inside, outside)

    wide = pl.ds(start, 32)
    for x in range(4):
        p = final_pad[x + 2, wide]
        m = mobile_ref[shift + (x + 9), wide]
        p_own = p[8:24]
        v = velocity[1, x] - m[8:24] * (0.5 * (p[9:25] - p[7:23]))
        v_low = v_rims[x : x + 1] - m[7:8] * (0.5 * (p[8:9] - p[6:7]))
        v_high = v_rims[4 + x : 5 + x] - m[24:25] * (0.5 * (p[25:26] - p[23:24]))
        p_zp = jnp.where(lane < LANES - 1, roll_lanes(p_own, -1), 0.0)
        p_zm = jnp.where(lane > 0, roll_lanes(p_own, 1), 0.0)
        w = velocity[2, x] - m[8:24] * (0.5 * (p_zp - p_zm))
        velocity_out[0, x] = u[x + 1]
        velocity_out[1, x] = v
        velocity_out[2, x] = w
        pressure_out[x] = p_own

        flow_xm, flow_xp = 0.5 * (u[x] + u[x + 1]), 0.5 * (u[x + 1] + u[x + 2])
        v_m = jnp.where(row == 0, v_low, roll_rows(v, 1))
        v_p = jnp.where(row == BLOCK - 1, v_high, roll_rows(v, -1))
        flow_ym, flow_yp = 0.5 * (v_m + v), 0.5 * (v + v_p)
        w_m = jnp.where(lane > 0, roll_lanes(w, 1), 0.0)
        w_p = jnp.where(lane < LANES - 1, roll_lanes(w, -1), 0.0)
        flow_zm, flow_zp = 0.5 * (w_m + w), 0.5 * (w + w_p)

        def leaves(high, low):
            return jnp.maximum(high, 0.0) - jnp.minimum(low, 0.0)

        keep = 1.0 - time_step * (
            leaves(flow_xp, flow_xm) + leaves(flow_yp, flow_ym) + leaves(flow_zp, flow_zm)
        )
        from_xm, from_xp = (
            time_step * jnp.maximum(flow_xm, 0.0),
            -time_step * jnp.minimum(flow_xp, 0.0),
        )
        from_ym, from_yp = (
            time_step * jnp.maximum(flow_ym, 0.0),
            -time_step * jnp.minimum(flow_yp, 0.0),
        )
        from_zm = jnp.where(lane > 0, time_step * jnp.maximum(flow_zm, 0.0), 0.0)
        from_zp = jnp.where(lane < LANES - 1, -time_step * jnp.minimum(flow_zp, 0.0), 0.0)
        for s in range(SPECIES):
            c = species[s, x]
            if x > 0:
                c_xm = species[s, x - 1]
            else:
                c_xm = species_beside(s, 0)
            if x < 3:
                c_xp = species[s, x + 1]
            else:
                c_xp = species_beside(s, 1)
            r = 4 * s + x
            c_ym = jnp.where(row == 0, y_low[r : r + 1], roll_rows(c, 1))
            c_yp = jnp.where(row == BLOCK - 1, y_high[r : r + 1], roll_rows(c, -1))
            total = keep * c + (from_xm * c_xm + from_xp * c_xp)
            total = total + (from_ym * c_ym + from_yp * c_yp)
            total = total + (from_zm * roll_lanes(c, 1) + from_zp * roll_lanes(c, -1))
            species_out[s, x] = total


def call(kernel, outs, scratch, *operands, where=pltpu.VMEM, semaphores=0, grant=24):
    vmem = pl.BlockSpec(memory_space=pltpu.VMEM)
    shapes = [jax.ShapeDtypeStruct(shape, jnp.float32) for shape in outs]
    scratch = [pltpu.VMEM(shape, jnp.float32) for shape in scratch]
    if semaphores:
        scratch = [*scratch, pltpu.SemaphoreType.DMA((semaphores,))]
    return pl.pallas_call(
        kernel,
        out_shape=shapes,
        in_specs=[pl.BlockSpec(memory_space=where) for _ in operands],
        out_specs=[vmem for _ in outs],
        scratch_shapes=scratch,
        cost_estimate=pl.CostEstimate(flops=1000000, bytes_accessed=1000000, transcendentals=0),
        compiler_params=pltpu.CompilerParams(vmem_limit_bytes=grant * 2**20),
        interpret=INTERPRET,
    )(*operands)


def gathered_over(array, groups):
    return lax.all_gather(array, ("slab", "cross"), axis_index_groups=groups)


def local(n_chips, velocity, density, source, species):
    def device(slab, cross):
        return 4 * slab + cross

    chips = [[device(2 * j + k, c) for c in range(4) for k in range(2)] for j in range(n_chips)]
    cores = [
        [device(2 * j, c), device(2 * j + 1, c)] for j in range(n_chips) for c in range(4)
    ]
    facing = [
        [device(2 * j + 1, c), device(2 * j + 2, c)] for j in range(n_chips - 1) for c in range(4)
    ]
    for slab in (0, 2 * n_chips - 1):
        facing += [[device(slab, 0), device(slab, 1)], [device(slab, 2), device(slab, 3)]]

    def both_ways(pairs):
        return [pair for left, right in pairs for pair in ((left, right), (right, left))]

    beside = both_ways([(2 * j + 1, 2 * j + 2) for j in range(n_chips - 1)])
    two_away = both_ways([(2 * j, 2 * j + 5) for j in range(n_chips - 2)])

    within = [pair for j in range(n_chips) for pair in ((2 * j, 2 * j + 1), (2 * j + 1, 2 * j))]
    upward = [(c, c + 1) for c in range(3)]
    downward = [(c + 1, c) for c in range(3)]

    def plane(n):
        return (n, ROWS, LANES)

    def padded(n, rows=ROWS):
        return (n, rows + 2 * PAD, LANES)

    def halved(n):
        return (n, HALF, LANES)

    def bind(kernel):
        return functools.partial(kernel, n_chips)

    (own,) = call(
        prepare, [(OWN, LANES)], [velocity.shape, density.shape, source.shape],
        velocity, density, source,
        where=HBM, semaphores=3, grant=63,
    )
    gathered = gathered_over(own, chips)
    sent, sent_far, edge = call(bind(assemble), [plane(17), plane(2), plane(2)], [], gathered)
    near = lax.ppermute(sent, "slab", beside)
    far = lax.ppermute(sent_far, "slab", two_away)
    species_near, species_beside, edge_low, edge_high = call(
        bind(species_edges), [(144, LANES), (144, LANES), (40, LANES), (40, LANES)], [], species
    )
    y_low = lax.ppermute(edge_high, "cross", upward)
    y_high = lax.ppermute(edge_low, "cross", downward)
    u_beside, v_rims = call(bind(flow_rims), [(BLOCK, LANES), (8, LANES)], [], gathered)
    mine = jnp.concatenate([near, far], 0)
    swapped = lax.ppermute(mine, "slab", within)
    mobile_w, weights, pressure, residual, coarse, outer, sent_two = call(
        bind(first_cycle),
        [
            padded(26), (8, *plane(24)), padded(24), halved(10), halved(12), PLANE, (272, LANES),
        ],
        [plane(24), padded(24), plane(10)],
        sent, edge, mine, swapped, species_near,
    )
    near = gathered_over(sent_two, facing).reshape(544, LANES)
    sides = gathered_over(jnp.concatenate([near, species_beside], 0), cores)
    pressure, residual, coarse_weights, sent = call(
        bind(second_cycle),
        [padded(14), halved(6), (8, *halved(18)), plane(2)],
        [
            padded(20, HALF), halved(18), padded(18, HALF), padded(18, HALF), padded(24), padded(24),
            plane(6),
        ],
        weights, pressure, residual, coarse, sides,
    )
    near = gathered_over(sent, facing)
    swapped = gathered_over(near[:, 1], cores)
    return call(
        bind(finish),
        [velocity.shape, density.shape, species.shape],
        [
            halved(14), plane(16), padded(12, HALF), padded(12, HALF), padded(12), padded(12),
            padded(8),
        ],
        mobile_w, weights, pressure, residual, coarse_weights, near, swapped,
        velocity, species, outer, u_beside, v_rims, sides, y_low, y_high,
    )


def solution(mesh):
    n_chips = mesh.shape["slab"] // 2
    block = P("slab", "cross", None)
    stack = P(None, "slab", "cross", None)

    def step(*arrays):
        return tuple(local(n_chips, *arrays))

    return jax.shard_map(
        step,
        mesh=mesh,
        in_specs=(stack, block, block, stack),
        out_specs=(stack, block, stack),
        check_vma=False,
    )
```
